8 devices in a mesh: dp: 2 (over z, y), tp: 4 (over x, core).
Axes of the slice: x: 2, y: 2, z: 1, core: 2. Of those that a mesh axis runs over, the one named last changes fastest.
Arguments:
- x_in: bfloat16 [2, 128, 2560], P('dp', 'tp'), parts along dimension 0
- y_grad: bfloat16 [2, 128, 2560], P('dp', 'tp'), parts along dimension 0
- ln_par: float32 [2, 4, 2560], replicated
- bias_d: float32 [2, 2, 2560], replicated
- w_qkv: bfloat16 [2, 2560, 3, 20, 128], P(None, None, None, 'tp')
- w_out: bfloat16 [2, 20, 128, 2560], P(None, 'tp')
- w_up: bfloat16 [2, 2560, 10240], P(None, None, 'tp')
- b_up: float32 [2, 10240], P(None, 'tp')
- w_down: bfloat16 [2, 10240, 2560], P(None, 'tp')
Outputs:
- output 1: bfloat16 [2, 128, 2560], P('dp', 'tp'), parts along dimension 0
- output 2: bfloat16 [2, 128, 2560], P('dp', 'tp'), parts along dimension 0
- output 3: float32 [4, 4, 2560], P('dp'), parts along dimension 0
- output 4: float32 [4, 2, 2560], P('dp'), parts along dimension 0
- output 5: bfloat16 [4, 2560, 3, 20, 128], P('dp', None, None, 'tp'), parts along dimension 0
- output 6: bfloat16 [4, 20, 128, 2560], P('dp', 'tp'), parts along dimension 0
- output 7: bfloat16 [4, 2560, 10240], P('dp', None, 'tp'), parts along dimension 0
- output 8: float32 [4, 10240], P('dp', 'tp'), parts along dimension 0
- output 9: bfloat16 [4, 10240, 2560], P('dp', 'tp'), parts along dimension 0
There are 2 independent parts. The reference program is written for one: setup_inputs(seed, part) draws one part's arguments, and reference() takes and returns one part's arrays. A program takes and returns all parts, laid end to end along the dimension named above; an argument that names none is the same for every part.
All inputs are finite; a program needn't handle non-finite values.
Results may differ from the reference program's by a relative error of at most 0.02.
Values are sent between devices in bfloat16 or wider.
A program may use at most 1 GiB of HBM per device.

```python
import math
import jax
import jax.numpy as jnp
from jax import lax

N_BATCH = 1
SEQ_LEN = 128
D_MODEL = 2560
N_HEADS = 20
HEAD_DIM = 128
FF_DIM = 10240
N_LAYERS = 2


def layer_norm(row_vals, ln_gain, ln_shift):
    mean_val = jnp.mean(row_vals, axis=-1, keepdims=True)
    centered = row_vals - mean_val
    var_val = jnp.mean(centered * centered, axis=-1, keepdims=True)
    return centered * lax.rsqrt(var_val + 1e-5) * ln_gain + ln_shift


def setup_inputs(seed: int = 0, part: int = 0) -> dict:
    part_key = jax.random.fold_in(jax.random.key(seed), part)
    part_list = jax.random.split(part_key, 3)
    key_list = jax.random.split(jax.random.key(seed + 1), 7)
    act_shape = (N_BATCH, SEQ_LEN, D_MODEL)
    token_scale = jax.random.uniform(part_list[0], (N_BATCH, SEQ_LEN, 1), jnp.float32, 0.5, 1.5)
    x_in = (jax.random.normal(part_list[1], act_shape, jnp.float32) * token_scale).astype(jnp.bfloat16)
    y_grad = jax.random.normal(part_list[2], act_shape, jnp.float32).astype(jnp.bfloat16)
    ln_base = jnp.array([1.0, 0.0, 1.0, 0.0], jnp.float32)[None, :, None]
    ln_par = ln_base + 0.2 * jax.random.normal(key_list[0], (N_LAYERS, 4, D_MODEL), jnp.float32)
    bias_d = 0.2 * jax.random.normal(key_list[1], (N_LAYERS, 2, D_MODEL), jnp.float32)
    qk_gain = (math.log(SEQ_LEN) / 2.0) ** 0.25
    qkv_gain = jnp.array([qk_gain, qk_gain, 1.0], jnp.float32)[None, None, :, None, None] * D_MODEL ** -0.5
    w_qkv = (jax.random.normal(key_list[2], (N_LAYERS, D_MODEL, 3, N_HEADS, HEAD_DIM), jnp.float32) * qkv_gain).astype(jnp.bfloat16)
    out_gain = 0.3 * SEQ_LEN ** 0.25 * D_MODEL ** -0.5
    w_out = (jax.random.normal(key_list[3], (N_LAYERS, N_HEADS, HEAD_DIM, D_MODEL), jnp.float32) * out_gain).astype(jnp.bfloat16)
    w_up = (jax.random.normal(key_list[4], (N_LAYERS, D_MODEL, FF_DIM), jnp.float32) * D_MODEL ** -0.5).astype(jnp.bfloat16)
    b_up = 0.5 * jax.random.normal(key_list[5], (N_LAYERS, FF_DIM), jnp.float32)
    w_down = (jax.random.normal(key_list[6], (N_LAYERS, FF_DIM, D_MODEL), jnp.float32) * FF_DIM ** -0.5).astype(jnp.bfloat16)
    return dict(x_in=x_in, y_grad=y_grad, ln_par=ln_par, bias_d=bias_d, w_qkv=w_qkv, w_out=w_out, w_up=w_up, b_up=b_up, w_down=w_down)


def head_attention(qkv_head):
    q_head = qkv_head[:, 0].astype(jnp.float32)
    k_head = qkv_head[:, 1].astype(jnp.float32)
    v_head = qkv_head[:, 2].astype(jnp.float32)
    scores = jnp.dot(q_head, k_head.T) * (HEAD_DIM ** -0.5)
    positions = jnp.arange(SEQ_LEN)
    causal = positions[:, None] >= positions[None, :]
    scores = jnp.where(causal, scores, -1e30)
    prob_bf = jax.nn.softmax(scores, axis=-1).astype(jnp.bfloat16)
    return jnp.dot(prob_bf.astype(jnp.float32), v_head).astype(jnp.bfloat16)


def attention_all(qkv_vals):
    per_head = jnp.transpose(qkv_vals, (0, 3, 1, 2, 4)).reshape(N_BATCH * N_HEADS, SEQ_LEN, 3, HEAD_DIM)
    head_out = lax.map(jax.checkpoint(head_attention), per_head)
    return jnp.transpose(head_out.reshape(N_BATCH, N_HEADS, SEQ_LEN, HEAD_DIM), (0, 2, 1, 3))


def block_forward(residual, layer_w):
    ln_vals, bias_vals, w_qkv, w_out, w_up, b_up, w_down = layer_w
    h_one = layer_norm(residual, ln_vals[0], ln_vals[1]).astype(jnp.bfloat16)
    qkv_vals = jnp.einsum('bsd,dche->bsche', h_one.astype(jnp.float32), w_qkv.astype(jnp.float32)).astype(jnp.bfloat16)
    attn_vals = attention_all(qkv_vals)
    attn_out = jnp.einsum('bshe,hed->bsd', attn_vals.astype(jnp.float32), w_out.astype(jnp.float32))
    residual = residual + attn_out + bias_vals[0]
    h_two = layer_norm(residual, ln_vals[2], ln_vals[3]).astype(jnp.bfloat16)
    pre_act = jnp.einsum('bsd,df->bsf', h_two.astype(jnp.float32), w_up.astype(jnp.float32)) + b_up
    act_vals = jax.nn.gelu(pre_act, approximate=True).astype(jnp.bfloat16)
    mlp_out = jnp.einsum('bsf,fd->bsd', act_vals.astype(jnp.float32), w_down.astype(jnp.float32))
    return residual + mlp_out + bias_vals[1]


def reference(x_in, y_grad, ln_par, bias_d, w_qkv, w_out, w_up, b_up, w_down):
    weights = (ln_par, bias_d, w_qkv, w_out, w_up, b_up, w_down)

    def forward(x_vals, layer_stack):
        def scan_body(residual, layer_w):
            return block_forward(residual, layer_w), None
        final_res, _ = lax.scan(scan_body, x_vals.astype(jnp.float32), layer_stack)
        return final_res

    final_res, pullback = jax.vjp(forward, x_in, weights)
    x_ct, w_ct = pullback(y_grad.astype(jnp.float32))
    return (final_res.astype(jnp.bfloat16), x_ct, w_ct[0], w_ct[1], w_ct[2], w_ct[3], w_ct[4], w_ct[5], w_ct[6])
```

```python
import jax
import jax.numpy as jnp
from jax import lax
from jax.experimental import pallas as pl
from jax.experimental.pallas import tpu as pltpu
from jax.sharding import PartitionSpec as P

MESH = pl.DeviceIdType.MESH
F32, BF16 = jnp.float32, jnp.bfloat16
N_LAYERS, SEQ, BLK, D, HEADS, HD, FF = 2, 128, 32, 2560, 5, 128, 2560
ATT = HEADS * HD
QKV = 3 * ATT
C = 512
NC = D // C
SCALE = HD ** -0.5
GELU_K = 0.7978845608028654
GELU_C = 0.044715
VMEM_ALL = 67043328


def mm(a, b):
    return jnp.dot(a, b, preferred_element_type=F32)


def mm_nt(a, b):
    return lax.dot_general(a, b, (((1,), (1,)), ((), ())), preferred_element_type=F32)


def mm_tn(a, b):
    return mm(a.T, b)


def chunk(c, size=C):
    return pl.ds(pl.multiple_of(c * size, size), size)


def chain_kernel(x_ref, dy_ref, ln_ref, bias_ref, bup_ref, wqkv_h, wo_h, wu_h, wd_h,
                 y_ref, xg_ref, small_ref, bupg_ref, h_o, h2_o, dm_o, da_o, a_o, act_o, dpre_o, dqkv_o,
                 wq, wo, wu, wd, h_g, h2_g, dm_g, da_g, qkv, prob, attn, act, gp, dpre, dqkv,
                 xh1, xh2, rs1, rs2, res, acc, acct, part, own, rr, xx, ss, sg, sgr,
                 wsem, osem, agsem, rssem, gsem):
    me = lax.axis_index('tp')
    x_id = lax.div(me, 2)
    core = lax.rem(me, 2)
    sib = x_id * 2 + (1 - core)
    cross = (1 - x_id) * 2 + core
    diag = (1 - x_id) * 2 + (1 - core)

    def remote(src, dst, send, recv, dev):
        return pltpu.make_async_remote_copy(src_ref=src, dst_ref=dst, send_sem=send, recv_sem=recv,
                                            device_id={'tp': dev}, device_id_type=MESH)

    def weight_copies(kind, layer):
        if kind == 0:
            return [pltpu.make_async_copy(wqkv_h.at[layer, j], wq.at[:, pl.ds(j * HD, HD)], wsem.at[0, j]) for j in range(3 * HEADS)]
        if kind == 1:
            return [pltpu.make_async_copy(wo_h.at[layer], wo, wsem.at[1, 0])]
        src, dst = ((wu_h, wu), (wd_h, wd))[kind - 2]
        return [pltpu.make_async_copy(src.at[layer, pl.ds(j * C, C)], dst.at[pl.ds(j * C, C)], wsem.at[kind, j]) for j in range(NC)]

    def load_w(kind, layer):
        for copy in weight_copies(kind, layer):
            copy.start()

    def wait_w(kind, layer):
        for copy in weight_copies(kind, layer):
            copy.wait()

    def out_copy(i, src, dst, layer):
        return pltpu.make_async_copy(src.at[layer], dst.at[layer], osem.at[i, layer])

    outs = [(h_g, h_o), (h2_g, h2_o), (dm_g, dm_o), (da_g, da_o), (attn, a_o), (act, act_o), (dpre, dpre_o), (dqkv, dqkv_o)]

    def ag_side(g, layer, c):
        mine = g.at[layer, me, :, chunk(c)]
        return remote(mine, mine, agsem.at[0, c], agsem.at[1, c], sib)

    def ag_across(g, layer, c):
        mine = g.at[layer, me, :, chunk(c)]
        return remote(mine, mine, agsem.at[2, c], agsem.at[3, c], cross)

    def ag_forward(g, layer, c):
        theirs = g.at[layer, cross, :, chunk(c)]
        return remote(theirs, theirs, agsem.at[4, c], agsem.at[5, c], sib)

    def ag_start(g, layer):
        for c in range(NC):
            ag_across(g, layer, c).start()
        for c in range(NC):
            ag_side(g, layer, c).start()

    def ag_consume(g, layer, compute):
        @pl.loop(0, NC + 1)
        def _(c):
            @pl.when(c < NC)
            def _():
                ag_across(g, layer, c).wait_recv()
                ag_forward(g, layer, c).start()

            @pl.when(c >= 1)
            def _():
                cc = c - 1
                ag_side(g, layer, cc).wait_recv()
                ag_forward(g, layer, cc).wait_recv()
                compute(cc)

        @pl.loop(0, NC)
        def _(c):
            ag_side(g, layer, c).wait_send()
            ag_across(g, layer, c).wait_send()
            ag_forward(g, layer, c).wait_send()

    def rs_side(par, c):
        return remote(part.at[:, 1 - core, :, chunk(c)], rr.at[par, :, :, chunk(c)], rssem.at[par, 0, c], rssem.at[par, 1, c], sib)

    def rs_across(par, c):
        return remote(ss.at[:, chunk(c)], xx.at[par, :, chunk(c)], rssem.at[par, 2, c], rssem.at[par, 3, c], cross)

    def rs_run(par, compute, lag=2):
        @pl.loop(0, NC + lag)
        def _(c):
            @pl.when(c < NC)
            def _():
                vals = compute(c)
                for b in range(4):
                    part[b // 2, b % 2, :, chunk(c)] = vals[b * BLK:(b + 1) * BLK]
                rs_side(par, c).start()

            @pl.when(c >= lag)
            def _():
                cc = c - lag
                rs_side(par, cc).wait_recv()
                cols = chunk(cc)
                ss[:, cols] = (part[1 - x_id, core, :, cols] + rr[par, 1 - x_id, :, cols]).astype(BF16)
                rs_across(par, cc).start()
                own[:, cols] = part[x_id, core, :, cols] + rr[par, x_id, :, cols]

        @pl.loop(0, NC)
        def _(c):
            rs_across(par, c).wait_recv()
            rs_side(par, c).wait_send()
            rs_across(par, c).wait_send()
            own[:, chunk(c)] += xx[par, :, chunk(c)].astype(F32)

    def normed(vals, gain, shift, xh, rs, layer):
        mean_val = jnp.mean(vals, axis=-1, keepdims=True)
        centered = vals - mean_val
        rstd = lax.rsqrt(jnp.mean(centered * centered, axis=-1, keepdims=True) + 1e-5)
        hat = centered * rstd
        xh[layer] = hat
        rs[layer] = jnp.broadcast_to(rstd, (BLK, 128))
        return (hat * gain + shift).astype(BF16)

    def norm_grad(d_out, gain, xh, rs, layer, gain_row):
        hat = xh[layer]
        rstd = rs[layer][:, :1]
        sg[layer, gain_row:gain_row + 1, :] = jnp.sum(d_out * hat, axis=0, keepdims=True)
        sg[layer, gain_row + 1:gain_row + 2, :] = jnp.sum(d_out, axis=0, keepdims=True)
        d_hat = d_out * gain
        m1 = jnp.mean(d_hat, axis=-1, keepdims=True)
        m2 = jnp.mean(d_hat * hat, axis=-1, keepdims=True)
        return rstd * (d_hat - m1 - hat * m2)

    def small_copies(layer):
        return [remote(sg.at[layer], sgr.at[layer, i], gsem.at[layer, 0, i], gsem.at[layer, 1, i], dev)
                for i, dev in enumerate((sib, cross, diag))]

    load_w(0, 0)
    barrier = pltpu.get_barrier_semaphore()
    for dev in (sib, cross, diag):
        pl.semaphore_signal(barrier, inc=1, device_id={'tp': dev}, device_id_type=MESH)
    res[...] = x_ref[0].astype(F32)
    pl.semaphore_wait(barrier, 3)

    row_id = lax.broadcasted_iota(jnp.int32, (SEQ, SEQ), 0)
    col_id = lax.broadcasted_iota(jnp.int32, (SEQ, SEQ), 1)
    causal = row_id >= col_id

    @pl.loop(0, N_LAYERS)
    def _(layer):
        first = layer == 0
        lnp = ln_ref[layer]
        h_g[layer, me] = normed(res[...], lnp[0:1], lnp[1:2], xh1, rs1, layer)
        ag_start(h_g, layer)
        acc[...] = jnp.zeros_like(acc)
        wait_w(0, layer)

        @pl.when(first)
        def _():
            load_w(1, 0)
            load_w(2, 0)

        def qkv_chunk(c):
            h = h_g[layer, :, :, chunk(c)].reshape(SEQ, C)
            for n in range(0, QKV, 640):
                acc[:, n:n + 640] += mm(h, wq[chunk(c), n:n + 640])
        ag_consume(h_g, layer, qkv_chunk)
        out_copy(0, h_g, h_o, layer).start()

        @pl.when(first)
        def _():
            load_w(0, 1)

        for j in range(3 * HEADS):
            qkv[layer, :, j * HD:(j + 1) * HD] = acc[:, j * HD:(j + 1) * HD].astype(BF16)
        for hd in range(HEADS):
            q = qkv[layer, :, hd * HD:(hd + 1) * HD]
            k = qkv[layer, :, ATT + hd * HD:ATT + (hd + 1) * HD]
            v = qkv[layer, :, 2 * ATT + hd * HD:2 * ATT + (hd + 1) * HD]
            scores = jnp.where(causal, mm_nt(q, k) * SCALE, -1e30)
            e = jnp.exp(scores - jnp.max(scores, axis=-1, keepdims=True))
            p = (e / jnp.sum(e, axis=-1, keepdims=True)).astype(BF16)
            prob[layer, hd] = p
            attn[layer, :, hd * HD:(hd + 1) * HD] = mm(p, v).astype(BF16)
        out_copy(4, attn, a_o, layer).start()
        wait_w(1, layer)

        @pl.when(first)
        def _():
            load_w(3, 0)
        rs_run(0, lambda c: mm(attn[layer], wo[:, chunk(c)]))

        @pl.when(first)
        def _():
            load_w(1, 1)
        res[...] = res[...] + own[...] + bias_ref[layer, 0:1]

        h2_g[layer, me] = normed(res[...], lnp[2:3], lnp[3:4], xh2, rs2, layer)
        ag_start(h2_g, layer)
        acc[...] = jnp.zeros_like(acc)
        wait_w(2, layer)

        def up_chunk(c):
            h = h2_g[layer, :, :, chunk(c)].reshape(SEQ, C)
            for n in range(0, FF, C):
                acc[:, n:n + C] += mm(h, wu[chunk(c), n:n + C])
        ag_consume(h2_g, layer, up_chunk)
        out_copy(1, h2_g, h2_o, layer).start()

        @pl.when(first)
        def _():
            load_w(2, 1)

        @pl.loop(0, FF // C)
        def _(c):
            pre = acc[:, chunk(c)] + bup_ref[pl.ds(layer, 1), chunk(c)]
            sq = pre * pre
            t = jnp.tanh(GELU_K * (pre + GELU_C * (sq * pre)))
            cdf = 0.5 * (1.0 + t)
            act[layer, :, chunk(c)] = (pre * cdf).astype(BF16)
            gp[layer, :, chunk(c)] = cdf + 0.5 * pre * (1.0 - t * t) * (GELU_K * (1.0 + 3.0 * GELU_C * sq))
        out_copy(5, act, act_o, layer).start()
        wait_w(3, layer)
        rs_run(1, lambda c: mm(act[layer], wd[:, chunk(c)]))

        @pl.when(first)
        def _():
            load_w(3, 1)
        res[...] = res[...] + own[...] + bias_ref[layer, 1:2]

    y_ref[...] = res[...].astype(BF16)
    res[...] = dy_ref[0].astype(F32)
    sg[...] = jnp.zeros_like(sg)

    @pl.loop(0, N_LAYERS)
    def _(step):
        layer = N_LAYERS - 1 - step
        top = step == 0
        low = step == N_LAYERS - 1
        lnp = ln_ref[layer]
        sg[layer, 5:6, :] = jnp.sum(res[...], axis=0, keepdims=True)
        dm_g[layer, me] = res[...].astype(BF16)
        ag_start(dm_g, layer)
        acct[...] = jnp.zeros_like(acct)

        @pl.when(low)
        def _():
            wait_w(3, 0)

        def dact_chunk(c):
            g = dm_g[layer, :, :, chunk(c)].reshape(SEQ, C)
            for n in range(0, FF, C):
                acct[n:n + C, :] += mm_nt(wd[n:n + C, chunk(c)], g)
        ag_consume(dm_g, layer, dact_chunk)
        out_copy(2, dm_g, dm_o, layer).start()

        @pl.when(top)
        def _():
            load_w(3, 0)

        @pl.loop(0, FF // C)
        def _(c):
            d_pre = acct[chunk(c), :].T * gp[layer, :, chunk(c)]
            bupg_ref[pl.ds(layer, 1), chunk(c)] = jnp.sum(d_pre, axis=0, keepdims=True)
            dpre[layer, :, chunk(c)] = d_pre.astype(BF16)
        out_copy(6, dpre, dpre_o, layer).start()

        @pl.when(low)
        def _():
            wait_w(2, 0)
        rs_run(0, lambda c: mm_nt(wu[chunk(c), :], dpre[layer]).T)

        @pl.when(top)
        def _():
            load_w(2, 0)
        res[...] = res[...] + norm_grad(own[...], lnp[2:3], xh2, rs2, layer, 2)

        sg[layer, 4:5, :] = jnp.sum(res[...], axis=0, keepdims=True)
        da_g[layer, me] = res[...].astype(BF16)
        ag_start(da_g, layer)
        acct[0:ATT, :] = jnp.zeros((ATT, SEQ), F32)

        @pl.when(low)
        def _():
            wait_w(1, 0)

        def dattn_chunk(c):
            g = da_g[layer, :, :, chunk(c)].reshape(SEQ, C)
            acct[0:ATT, :] += mm_nt(wo[:, chunk(c)], g)
        ag_consume(da_g, layer, dattn_chunk)
        out_copy(3, da_g, da_o, layer).start()

        @pl.when(top)
        def _():
            load_w(1, 0)

        @pl.when(low)
        def _():
            for copy in small_copies(N_LAYERS - 1):
                copy.start()

        for hd in range(HEADS):
            q = qkv[layer, :, hd * HD:(hd + 1) * HD]
            k = qkv[layer, :, ATT + hd * HD:ATT + (hd + 1) * HD]
            v = qkv[layer, :, 2 * ATT + hd * HD:2 * ATT + (hd + 1) * HD]
            p = prob[layer, hd]
            d_o = acct[hd * HD:(hd + 1) * HD, :].T.astype(BF16)
            d_p = mm_nt(d_o, v)
            d_v = mm(p.T, d_o)
            pf = p.astype(F32)
            dot = jnp.sum(d_p * pf, axis=-1, keepdims=True)
            d_s = (pf * (d_p - dot) * SCALE).astype(BF16)
            dqkv[layer, :, hd * HD:(hd + 1) * HD] = mm(d_s, k).astype(BF16)
            dqkv[layer, :, ATT + hd * HD:ATT + (hd + 1) * HD] = mm(d_s.T, q).astype(BF16)
            dqkv[layer, :, 2 * ATT + hd * HD:2 * ATT + (hd + 1) * HD] = d_v.astype(BF16)
        out_copy(7, dqkv, dqkv_o, layer).start()

        @pl.when(low)
        def _():
            wait_w(0, 0)
        rs_run(1, lambda c: mm_nt(wq[chunk(c), :], dqkv[layer]).T)

        @pl.when(top)
        def _():
            load_w(0, 0)
        res[...] = res[...] + norm_grad(own[...], lnp[0:1], xh1, rs1, layer, 0)

    for copy in small_copies(0):
        copy.start()
    xg_ref[...] = res[...].astype(BF16)
    for layer in reversed(range(N_LAYERS)):
        for copy in small_copies(layer):
            copy.wait()
        small_ref[layer] = (sg[layer] + sgr[layer, 0]) + (sgr[layer, 1] + sgr[layer, 2])
    for layer in range(N_LAYERS):
        for i, (src, dst) in enumerate(outs):
            out_copy(i, src, dst, layer).wait()


def grads_kernel(y_in, xg_in, small_in, bupg_in, h_h, h2_h, dm_h, da_h, a_h, act_h, dpre_h, dqkv_h,
                 y_o, xg_o, lng_o, biasg_o, wqkv_o, wo_o, wu_o, bupg_o, wd_o,
                 h, h2, dm, da, attn, act, dpre, dqkv, big, qbuf, obuf, isem, bsem, qsem, osem):
    ins = [(dm_h, dm), (act_h, act), (h2_h, h2), (dpre_h, dpre), (da_h, da), (a_h, attn), (h_h, h), (dqkv_h, dqkv)]

    def in_copy(i, layer):
        return pltpu.make_async_copy(ins[i][0].at[layer], ins[i][1].at[layer], isem.at[i, layer])

    for layer in reversed(range(N_LAYERS)):
        for i in range(len(ins)):
            in_copy(i, layer).start()
    y_o[...] = y_in[...]
    xg_o[...] = xg_in[...]
    lng_o[...] = small_in[:, 0:4, :]
    biasg_o[...] = small_in[:, 4:6, :]
    bupg_o[...] = bupg_in[...]

    def big_copy(dst, layer, c, slot):
        return pltpu.make_async_copy(big.at[slot], dst.at[layer, chunk(c)], bsem.at[slot])

    def q_copy(layer, c, slot):
        return pltpu.make_async_copy(qbuf.at[slot], wqkv_o.at[layer, :, chunk(c), :], qsem.at[slot])

    def o_copy(layer, c):
        return pltpu.make_async_copy(obuf.at[c], wo_o.at[layer, pl.ds(c * (ATT // 2), ATT // 2)], osem.at[c])

    for step, layer in enumerate(reversed(range(N_LAYERS))):
        for w, (dst, left, right) in enumerate(((wd_o, act, dm), (wu_o, h2, dpre))):
            in_copy(2 * w, layer).wait()
            in_copy(2 * w + 1, layer).wait()
            base = (2 * step + w) * NC

            @pl.loop(0, NC)
            def _(c):
                slot = lax.rem(base + c, 3)

                @pl.when(base + c >= 3)
                def _():
                    big_copy(dst, layer, c, slot).wait()
                lt = left[layer, :, chunk(c)].T
                for n in range(0, D, C):
                    big[slot, :, n:n + C] = mm(lt, right[layer, :, n:n + C]).astype(BF16)
                big_copy(dst, layer, c, slot).start()
        in_copy(4, layer).wait()
        in_copy(5, layer).wait()
        for c in range(2):
            if step > 0:
                o_copy(layer, c).wait()
            lt = attn[layer, :, :].T[c * (ATT // 2):(c + 1) * (ATT // 2)]
            for n in range(0, D, C):
                obuf[c, :, n:n + C] = mm(lt, da[layer, :, n:n + C]).astype(BF16)
            o_copy(layer, c).start()
        in_copy(6, layer).wait()
        in_copy(7, layer).wait()
        qbase = step * NC

        @pl.loop(0, NC)
        def _(c):
            slot = lax.rem(qbase + c, 3)

            @pl.when(qbase + c >= 3)
            def _():
                q_copy(layer, c, slot).wait()
            lt = h[layer, :, chunk(c)].T
            for n in range(0, QKV, 3 * HD):
                vals = mm(lt, dqkv[layer, :, n:n + 3 * HD]).astype(BF16)
                for j in range(3):
                    qbuf[slot, n // HD + j] = vals[:, j * HD:(j + 1) * HD]
            q_copy(layer, c, slot).start()
    for slot in range(3):
        big_copy(wu_o, 0, 0, slot).wait()
        q_copy(0, 0, slot).wait()
    for c in range(2):
        o_copy(0, c).wait()


def solution(mesh):
    vmem = pl.BlockSpec(memory_space=pltpu.VMEM)
    hbm = pl.BlockSpec(memory_space=pl.ANY)

    def device_step(x_loc, dy_loc, ln_par, bias_d, w_qkv, w_out, w_up, b_up, w_down):
        wqkv_t = jnp.transpose(w_qkv, (0, 2, 3, 1, 4)).reshape(N_LAYERS, 3 * HEADS, D, HD)
        wo_t = w_out.reshape(N_LAYERS, ATT, D)
        sds = jax.ShapeDtypeStruct
        gath = (N_LAYERS, 4, BLK, D)
        dma = pltpu.SemaphoreType.DMA
        chain_out = pl.pallas_call(
            chain_kernel,
            name='chain',
            out_shape=(sds((BLK, D), BF16), sds((BLK, D), BF16), sds((N_LAYERS, 8, D), F32), sds((N_LAYERS, FF), F32),
                       sds(gath, BF16), sds(gath, BF16), sds(gath, BF16), sds(gath, BF16),
                       sds((N_LAYERS, SEQ, ATT), BF16), sds((N_LAYERS, SEQ, FF), BF16), sds((N_LAYERS, SEQ, FF), BF16),
                       sds((N_LAYERS, SEQ, QKV), BF16)),
            in_specs=[vmem] * 5 + [hbm] * 4,
            out_specs=tuple([vmem] * 4 + [hbm] * 8),
            scratch_shapes=[
                pltpu.VMEM((D, QKV), BF16), pltpu.VMEM((ATT, D), BF16), pltpu.VMEM((D, FF), BF16), pltpu.VMEM((FF, D), BF16),
                pltpu.VMEM(gath, BF16), pltpu.VMEM(gath, BF16), pltpu.VMEM(gath, BF16), pltpu.VMEM(gath, BF16),
                pltpu.VMEM((N_LAYERS, SEQ, QKV), BF16), pltpu.VMEM((N_LAYERS, HEADS, SEQ, SEQ), BF16),
                pltpu.VMEM((N_LAYERS, SEQ, ATT), BF16), pltpu.VMEM((N_LAYERS, SEQ, FF), BF16), pltpu.VMEM((N_LAYERS, SEQ, FF), F32),
                pltpu.VMEM((N_LAYERS, SEQ, FF), BF16), pltpu.VMEM((N_LAYERS, SEQ, QKV), BF16),
                pltpu.VMEM((N_LAYERS, BLK, D), F32), pltpu.VMEM((N_LAYERS, BLK, D), F32),
                pltpu.VMEM((N_LAYERS, BLK, 128), F32), pltpu.VMEM((N_LAYERS, BLK, 128), F32),
                pltpu.VMEM((BLK, D), F32), pltpu.VMEM((SEQ, D), F32), pltpu.VMEM((D, SEQ), F32),
                pltpu.VMEM((2, 2, BLK, D), F32), pltpu.VMEM((BLK, D), F32), pltpu.VMEM((2, 2, BLK, D), F32),
                pltpu.VMEM((2, BLK, D), BF16), pltpu.VMEM((BLK, D), BF16),
                pltpu.VMEM((N_LAYERS, 8, D), F32), pltpu.VMEM((N_LAYERS, 3, 8, D), F32),
                dma((4, 3 * HEADS)), dma((8, N_LAYERS)), dma((6, NC)), dma((2, 4, NC)), dma((N_LAYERS, 2, 3)),
            ],
            compiler_params=pltpu.CompilerParams(collective_id=0, has_side_effects=True, vmem_limit_bytes=VMEM_ALL),
        )(x_loc, dy_loc, ln_par, bias_d, b_up, wqkv_t, wo_t, w_up, w_down)
        y_loc, xg_loc, small, bupg, h, h2, dm, da, attn, act, dpre, dqkv = chain_out
        flat = (N_LAYERS, SEQ, D)
        y_out, x_grad, lng, biasg, wqkv_g, wo_g, wu_g, bupg_o, wd_g = pl.pallas_call(
            grads_kernel,
            name='grads',
            out_shape=(sds((BLK, D), BF16), sds((BLK, D), BF16), sds((N_LAYERS, 4, D), F32), sds((N_LAYERS, 2, D), F32),
                       sds((N_LAYERS, 3 * HEADS, D, HD), BF16), sds((N_LAYERS, ATT, D), BF16), sds((N_LAYERS, D, FF), BF16),
                       sds((N_LAYERS, FF), F32), sds((N_LAYERS, FF, D), BF16)),
            in_specs=[vmem] * 4 + [hbm] * 8,
            out_specs=(vmem, vmem, vmem, vmem, hbm, hbm, hbm, vmem, hbm),
            scratch_shapes=[
                pltpu.VMEM(flat, BF16), pltpu.VMEM(flat, BF16), pltpu.VMEM(flat, BF16), pltpu.VMEM(flat, BF16),
                pltpu.VMEM((N_LAYERS, SEQ, ATT), BF16), pltpu.VMEM((N_LAYERS, SEQ, FF), BF16), pltpu.VMEM((N_LAYERS, SEQ, FF), BF16),
                pltpu.VMEM((N_LAYERS, SEQ, QKV), BF16),
                pltpu.VMEM((3, C, D), BF16), pltpu.VMEM((3, 3 * HEADS, C, HD), BF16), pltpu.VMEM((2, ATT // 2, D), BF16),
                dma((8, N_LAYERS)), dma((3,)), dma((3,)), dma((2,)),
            ],
            compiler_params=pltpu.CompilerParams(vmem_limit_bytes=VMEM_ALL),
        )(y_loc, xg_loc, small, bupg, h.reshape(flat), h2.reshape(flat), dm.reshape(flat), da.reshape(flat), attn, act, dpre, dqkv)
        wqkv_g = jnp.transpose(wqkv_g.reshape(N_LAYERS, 3, HEADS, D, HD), (0, 3, 1, 2, 4))
        return (y_out[None], x_grad[None], lng, biasg, wqkv_g, wo_g.reshape(N_LAYERS, HEADS, HD, D), wu_g, bupg_o, wd_g)

    in_specs = (P('dp', 'tp', None), P('dp', 'tp', None), P(None, None, None), P(None, None, None),
                P(None, None, None, 'tp', None), P(None, 'tp', None, None), P(None, None, 'tp'), P(None, 'tp'), P(None, 'tp', None))
    out_specs = (P('dp', 'tp', None), P('dp', 'tp', None), P('dp', None, None), P('dp', None, None),
                 P('dp', None, None, 'tp', None), P('dp', 'tp', None, None), P('dp', None, 'tp'), P('dp', 'tp'), P('dp', 'tp', None))
    return jax.shard_map(device_step, mesh=mesh, in_specs=in_specs, out_specs=out_specs, check_vma=False)
```

```python
import jax
import jax.numpy as jnp
from jax import lax
from jax.experimental import pallas as pl
from jax.experimental.pallas import tpu as pltpu
from jax.sharding import PartitionSpec as P

MESH = pl.DeviceIdType.MESH
F32, BF16 = jnp.float32, jnp.bfloat16
N_LAYERS, SEQ, BLK, D, HEADS, HD, FF = 2, 128, 32, 2560, 5, 128, 2560
ATT = HEADS * HD
QKV = 3 * ATT
C = 512
NC = D // C
SCALE = HD ** -0.5
GELU_K = 0.7978845608028654
GELU_C = 0.044715
VMEM_ALL = 67043328


def mm(a, b):
    return jnp.dot(a, b, preferred_element_type=F32)


def mm_nt(a, b):
    return lax.dot_general(a, b, (((1,), (1,)), ((), ())), preferred_element_type=F32)


def mm_tn(a, b):
    return mm(a.T, b)


def chunk(c, size=C):
    return pl.ds(pl.multiple_of(c * size, size), size)


def chain_kernel(x_ref, dy_ref, ln_ref, bias_ref, bup_ref, wqkv_h, wo_h, wu_h, wd_h,
                 y_ref, xg_ref, small_ref, bupg_ref, h_o, h2_o, dm_o, da_o, a_o, act_o, dpre_o, dqkv_o,
                 wq, wo, wu, wd, h_g, h2_g, dm_g, da_g, qkv, prob, attn, act, gp, dpre, dqkv,
                 xh1, xh2, rs1, rs2, res, dres, acc, acct, part, own, rr, xx, ss, sg, sgr,
                 wsem, osem, agsem, rssem, gsem):
    me = lax.axis_index('tp')
    x_id = lax.div(me, 2)
    core = lax.rem(me, 2)
    sib = x_id * 2 + (1 - core)
    cross = (1 - x_id) * 2 + core
    diag = (1 - x_id) * 2 + (1 - core)

    def remote(src, dst, send, recv, dev):
        return pltpu.make_async_remote_copy(src_ref=src, dst_ref=dst, send_sem=send, recv_sem=recv,
                                            device_id={'tp': dev}, device_id_type=MESH)

    def weight_copies(kind, layer):
        if kind == 0:
            return [pltpu.make_async_copy(wqkv_h.at[layer, j], wq.at[:, pl.ds(j * HD, HD)], wsem.at[0, j]) for j in range(3 * HEADS)]
        if kind == 1:
            return [pltpu.make_async_copy(wo_h.at[layer], wo, wsem.at[1, 0])]
        src, dst = ((wu_h, wu), (wd_h, wd))[kind - 2]
        return [pltpu.make_async_copy(src.at[layer, pl.ds(j * C, C)], dst.at[pl.ds(j * C, C)], wsem.at[kind, j]) for j in range(NC)]

    def load_w(kind, layer):
        for copy in weight_copies(kind, layer):
            copy.start()

    def wait_w(kind, layer):
        for copy in weight_copies(kind, layer):
            copy.wait()

    def out_copy(i, src, dst, layer):
        return pltpu.make_async_copy(src.at[layer], dst.at[layer], osem.at[i, layer])

    outs = [(h_g, h_o), (h2_g, h2_o), (dm_g, dm_o), (da_g, da_o), (attn, a_o), (act, act_o), (dpre, dpre_o), (dqkv, dqkv_o)]

    def ag_side(g, layer, c, k=0):
        mine = g.at[layer, me, :, chunk(c)]
        return remote(mine, mine, agsem.at[k, 0, c], agsem.at[k, 1, c], sib)

    def ag_across(g, layer, c, k=0):
        mine = g.at[layer, me, :, chunk(c)]
        return remote(mine, mine, agsem.at[k, 2, c], agsem.at[k, 3, c], cross)

    def ag_forward(g, layer, c, k=0):
        theirs = g.at[layer, cross, :, chunk(c)]
        return remote(theirs, theirs, agsem.at[k, 4, c], agsem.at[k, 5, c], sib)

    def ag_relay(g, layer, k):
        @pl.loop(0, NC)
        def _(c):
            ag_across(g, layer, c, k).wait_recv()
            ag_forward(g, layer, c, k).start()

    def ag_finish(g, layer, k):
        @pl.loop(0, NC)
        def _(c):
            ag_side(g, layer, c, k).wait()
            ag_forward(g, layer, c, k).wait()
            ag_across(g, layer, c, k).wait_send()

    def ag_start(g, layer, k=0):
        for c in range(NC):
            ag_across(g, layer, c, k).start()
        for c in range(NC):
            ag_side(g, layer, c, k).start()

    def ag_consume(g, layer, compute):
        @pl.loop(0, NC + 1)
        def _(c):
            @pl.when(c < NC)
            def _():
                ag_across(g, layer, c).wait_recv()
                ag_forward(g, layer, c).start()

            @pl.when(c >= 1)
            def _():
                cc = c - 1
                ag_side(g, layer, cc).wait_recv()
                ag_forward(g, layer, cc).wait_recv()
                compute(cc)

        @pl.loop(0, NC)
        def _(c):
            ag_side(g, layer, c).wait_send()
            ag_across(g, layer, c).wait_send()
            ag_forward(g, layer, c).wait_send()

    def rs_side(par, c):
        return remote(part.at[par // 2, :, 1 - core, :, chunk(c)], rr.at[par, :, :, chunk(c)],
                      rssem.at[par, 0, c], rssem.at[par, 1, c], sib)

    def rs_across(par, c):
        return remote(ss.at[par // 2, :, chunk(c)], xx.at[par, :, chunk(c)], rssem.at[par, 2, c], rssem.at[par, 3, c], cross)

    def rs_send(par, compute, lag=2):
        buf = par // 2

        @pl.loop(0, NC + lag)
        def _(c):
            @pl.when(c < NC)
            def _():
                vals = compute(c)
                for b in range(4):
                    part[buf, b // 2, b % 2, :, chunk(c)] = vals[b * BLK:(b + 1) * BLK]
                rs_side(par, c).start()

            @pl.when(c >= lag)
            def _():
                cc = c - lag
                rs_side(par, cc).wait_recv()
                cols = chunk(cc)
                ss[buf, :, cols] = (part[buf, 1 - x_id, core, :, cols] + rr[par, 1 - x_id, :, cols]).astype(BF16)
                rs_across(par, cc).start()
                own[buf, :, cols] = part[buf, x_id, core, :, cols] + rr[par, x_id, :, cols]

    def rs_finish(par):
        @pl.loop(0, NC)
        def _(c):
            rs_across(par, c).wait_recv()
            rs_side(par, c).wait_send()
            rs_across(par, c).wait_send()
            own[par // 2, :, chunk(c)] += xx[par, :, chunk(c)].astype(F32)

    def normed(vals, gain, shift, xh, rs, layer):
        mean_val = jnp.mean(vals, axis=-1, keepdims=True)
        centered = vals - mean_val
        rstd = lax.rsqrt(jnp.mean(centered * centered, axis=-1, keepdims=True) + 1e-5)
        hat = centered * rstd
        xh[layer] = hat
        rs[layer] = jnp.broadcast_to(rstd, (BLK, 128))
        return (hat * gain + shift).astype(BF16)

    def norm_grad(d_out, gain, xh, rs, layer, gain_row):
        hat = xh[layer]
        rstd = rs[layer][:, :1]
        sg[layer, gain_row:gain_row + 1, :] = jnp.sum(d_out * hat, axis=0, keepdims=True)
        sg[layer, gain_row + 1:gain_row + 2, :] = jnp.sum(d_out, axis=0, keepdims=True)
        d_hat = d_out * gain
        m1 = jnp.mean(d_hat, axis=-1, keepdims=True)
        m2 = jnp.mean(d_hat * hat, axis=-1, keepdims=True)
        return rstd * (d_hat - m1 - hat * m2)

    def small_copies(layer):
        return [remote(sg.at[layer], sgr.at[layer, i], gsem.at[layer, 0, i], gsem.at[layer, 1, i], dev)
                for i, dev in enumerate((sib, cross, diag))]

    load_w(0, 0)
    barrier = pltpu.get_barrier_semaphore()
    for dev in (sib, cross, diag):
        pl.semaphore_signal(barrier, inc=1, device_id={'tp': dev}, device_id_type=MESH)
    res[...] = x_ref[0].astype(F32)
    pl.semaphore_wait(barrier, 3)

    row_id = lax.broadcasted_iota(jnp.int32, (SEQ, SEQ), 0)
    col_id = lax.broadcasted_iota(jnp.int32, (SEQ, SEQ), 1)
    causal = row_id >= col_id

    def dact_chunk(c):
        g = dm_g[0, :, :, chunk(c)].reshape(SEQ, C)
        acct[...] += mm_nt(wd[:, chunk(c)], g)

    def dact_early(layer, lo, hi):
        @pl.when(layer == N_LAYERS - 1)
        def _():
            @pl.loop(lo, hi)
            def _(c):
                acct[chunk(c), :] = mm_nt(wd[chunk(c), :], dm_g[N_LAYERS - 1].reshape(SEQ, D))

    @pl.loop(0, N_LAYERS)
    def _(layer):
        first = layer == 0
        last = layer == N_LAYERS - 1
        lnp = ln_ref[layer]
        h_g[layer, me] = normed(res[...], lnp[0:1], lnp[1:2], xh1, rs1, layer)
        ag_start(h_g, layer)
        acc[...] = jnp.zeros_like(acc)
        wait_w(0, layer)

        @pl.when(first)
        def _():
            load_w(1, 0)
            load_w(2, 0)

        def qkv_chunk(c):
            h = h_g[layer, :, :, chunk(c)].reshape(SEQ, C)
            for n in range(0, QKV, 640):
                acc[:, n:n + 640] += mm(h, wq[chunk(c), n:n + 640])
        ag_consume(h_g, layer, qkv_chunk)
        out_copy(0, h_g, h_o, layer).start()

        @pl.when(first)
        def _():
            load_w(0, 1)
            dm_g[N_LAYERS - 1, me] = dy_ref[0]
            ag_start(dm_g, N_LAYERS - 1, 1)

        for j in range(3 * HEADS):
            qkv[layer, :, j * HD:(j + 1) * HD] = acc[:, j * HD:(j + 1) * HD].astype(BF16)
        for hd in range(HEADS):
            q = qkv[layer, :, hd * HD:(hd + 1) * HD]
            k = qkv[layer, :, ATT + hd * HD:ATT + (hd + 1) * HD]
            v = qkv[layer, :, 2 * ATT + hd * HD:2 * ATT + (hd + 1) * HD]
            scores = jnp.where(causal, mm_nt(q, k) * SCALE, -1e30)
            e = jnp.exp(scores - jnp.max(scores, axis=-1, keepdims=True))
            p = (e / jnp.sum(e, axis=-1, keepdims=True)).astype(BF16)
            prob[layer, hd] = p
            attn[layer, :, hd * HD:(hd + 1) * HD] = mm(p, v).astype(BF16)
        out_copy(4, attn, a_o, layer).start()
        wait_w(1, layer)

        @pl.when(first)
        def _():
            load_w(3, 0)
        @pl.when(first)
        def _():
            ag_relay(dm_g, N_LAYERS - 1, 1)

        @pl.when(last)
        def _():
            wait_w(3, N_LAYERS - 1)
        rs_send(0, lambda c: mm(attn[layer], wo[:, chunk(c)]))
        dact_early(layer, 0, 2)
        rs_finish(0)

        @pl.when(first)
        def _():
            load_w(1, 1)
            ag_finish(dm_g, N_LAYERS - 1, 1)
            out_copy(2, dm_g, dm_o, N_LAYERS - 1).start()
        res[...] = res[...] + own[0] + bias_ref[layer, 0:1]

        h2_g[layer, me] = normed(res[...], lnp[2:3], lnp[3:4], xh2, rs2, layer)
        ag_start(h2_g, layer)
        acc[...] = jnp.zeros_like(acc)
        wait_w(2, layer)
        dact_early(layer, 2, NC)

        def up_chunk(c):
            h = h2_g[layer, :, :, chunk(c)].reshape(SEQ, C)
            for n in range(0, FF, C):
                acc[:, n:n + C] += mm(h, wu[chunk(c), n:n + C])
        ag_consume(h2_g, layer, up_chunk)
        out_copy(1, h2_g, h2_o, layer).start()

        @pl.when(first)
        def _():
            load_w(2, 1)

        @pl.loop(0, FF // C)
        def _(c):
            pre = acc[:, chunk(c)] + bup_ref[pl.ds(layer, 1), chunk(c)]
            sq = pre * pre
            t = jnp.tanh(GELU_K * (pre + GELU_C * (sq * pre)))
            cdf = 0.5 * (1.0 + t)
            act[layer, :, chunk(c)] = (pre * cdf).astype(BF16)
            gp[layer, :, chunk(c)] = cdf + 0.5 * pre * (1.0 - t * t) * (GELU_K * (1.0 + 3.0 * GELU_C * sq))
        out_copy(5, act, act_o, layer).start()

        @pl.when(first)
        def _():
            wait_w(3, 0)
            rs_send(1, lambda c: mm(act[0], wd[:, chunk(c)]))
            rs_finish(1)
            load_w(3, 1)
            res[...] = res[...] + own[0] + bias_ref[0, 1:2]

    dres[...] = dy_ref[0].astype(F32)
    sg[...] = jnp.zeros_like(sg)

    @pl.loop(0, N_LAYERS)
    def _(step):
        layer = N_LAYERS - 1 - step
        top = step == 0
        low = step == N_LAYERS - 1
        lnp = ln_ref[layer]
        sg[layer, 5:6, :] = jnp.sum(dres[...], axis=0, keepdims=True)
        @pl.when(low)
        def _():
            dm_g[0, me] = dres[...].astype(BF16)
            ag_start(dm_g, 0)
            acct[...] = jnp.zeros_like(acct)
            wait_w(3, 0)
            ag_consume(dm_g, 0, dact_chunk)
            out_copy(2, dm_g, dm_o, 0).start()

        @pl.loop(0, FF // C)
        def _(c):
            d_pre = acct[chunk(c), :].T * gp[layer, :, chunk(c)]
            bupg_ref[pl.ds(layer, 1), chunk(c)] = jnp.sum(d_pre, axis=0, keepdims=True)
            dpre[layer, :, chunk(c)] = d_pre.astype(BF16)
        out_copy(6, dpre, dpre_o, layer).start()

        @pl.when(low)
        def _():
            wait_w(2, 0)
        rs_send(0, lambda c: mm_nt(wu[chunk(c), :], dpre[layer]).T)

        @pl.when(top)
        def _():
            load_w(2, 0)
            rs_send(2, lambda c: mm(act[N_LAYERS - 1], wd[:, chunk(c)]))
            load_w(3, 0)
        rs_finish(0)
        dres[...] = dres[...] + norm_grad(own[0], lnp[2:3], xh2, rs2, layer, 2)

        sg[layer, 4:5, :] = jnp.sum(dres[...], axis=0, keepdims=True)
        da_g[layer, me] = dres[...].astype(BF16)
        ag_start(da_g, layer)
        acct[0:ATT, :] = jnp.zeros((ATT, SEQ), F32)

        @pl.when(low)
        def _():
            wait_w(1, 0)

        def dattn_chunk(c):
            g = da_g[layer, :, :, chunk(c)].reshape(SEQ, C)
            acct[0:ATT, :] += mm_nt(wo[:, chunk(c)], g)
        ag_consume(da_g, layer, dattn_chunk)
        out_copy(3, da_g, da_o, layer).start()

        @pl.when(top)
        def _():
            load_w(1, 0)
            rs_finish(2)
            y_ref[...] = (res[...] + own[1] + bias_ref[N_LAYERS - 1, 1:2]).astype(BF16)

        @pl.when(low)
        def _():
            for copy in small_copies(N_LAYERS - 1):
                copy.start()

        for hd in range(HEADS):
            q = qkv[layer, :, hd * HD:(hd + 1) * HD]
            k = qkv[layer, :, ATT + hd * HD:ATT + (hd + 1) * HD]
            v = qkv[layer, :, 2 * ATT + hd * HD:2 * ATT + (hd + 1) * HD]
            p = prob[layer, hd]
            d_o = acct[hd * HD:(hd + 1) * HD, :].T.astype(BF16)
            d_p = mm_nt(d_o, v)
            d_v = mm(p.T, d_o)
            pf = p.astype(F32)
            dot = jnp.sum(d_p * pf, axis=-1, keepdims=True)
            d_s = (pf * (d_p - dot) * SCALE).astype(BF16)
            dqkv[layer, :, hd * HD:(hd + 1) * HD] = mm(d_s, k).astype(BF16)
            dqkv[layer, :, ATT + hd * HD:ATT + (hd + 1) * HD] = mm(d_s.T, q).astype(BF16)
            dqkv[layer, :, 2 * ATT + hd * HD:2 * ATT + (hd + 1) * HD] = d_v.astype(BF16)
        out_copy(7, dqkv, dqkv_o, layer).start()

        @pl.when(low)
        def _():
            wait_w(0, 0)
        rs_send(1, lambda c: mm_nt(wq[chunk(c), :], dqkv[layer]).T)
        rs_finish(1)

        @pl.when(top)
        def _():
            load_w(0, 0)
        dres[...] = dres[...] + norm_grad(own[0], lnp[0:1], xh1, rs1, layer, 0)

    for copy in small_copies(0):
        copy.start()
    xg_ref[...] = dres[...].astype(BF16)
    for layer in reversed(range(N_LAYERS)):
        for copy in small_copies(layer):
            copy.wait()
        small_ref[layer] = (sg[layer] + sgr[layer, 0]) + (sgr[layer, 1] + sgr[layer, 2])
    for layer in range(N_LAYERS):
        for i, (src, dst) in enumerate(outs):
            out_copy(i, src, dst, layer).wait()


def grads_kernel(y_in, xg_in, small_in, bupg_in, h_h, h2_h, dm_h, da_h, a_h, act_h, dpre_h, dqkv_h,
                 y_o, xg_o, lng_o, biasg_o, wqkv_o, wo_o, wu_o, bupg_o, wd_o,
                 h, h2, dm, da, attn, act, dpre, dqkv, big, qbuf, obuf, isem, bsem, qsem, osem):
    ins = [(dm_h, dm), (act_h, act), (h2_h, h2), (dpre_h, dpre), (da_h, da), (a_h, attn), (h_h, h), (dqkv_h, dqkv)]

    def in_copy(i, layer):
        return pltpu.make_async_copy(ins[i][0].at[layer], ins[i][1].at[layer], isem.at[i, layer])

    order = [(i, layer) for layer in reversed(range(N_LAYERS)) for i in range(0, len(ins), 2)]

    def prefetch(k):
        if k < len(order):
            in_copy(order[k][0], order[k][1]).start()
            in_copy(order[k][0] + 1, order[k][1]).start()

    prefetch(0)
    prefetch(1)
    y_o[...] = y_in[...]
    xg_o[...] = xg_in[...]
    lng_o[...] = small_in[:, 0:4, :]
    biasg_o[...] = small_in[:, 4:6, :]
    bupg_o[...] = bupg_in[...]

    def big_copy(dst, layer, c, slot):
        return pltpu.make_async_copy(big.at[slot], dst.at[layer, chunk(c)], bsem.at[slot])

    def q_copy(layer, c, slot):
        return pltpu.make_async_copy(qbuf.at[slot], wqkv_o.at[layer, :, chunk(c), :], qsem.at[slot])

    def o_copy(layer, c):
        return pltpu.make_async_copy(obuf.at[c], wo_o.at[layer, pl.ds(c * (ATT // 2), ATT // 2)], osem.at[c])

    for step, layer in enumerate(reversed(range(N_LAYERS))):
        for w, (dst, left, right) in enumerate(((wd_o, act, dm), (wu_o, h2, dpre))):
            in_copy(2 * w, layer).wait()
            in_copy(2 * w + 1, layer).wait()
            prefetch(4 * step + w + 2)
            base = (2 * step + w) * NC

            @pl.loop(0, NC)
            def _(c):
                slot = lax.rem(base + c, 3)

                @pl.when(base + c >= 3)
                def _():
                    big_copy(dst, layer, c, slot).wait()
                lt = left[layer, :, chunk(c)].T
                for n in range(0, D, C):
                    big[slot, :, n:n + C] = mm(lt, right[layer, :, n:n + C]).astype(BF16)
                big_copy(dst, layer, c, slot).start()
        in_copy(4, layer).wait()
        in_copy(5, layer).wait()
        prefetch(4 * step + 4)
        for c in range(2):
            if step > 0:
                o_copy(layer, c).wait()
            lt = attn[layer, :, :].T[c * (ATT // 2):(c + 1) * (ATT // 2)]
            for n in range(0, D, C):
                obuf[c, :, n:n + C] = mm(lt, da[layer, :, n:n + C]).astype(BF16)
            o_copy(layer, c).start()
        in_copy(6, layer).wait()
        in_copy(7, layer).wait()
        prefetch(4 * step + 5)
        qbase = step * NC

        @pl.loop(0, NC)
        def _(c):
            slot = lax.rem(qbase + c, 3)

            @pl.when(qbase + c >= 3)
            def _():
                q_copy(layer, c, slot).wait()
            lt = h[layer, :, chunk(c)].T
            for n in range(0, QKV, 3 * HD):
                vals = mm(lt, dqkv[layer, :, n:n + 3 * HD]).astype(BF16)
                for j in range(3):
                    qbuf[slot, n // HD + j] = vals[:, j * HD:(j + 1) * HD]
            q_copy(layer, c, slot).start()
    for slot in range(3):
        big_copy(wu_o, 0, 0, slot).wait()
        q_copy(0, 0, slot).wait()
    for c in range(2):
        o_copy(0, c).wait()


def solution(mesh):
    vmem = pl.BlockSpec(memory_space=pltpu.VMEM)
    hbm = pl.BlockSpec(memory_space=pl.ANY)

    def device_step(x_loc, dy_loc, ln_par, bias_d, w_qkv, w_out, w_up, b_up, w_down):
        wqkv_t = jnp.transpose(w_qkv, (0, 2, 3, 1, 4)).reshape(N_LAYERS, 3 * HEADS, D, HD)
        wo_t = w_out.reshape(N_LAYERS, ATT, D)
        sds = jax.ShapeDtypeStruct
        gath = (N_LAYERS, 4, BLK, D)
        dma = pltpu.SemaphoreType.DMA
        chain_out = pl.pallas_call(
            chain_kernel,
            name='chain',
            out_shape=(sds((BLK, D), BF16), sds((BLK, D), BF16), sds((N_LAYERS, 8, D), F32), sds((N_LAYERS, FF), F32),
                       sds(gath, BF16), sds(gath, BF16), sds(gath, BF16), sds(gath, BF16),
                       sds((N_LAYERS, SEQ, ATT), BF16), sds((N_LAYERS, SEQ, FF), BF16), sds((N_LAYERS, SEQ, FF), BF16),
                       sds((N_LAYERS, SEQ, QKV), BF16)),
            in_specs=[vmem] * 5 + [hbm] * 4,
            out_specs=tuple([vmem] * 4 + [hbm] * 8),
            scratch_shapes=[
                pltpu.VMEM((D, QKV), BF16), pltpu.VMEM((ATT, D), BF16), pltpu.VMEM((D, FF), BF16), pltpu.VMEM((FF, D), BF16),
                pltpu.VMEM(gath, BF16), pltpu.VMEM(gath, BF16), pltpu.VMEM(gath, BF16), pltpu.VMEM(gath, BF16),
                pltpu.VMEM((N_LAYERS, SEQ, QKV), BF16), pltpu.VMEM((N_LAYERS, HEADS, SEQ, SEQ), BF16),
                pltpu.VMEM((N_LAYERS, SEQ, ATT), BF16), pltpu.VMEM((N_LAYERS, SEQ, FF), BF16), pltpu.VMEM((N_LAYERS, SEQ, FF), F32),
                pltpu.VMEM((N_LAYERS, SEQ, FF), BF16), pltpu.VMEM((N_LAYERS, SEQ, QKV), BF16),
                pltpu.VMEM((N_LAYERS, BLK, D), F32), pltpu.VMEM((N_LAYERS, BLK, D), F32),
                pltpu.VMEM((N_LAYERS, BLK, 128), F32), pltpu.VMEM((N_LAYERS, BLK, 128), F32),
                pltpu.VMEM((BLK, D), F32), pltpu.VMEM((BLK, D), F32), pltpu.VMEM((SEQ, D), F32), pltpu.VMEM((D, SEQ), F32),
                pltpu.VMEM((2, 2, 2, BLK, D), F32), pltpu.VMEM((2, BLK, D), F32), pltpu.VMEM((3, 2, BLK, D), F32),
                pltpu.VMEM((3, BLK, D), BF16), pltpu.VMEM((2, BLK, D), BF16),
                pltpu.VMEM((N_LAYERS, 8, D), F32), pltpu.VMEM((N_LAYERS, 3, 8, D), F32),
                dma((4, 3 * HEADS)), dma((8, N_LAYERS)), dma((2, 6, NC)), dma((3, 4, NC)), dma((N_LAYERS, 2, 3)),
            ],
            compiler_params=pltpu.CompilerParams(collective_id=0, has_side_effects=True, vmem_limit_bytes=VMEM_ALL),
        )(x_loc, dy_loc, ln_par, bias_d, b_up, wqkv_t, wo_t, w_up, w_down)
        y_loc, xg_loc, small, bupg, h, h2, dm, da, attn, act, dpre, dqkv = chain_out
        flat = (N_LAYERS, SEQ, D)
        y_out, x_grad, lng, biasg, wqkv_g, wo_g, wu_g, bupg_o, wd_g = pl.pallas_call(
            grads_kernel,
            name='grads',
            out_shape=(sds((BLK, D), BF16), sds((BLK, D), BF16), sds((N_LAYERS, 4, D), F32), sds((N_LAYERS, 2, D), F32),
                       sds((N_LAYERS, 3 * HEADS, D, HD), BF16), sds((N_LAYERS, ATT, D), BF16), sds((N_LAYERS, D, FF), BF16),
                       sds((N_LAYERS, FF), F32), sds((N_LAYERS, FF, D), BF16)),
            in_specs=[vmem] * 4 + [hbm] * 8,
            out_specs=(vmem, vmem, vmem, vmem, hbm, hbm, hbm, vmem, hbm),
            scratch_shapes=[
                pltpu.VMEM(flat, BF16), pltpu.VMEM(flat, BF16), pltpu.VMEM(flat, BF16), pltpu.VMEM(flat, BF16),
                pltpu.VMEM((N_LAYERS, SEQ, ATT), BF16), pltpu.VMEM((N_LAYERS, SEQ, FF), BF16), pltpu.VMEM((N_LAYERS, SEQ, FF), BF16),
                pltpu.VMEM((N_LAYERS, SEQ, QKV), BF16),
                pltpu.VMEM((3, C, D), BF16), pltpu.VMEM((3, 3 * HEADS, C, HD), BF16), pltpu.VMEM((2, ATT // 2, D), BF16),
                dma((8, N_LAYERS)), dma((3,)), dma((3,)), dma((2,)),
            ],
            compiler_params=pltpu.CompilerParams(vmem_limit_bytes=VMEM_ALL),
        )(y_loc, xg_loc, small, bupg, h.reshape(flat), h2.reshape(flat), dm.reshape(flat), da.reshape(flat), attn, act, dpre, dqkv)
        wqkv_g = jnp.transpose(wqkv_g.reshape(N_LAYERS, 3, HEADS, D, HD), (0, 3, 1, 2, 4))
        return (y_out[None], x_grad[None], lng, biasg, wqkv_g, wo_g.reshape(N_LAYERS, HEADS, HD, D), wu_g, bupg_o, wd_g)

    in_specs = (P('dp', 'tp', None), P('dp', 'tp', None), P(None, None, None), P(None, None, None),
                P(None, None, None, 'tp', None), P(None, 'tp', None, None), P(None, None, 'tp'), P(None, 'tp'), P(None, 'tp', None))
    out_specs = (P('dp', 'tp', None), P('dp', 'tp', None), P('dp', None, None), P('dp', None, None),
                 P('dp', None, None, 'tp', None), P('dp', 'tp', None, None), P('dp', None, 'tp'), P('dp', 'tp'), P('dp', 'tp', None))
    return jax.shard_map(device_step, mesh=mesh, in_specs=in_specs, out_specs=out_specs, check_vma=False)
```

```python
import jax
import jax.numpy as jnp
from jax import lax
from jax.experimental import pallas as pl
from jax.experimental.pallas import tpu as pltpu
from jax.sharding import PartitionSpec as P

MESH = pl.DeviceIdType.MESH
F32, BF16 = jnp.float32, jnp.bfloat16
N_LAYERS, SEQ, BLK, D, HEADS, HD, FF = 2, 128, 32, 2560, 5, 128, 2560
ATT = HEADS * HD
QKV = 3 * ATT
C = 512
NC = D // C
SLOTS = 4
SCALE = HD ** -0.5
GELU_K = 0.7978845608028654
GELU_C = 0.044715
VMEM_ALL = 67043328


def mm(a, b):
    return jnp.dot(a, b, preferred_element_type=F32)


def mm_nt(a, b):
    return lax.dot_general(a, b, (((1,), (1,)), ((), ())), preferred_element_type=F32)


def mm_tn(a, b):
    return mm(a.T, b)


def chunk(c, size=C):
    return pl.ds(pl.multiple_of(c * size, size), size)


def chain_kernel(x_ref, dy_ref, ln_ref, bias_ref, bup_ref, wqkv_h, wo_h, wu_h, wd_h,
                 y_ref, xg_ref, small1_ref, small2_ref, bupg_ref, h_o, h2_o, dm_o, da_o, a_o, act_o, dpre_o, dqkv_o,
                 wq, wo, wu, wd, h_g, h2_g, dm_g, da_g, qkv, prob, attn, act, gp, dpre, dqkv,
                 xh1, xh2, rs1, rs2, res, dres, acc, acct, part, own, rr, xx, ss, sg1, sg2, sgr1, sgr2,
                 wsem, osem, agsem, rssem, gsem):
    me = lax.axis_index('tp')
    x_id = lax.div(me, 2)
    core = lax.rem(me, 2)
    sib = x_id * 2 + (1 - core)
    cross = (1 - x_id) * 2 + core
    diag = (1 - x_id) * 2 + (1 - core)

    def remote(src, dst, send, recv, dev):
        return pltpu.make_async_remote_copy(src_ref=src, dst_ref=dst, send_sem=send, recv_sem=recv,
                                            device_id={'tp': dev}, device_id_type=MESH)

    def weight_copies(kind, layer):
        if kind == 0:
            return [pltpu.make_async_copy(wqkv_h.at[layer, j], wq.at[:, pl.ds(j * HD, HD)], wsem.at[0, j]) for j in range(3 * HEADS)]
        if kind == 1:
            return [pltpu.make_async_copy(wo_h.at[layer], wo, wsem.at[1, 0])]
        src, dst = ((wu_h, wu), (wd_h, wd))[kind - 2]
        return [pltpu.make_async_copy(src.at[layer, pl.ds(j * C, C)], dst.at[pl.ds(j * C, C)], wsem.at[kind, j]) for j in range(NC)]

    def load_w(kind, layer):
        for copy in weight_copies(kind, layer):
            copy.start()

    def wait_w(kind, layer):
        for copy in weight_copies(kind, layer):
            copy.wait()

    def out_copy(i, src, dst, layer):
        return pltpu.make_async_copy(src.at[layer], dst.at[layer], osem.at[i, layer])

    outs = [(h_g, h_o), (h2_g, h2_o), (dm_g, dm_o), (da_g, da_o), (attn, a_o), (act, act_o), (dpre, dpre_o), (dqkv, dqkv_o)]

    def ag_side(g, layer, c, k=0):
        mine = g.at[layer, me, :, chunk(c)]
        return remote(mine, mine, agsem.at[k, 0, c], agsem.at[k, 1, c], sib)

    def ag_across(g, layer, c, k=0):
        mine = g.at[layer, me, :, chunk(c)]
        return remote(mine, mine, agsem.at[k, 2, c], agsem.at[k, 3, c], cross)

    def ag_forward(g, layer, c, k=0):
        theirs = g.at[layer, cross, :, chunk(c)]
        return remote(theirs, theirs, agsem.at[k, 4, c], agsem.at[k, 5, c], sib)

    def ag_relay(g, layer, k):
        @pl.loop(0, NC)
        def _(c):
            ag_across(g, layer, c, k).wait_recv()
            ag_forward(g, layer, c, k).start()

    def ag_finish(g, layer, k):
        @pl.loop(0, NC)
        def _(c):
            ag_side(g, layer, c, k).wait()
            ag_forward(g, layer, c, k).wait()
            ag_across(g, layer, c, k).wait_send()

    def ag_start(g, layer, k=0):
        for c in range(NC):
            ag_across(g, layer, c, k).start()
        for c in range(NC):
            ag_side(g, layer, c, k).start()

    def ag_consume(g, layer, compute, lag=2):
        @pl.loop(0, NC + lag)
        def _(c):
            @pl.when(c < NC)
            def _():
                ag_across(g, layer, c).wait_recv()
                ag_forward(g, layer, c).start()

            @pl.when(c >= lag)
            def _():
                cc = c - lag
                ag_side(g, layer, cc).wait_recv()
                ag_forward(g, layer, cc).wait_recv()
                compute(cc)

        @pl.loop(0, NC)
        def _(c):
            ag_side(g, layer, c).wait_send()
            ag_across(g, layer, c).wait_send()
            ag_forward(g, layer, c).wait_send()

    def rs_side(par, c):
        return remote(part.at[par // 2, :, 1 - core, :, chunk(c)], rr.at[par, :, :, chunk(c)],
                      rssem.at[par, 0, c], rssem.at[par, 1, c], sib)

    def rs_across(par, c):
        return remote(ss.at[par // 2, :, chunk(c)], xx.at[par, :, chunk(c)], rssem.at[par, 2, c], rssem.at[par, 3, c], cross)

    def rs_send(par, compute, lag=2):
        buf = par // 2

        @pl.loop(0, NC + lag)
        def _(c):
            @pl.when(c < NC)
            def _():
                vals = compute(c)
                for b in range(4):
                    part[buf, b // 2, b % 2, :, chunk(c)] = vals[b * BLK:(b + 1) * BLK]
                rs_side(par, c).start()

            @pl.when(c >= lag)
            def _():
                cc = c - lag
                rs_side(par, cc).wait_recv()
                cols = chunk(cc)
                ss[buf, :, cols] = (part[buf, 1 - x_id, core, :, cols] + rr[par, 1 - x_id, :, cols]).astype(BF16)
                rs_across(par, cc).start()
                own[buf, :, cols] = part[buf, x_id, core, :, cols] + rr[par, x_id, :, cols]

    def rs_finish(par):
        @pl.loop(0, NC)
        def _(c):
            rs_across(par, c).wait_recv()
            rs_side(par, c).wait_send()
            rs_across(par, c).wait_send()
            own[par // 2, :, chunk(c)] += xx[par, :, chunk(c)].astype(F32)

    def normed(vals, gain, shift, xh, rs, layer):
        mean_val = jnp.mean(vals, axis=-1, keepdims=True)
        centered = vals - mean_val
        rstd = lax.rsqrt(jnp.mean(centered * centered, axis=-1, keepdims=True) + 1e-5)
        hat = centered * rstd
        xh[layer] = hat
        rs[layer] = jnp.broadcast_to(rstd, (BLK, 128))
        return (hat * gain + shift).astype(BF16)

    def norm_grad(d_out, gain, xh, rs, layer, rows):
        hat = xh[layer]
        rstd = rs[layer][:, :1]
        rows[layer, 0:1, :] = jnp.sum(d_out * hat, axis=0, keepdims=True)
        rows[layer, 1:2, :] = jnp.sum(d_out, axis=0, keepdims=True)
        d_hat = d_out * gain
        m1 = jnp.mean(d_hat, axis=-1, keepdims=True)
        m2 = jnp.mean(d_hat * hat, axis=-1, keepdims=True)
        return rstd * (d_hat - m1 - hat * m2)

    def small_copies(kind, layer):
        src, dst = ((sg1, sgr1), (sg2, sgr2))[kind]
        return [remote(src.at[layer], dst.at[layer, i], gsem.at[kind, layer, 0, i], gsem.at[kind, layer, 1, i], dev)
                for i, dev in enumerate((sib, cross, diag))]

    def small_start(kind, layer):
        for copy in small_copies(kind, layer):
            copy.start()

    load_w(0, 0)
    barrier = pltpu.get_barrier_semaphore()
    for dev in (sib, cross, diag):
        pl.semaphore_signal(barrier, inc=1, device_id={'tp': dev}, device_id_type=MESH)
    res[...] = x_ref[0].astype(F32)
    pl.semaphore_wait(barrier, 3)

    row_id = lax.broadcasted_iota(jnp.int32, (SEQ, SEQ), 0)
    col_id = lax.broadcasted_iota(jnp.int32, (SEQ, SEQ), 1)
    causal = row_id >= col_id

    def dact_chunk(c):
        g = dm_g[0, :, :, chunk(c)].reshape(SEQ, C)
        acct[...] += mm_nt(wd[:, chunk(c)], g)

    def dact_early(layer, lo, hi):
        @pl.when(layer == N_LAYERS - 1)
        def _():
            @pl.loop(lo, hi)
            def _(c):
                acct[chunk(c), :] = mm_nt(wd[chunk(c), :], dm_g[N_LAYERS - 1].reshape(SEQ, D))

    @pl.loop(0, N_LAYERS)
    def _(layer):
        first = layer == 0
        last = layer == N_LAYERS - 1
        lnp = ln_ref[layer]
        h_g[layer, me] = normed(res[...], lnp[0:1], lnp[1:2], xh1, rs1, layer)
        ag_start(h_g, layer)
        acc[...] = jnp.zeros_like(acc)
        wait_w(0, layer)

        @pl.when(first)
        def _():
            load_w(1, 0)
            load_w(2, 0)

        def qkv_chunk(c):
            h = h_g[layer, :, :, chunk(c)].reshape(SEQ, C)
            for n in range(0, QKV, 640):
                acc[:, n:n + 640] += mm(h, wq[chunk(c), n:n + 640])
        ag_consume(h_g, layer, qkv_chunk)
        out_copy(0, h_g, h_o, layer).start()

        @pl.when(first)
        def _():
            load_w(0, 1)
            dm_g[N_LAYERS - 1, me] = dy_ref[0]
            ag_start(dm_g, N_LAYERS - 1, 1)

        for j in range(3 * HEADS):
            qkv[layer, :, j * HD:(j + 1) * HD] = acc[:, j * HD:(j + 1) * HD].astype(BF16)
        for hd in range(HEADS):
            q = qkv[layer, :, hd * HD:(hd + 1) * HD]
            k = qkv[layer, :, ATT + hd * HD:ATT + (hd + 1) * HD]
            v = qkv[layer, :, 2 * ATT + hd * HD:2 * ATT + (hd + 1) * HD]
            scores = jnp.where(causal, mm_nt(q, k) * SCALE, -1e30)
            e = jnp.exp(scores - jnp.max(scores, axis=-1, keepdims=True))
            p = (e / jnp.sum(e, axis=-1, keepdims=True)).astype(BF16)
            prob[layer, hd] = p
            attn[layer, :, hd * HD:(hd + 1) * HD] = mm(p, v).astype(BF16)
        out_copy(4, attn, a_o, layer).start()
        wait_w(1, layer)

        @pl.when(first)
        def _():
            load_w(3, 0)
        @pl.when(last)
        def _():
            wait_w(3, N_LAYERS - 1)
        rs_send(0, lambda c: mm(attn[layer], wo[:, chunk(c)]))
        dact_early(layer, 0, 2)

        @pl.when(first)
        def _():
            ag_relay(dm_g, N_LAYERS - 1, 1)
        rs_finish(0)

        @pl.when(first)
        def _():
            load_w(1, 1)
            ag_finish(dm_g, N_LAYERS - 1, 1)
            out_copy(2, dm_g, dm_o, N_LAYERS - 1).start()
        res[...] = res[...] + own[0] + bias_ref[layer, 0:1]

        h2_g[layer, me] = normed(res[...], lnp[2:3], lnp[3:4], xh2, rs2, layer)
        ag_start(h2_g, layer)
        acc[...] = jnp.zeros_like(acc)
        wait_w(2, layer)
        dact_early(layer, 2, NC)

        def up_chunk(c):
            h = h2_g[layer, :, :, chunk(c)].reshape(SEQ, C)
            for n in range(0, FF, C):
                acc[:, n:n + C] += mm(h, wu[chunk(c), n:n + C])
        ag_consume(h2_g, layer, up_chunk)
        out_copy(1, h2_g, h2_o, layer).start()

        @pl.when(first)
        def _():
            load_w(2, 1)

        @pl.loop(0, FF // C)
        def _(c):
            pre = acc[:, chunk(c)] + bup_ref[pl.ds(layer, 1), chunk(c)]
            sq = pre * pre
            t = jnp.tanh(GELU_K * (pre + GELU_C * (sq * pre)))
            cdf = 0.5 * (1.0 + t)
            act[layer, :, chunk(c)] = (pre * cdf).astype(BF16)
            gp[layer, :, chunk(c)] = cdf + 0.5 * pre * (1.0 - t * t) * (GELU_K * (1.0 + 3.0 * GELU_C * sq))
        out_copy(5, act, act_o, layer).start()

        @pl.when(first)
        def _():
            wait_w(3, 0)
            rs_send(1, lambda c: mm(act[0], wd[:, chunk(c)]))
            rs_finish(1)
            load_w(3, 1)
            res[...] = res[...] + own[0] + bias_ref[0, 1:2]

    dres[...] = dy_ref[0].astype(F32)

    @pl.loop(0, N_LAYERS)
    def _(step):
        layer = N_LAYERS - 1 - step
        top = step == 0
        low = step == N_LAYERS - 1
        lnp = ln_ref[layer]
        sg2[layer, 3:4, :] = jnp.sum(dres[...], axis=0, keepdims=True)
        @pl.when(low)
        def _():
            dm_g[0, me] = dres[...].astype(BF16)
            ag_start(dm_g, 0)
            acct[...] = jnp.zeros_like(acct)
            wait_w(3, 0)
            ag_consume(dm_g, 0, dact_chunk)
            out_copy(2, dm_g, dm_o, 0).start()

        @pl.loop(0, FF // C)
        def _(c):
            d_pre = acct[chunk(c), :].T * gp[layer, :, chunk(c)]
            bupg_ref[pl.ds(layer, 1), chunk(c)] = jnp.sum(d_pre, axis=0, keepdims=True)
            dpre[layer, :, chunk(c)] = d_pre.astype(BF16)
        out_copy(6, dpre, dpre_o, layer).start()

        @pl.when(low)
        def _():
            small_start(0, N_LAYERS - 1)
            small_start(1, N_LAYERS - 1)
            wait_w(2, 0)
        rs_send(0, lambda c: mm_nt(wu[chunk(c), :], dpre[layer]).T)

        @pl.when(top)
        def _():
            load_w(2, 0)
            rs_send(2, lambda c: mm(act[N_LAYERS - 1], wd[:, chunk(c)]))
            load_w(3, 0)
        rs_finish(0)
        dres[...] = dres[...] + norm_grad(own[0], lnp[2:3], xh2, rs2, layer, sg2)

        sg2[layer, 2:3, :] = jnp.sum(dres[...], axis=0, keepdims=True)
        da_g[layer, me] = dres[...].astype(BF16)
        ag_start(da_g, layer)
        acct[0:ATT, :] = jnp.zeros((ATT, SEQ), F32)

        @pl.when(low)
        def _():
            wait_w(1, 0)

        def dattn_chunk(c):
            g = da_g[layer, :, :, chunk(c)].reshape(SEQ, C)
            acct[0:ATT, :] += mm_nt(wo[:, chunk(c)], g)
        ag_consume(da_g, layer, dattn_chunk)
        out_copy(3, da_g, da_o, layer).start()

        @pl.when(top)
        def _():
            load_w(1, 0)
            rs_finish(2)
            y_ref[...] = (res[...] + own[1] + bias_ref[N_LAYERS - 1, 1:2]).astype(BF16)

        @pl.when(low)
        def _():
            small_start(1, 0)

        for hd in range(HEADS):
            q = qkv[layer, :, hd * HD:(hd + 1) * HD]
            k = qkv[layer, :, ATT + hd * HD:ATT + (hd + 1) * HD]
            v = qkv[layer, :, 2 * ATT + hd * HD:2 * ATT + (hd + 1) * HD]
            p = prob[layer, hd]
            d_o = acct[hd * HD:(hd + 1) * HD, :].T.astype(BF16)
            d_p = mm_nt(d_o, v)
            d_v = mm(p.T, d_o)
            pf = p.astype(F32)
            dot = jnp.sum(d_p * pf, axis=-1, keepdims=True)
            d_s = (pf * (d_p - dot) * SCALE).astype(BF16)
            dqkv[layer, :, hd * HD:(hd + 1) * HD] = mm(d_s, k).astype(BF16)
            dqkv[layer, :, ATT + hd * HD:ATT + (hd + 1) * HD] = mm(d_s.T, q).astype(BF16)
            dqkv[layer, :, 2 * ATT + hd * HD:2 * ATT + (hd + 1) * HD] = d_v.astype(BF16)
        out_copy(7, dqkv, dqkv_o, layer).start()

        @pl.when(low)
        def _():
            wait_w(0, 0)
        rs_send(1, lambda c: mm_nt(wq[chunk(c), :], dqkv[layer]).T)
        rs_finish(1)

        @pl.when(top)
        def _():
            load_w(0, 0)
        dres[...] = dres[...] + norm_grad(own[0], lnp[0:1], xh1, rs1, layer, sg1)

    small_start(0, 0)
    xg_ref[...] = dres[...].astype(BF16)
    for kind, layer in ((0, 1), (1, 1), (1, 0), (0, 0)):
        src, dst, out = ((sg1, sgr1, small1_ref), (sg2, sgr2, small2_ref))[kind]
        for copy in small_copies(kind, layer):
            copy.wait()
        out[layer] = (src[layer] + dst[layer, 0]) + (dst[layer, 1] + dst[layer, 2])
    for layer in range(N_LAYERS):
        for i, (src, dst) in enumerate(outs):
            out_copy(i, src, dst, layer).wait()


def grads_kernel(y_in, xg_in, small1_in, small2_in, bupg_in, h_h, h2_h, dm_h, da_h, a_h, act_h, dpre_h, dqkv_h,
                 y_o, xg_o, lng_o, biasg_o, wqkv_o, wo_o, wu_o, bupg_o, wd_o,
                 h, h2, dm, da, attn, act, dpre, dqkv, big, qbuf, obuf, isem, bsem, qsem, osem):
    ins = [(dm_h, dm), (act_h, act), (h2_h, h2), (dpre_h, dpre), (da_h, da), (a_h, attn), (h_h, h), (dqkv_h, dqkv)]

    def in_copy(i, layer):
        return pltpu.make_async_copy(ins[i][0].at[layer], ins[i][1].at[layer], isem.at[i, layer])

    order = [(i, layer) for layer in reversed(range(N_LAYERS)) for i in range(0, len(ins), 2)]

    def prefetch(k):
        if k < len(order):
            in_copy(order[k][0], order[k][1]).start()
            in_copy(order[k][0] + 1, order[k][1]).start()

    prefetch(0)
    prefetch(1)
    y_o[...] = y_in[...]
    xg_o[...] = xg_in[...]
    lng_o[:, 0:2, :] = small1_in[...]
    lng_o[:, 2:4, :] = small2_in[:, 0:2, :]
    biasg_o[...] = small2_in[:, 2:4, :]
    bupg_o[...] = bupg_in[...]

    def big_copies(dst, layer, c, slot):
        return [pltpu.make_async_copy(big.at[slot, pl.ds(r * 128, 128)], dst.at[layer, pl.ds(pl.multiple_of(c * C + r * 128, 128), 128)],
                                      bsem.at[slot, r]) for r in range(C // 128)]

    def q_copies(layer, c, slot):
        return [pltpu.make_async_copy(qbuf.at[slot, pl.ds(3 * j, 3)], wqkv_o.at[layer, pl.ds(3 * j, 3), chunk(c), :], qsem.at[slot, j])
                for j in range(HEADS)]

    def o_copies(layer, c):
        return [pltpu.make_async_copy(obuf.at[c, pl.ds(r * 160, 160)], wo_o.at[layer, pl.ds(c * (ATT // 2) + r * 160, 160)], osem.at[c, r])
                for r in range(2)]

    def start(copies):
        for copy in copies:
            copy.start()

    def wait(copies):
        for copy in copies:
            copy.wait()

    for step, layer in enumerate(reversed(range(N_LAYERS))):
        for w, (dst, left, right) in enumerate(((wd_o, act, dm), (wu_o, h2, dpre))):
            in_copy(2 * w, layer).wait()
            in_copy(2 * w + 1, layer).wait()
            prefetch(4 * step + w + 2)
            base = (2 * step + w) * NC

            @pl.loop(0, NC)
            def _(c):
                slot = lax.rem(base + c, SLOTS)

                @pl.when(base + c >= SLOTS)
                def _():
                    wait(big_copies(dst, layer, c, slot))
                lt = left[layer, :, chunk(c)].T
                for n in range(0, D, C):
                    big[slot, :, n:n + C] = mm(lt, right[layer, :, n:n + C]).astype(BF16)
                start(big_copies(dst, layer, c, slot))
        in_copy(4, layer).wait()
        in_copy(5, layer).wait()
        prefetch(4 * step + 4)
        for c in range(2):
            if step > 0:
                wait(o_copies(layer, c))
            lt = attn[layer, :, :].T[c * (ATT // 2):(c + 1) * (ATT // 2)]
            for n in range(0, D, C):
                obuf[c, :, n:n + C] = mm(lt, da[layer, :, n:n + C]).astype(BF16)
            start(o_copies(layer, c))
        in_copy(6, layer).wait()
        in_copy(7, layer).wait()
        prefetch(4 * step + 5)
        qbase = step * NC

        @pl.loop(0, NC)
        def _(c):
            slot = lax.rem(qbase + c, 3)

            @pl.when(qbase + c >= 3)
            def _():
                wait(q_copies(layer, c, slot))
            lt = h[layer, :, chunk(c)].T
            for n in range(0, QKV, 3 * HD):
                vals = mm(lt, dqkv[layer, :, n:n + 3 * HD]).astype(BF16)
                for j in range(3):
                    qbuf[slot, n // HD + j] = vals[:, j * HD:(j + 1) * HD]
            start(q_copies(layer, c, slot))
    for slot in range(SLOTS):
        wait(big_copies(wu_o, 0, 0, slot))
    for slot in range(3):
        wait(q_copies(0, 0, slot))
    for c in range(2):
        wait(o_copies(0, c))


def solution(mesh):
    vmem = pl.BlockSpec(memory_space=pltpu.VMEM)
    hbm = pl.BlockSpec(memory_space=pl.ANY)

    def device_step(x_loc, dy_loc, ln_par, bias_d, w_qkv, w_out, w_up, b_up, w_down):
        wqkv_t = jnp.transpose(w_qkv, (0, 2, 3, 1, 4)).reshape(N_LAYERS, 3 * HEADS, D, HD)
        wo_t = w_out.reshape(N_LAYERS, ATT, D)
        sds = jax.ShapeDtypeStruct
        gath = (N_LAYERS, 4, BLK, D)
        dma = pltpu.SemaphoreType.DMA
        chain_out = pl.pallas_call(
            chain_kernel,
            name='chain',
            out_shape=(sds((BLK, D), BF16), sds((BLK, D), BF16), sds((N_LAYERS, 2, D), F32), sds((N_LAYERS, 4, D), F32), sds((N_LAYERS, FF), F32),
                       sds(gath, BF16), sds(gath, BF16), sds(gath, BF16), sds(gath, BF16),
                       sds((N_LAYERS, SEQ, ATT), BF16), sds((N_LAYERS, SEQ, FF), BF16), sds((N_LAYERS, SEQ, FF), BF16),
                       sds((N_LAYERS, SEQ, QKV), BF16)),
            in_specs=[vmem] * 5 + [hbm] * 4,
            out_specs=tuple([vmem] * 5 + [hbm] * 8),
            scratch_shapes=[
                pltpu.VMEM((D, QKV), BF16), pltpu.VMEM((ATT, D), BF16), pltpu.VMEM((D, FF), BF16), pltpu.VMEM((FF, D), BF16),
                pltpu.VMEM(gath, BF16), pltpu.VMEM(gath, BF16), pltpu.VMEM(gath, BF16), pltpu.VMEM(gath, BF16),
                pltpu.VMEM((N_LAYERS, SEQ, QKV), BF16), pltpu.VMEM((N_LAYERS, HEADS, SEQ, SEQ), BF16),
                pltpu.VMEM((N_LAYERS, SEQ, ATT), BF16), pltpu.VMEM((N_LAYERS, SEQ, FF), BF16), pltpu.VMEM((N_LAYERS, SEQ, FF), F32),
                pltpu.VMEM((N_LAYERS, SEQ, FF), BF16), pltpu.VMEM((N_LAYERS, SEQ, QKV), BF16),
                pltpu.VMEM((N_LAYERS, BLK, D), F32), pltpu.VMEM((N_LAYERS, BLK, D), F32),
                pltpu.VMEM((N_LAYERS, BLK, 128), F32), pltpu.VMEM((N_LAYERS, BLK, 128), F32),
                pltpu.VMEM((BLK, D), F32), pltpu.VMEM((BLK, D), F32), pltpu.VMEM((SEQ, D), F32), pltpu.VMEM((D, SEQ), F32),
                pltpu.VMEM((2, 2, 2, BLK, D), F32), pltpu.VMEM((2, BLK, D), F32), pltpu.VMEM((3, 2, BLK, D), F32),
                pltpu.VMEM((3, BLK, D), BF16), pltpu.VMEM((2, BLK, D), BF16),
                pltpu.VMEM((N_LAYERS, 2, D), F32), pltpu.VMEM((N_LAYERS, 4, D), F32), pltpu.VMEM((N_LAYERS, 3, 2, D), F32), pltpu.VMEM((N_LAYERS, 3, 4, D), F32),
                dma((4, 3 * HEADS)), dma((8, N_LAYERS)), dma((2, 6, NC)), dma((3, 4, NC)), dma((2, N_LAYERS, 2, 3)),
            ],
            compiler_params=pltpu.CompilerParams(collective_id=0, has_side_effects=True, vmem_limit_bytes=VMEM_ALL),
        )(x_loc, dy_loc, ln_par, bias_d, b_up, wqkv_t, wo_t, w_up, w_down)
        y_loc, xg_loc, small1, small2, bupg, h, h2, dm, da, attn, act, dpre, dqkv = chain_out
        flat = (N_LAYERS, SEQ, D)
        y_out, x_grad, lng, biasg, wqkv_g, wo_g, wu_g, bupg_o, wd_g = pl.pallas_call(
            grads_kernel,
            name='grads',
            out_shape=(sds((BLK, D), BF16), sds((BLK, D), BF16), sds((N_LAYERS, 4, D), F32), sds((N_LAYERS, 2, D), F32),
                       sds((N_LAYERS, 3 * HEADS, D, HD), BF16), sds((N_LAYERS, ATT, D), BF16), sds((N_LAYERS, D, FF), BF16),
                       sds((N_LAYERS, FF), F32), sds((N_LAYERS, FF, D), BF16)),
            in_specs=[vmem] * 5 + [hbm] * 8,
            out_specs=(vmem, vmem, vmem, vmem, hbm, hbm, hbm, vmem, hbm),
            scratch_shapes=[
                pltpu.VMEM(flat, BF16), pltpu.VMEM(flat, BF16), pltpu.VMEM(flat, BF16), pltpu.VMEM(flat, BF16),
                pltpu.VMEM((N_LAYERS, SEQ, ATT), BF16), pltpu.VMEM((N_LAYERS, SEQ, FF), BF16), pltpu.VMEM((N_LAYERS, SEQ, FF), BF16),
                pltpu.VMEM((N_LAYERS, SEQ, QKV), BF16),
                pltpu.VMEM((SLOTS, C, D), BF16), pltpu.VMEM((3, 3 * HEADS, C, HD), BF16), pltpu.VMEM((2, ATT // 2, D), BF16),
                dma((8, N_LAYERS)), dma((SLOTS, C // 128)), dma((3, HEADS)), dma((2, 2)),
            ],
            compiler_params=pltpu.CompilerParams(vmem_limit_bytes=VMEM_ALL),
        )(y_loc, xg_loc, small1, small2, bupg, h.reshape(flat), h2.reshape(flat), dm.reshape(flat), da.reshape(flat), attn, act, dpre, dqkv)
        wqkv_g = jnp.transpose(wqkv_g.reshape(N_LAYERS, 3, HEADS, D, HD), (0, 3, 1, 2, 4))
        return (y_out[None], x_grad[None], lng, biasg, wqkv_g, wo_g.reshape(N_LAYERS, HEADS, HD, D), wu_g, bupg_o, wd_g)

    in_specs = (P('dp', 'tp', None), P('dp', 'tp', None), P(None, None, None), P(None, None, None),
                P(None, None, None, 'tp', None), P(None, 'tp', None, None), P(None, None, 'tp'), P(None, 'tp'), P(None, 'tp', None))
    out_specs = (P('dp', 'tp', None), P('dp', 'tp', None), P('dp', None, None), P('dp', None, None),
                 P('dp', None, None, 'tp', None), P('dp', 'tp', None, None), P('dp', None, 'tp'), P('dp', 'tp'), P('dp', 'tp', None))
    return jax.shard_map(device_step, mesh=mesh, in_specs=in_specs, out_specs=out_specs, check_vma=False)
```

```python
import jax
import jax.numpy as jnp
from jax import lax
from jax.experimental import pallas as pl
from jax.experimental.pallas import tpu as pltpu
from jax.sharding import PartitionSpec as P

MESH = pl.DeviceIdType.MESH
F32, BF16 = jnp.float32, jnp.bfloat16
N_LAYERS, SEQ, BLK, D, HEADS, HD, FF = 2, 128, 32, 2560, 5, 128, 2560
ATT = HEADS * HD
QKV = 3 * ATT
C = 512
NC = D // C
SLOTS = 4
CA = 256
NA = D // CA
ND = 2
SCALE = HD ** -0.5
GELU_K = 0.7978845608028654
GELU_C = 0.044715
VMEM_ALL = 67043328


def mm(a, b):
    return jnp.dot(a, b, preferred_element_type=F32)


def mm_nt(a, b):
    return lax.dot_general(a, b, (((1,), (1,)), ((), ())), preferred_element_type=F32)


def chunk(c, size=C):
    return pl.ds(pl.multiple_of(c * size, size), size)


def chain_kernel(x_ref, dy_ref, ln_ref, bias_ref, bup_ref, wqkv_h, wo_h, wu_h, wd_h,
                 y_ref, xg_ref, small1_ref, small2_ref, bupg_ref, h_o, h2_o, dm_o, da_o, a_o, act_o, dpre_o, dqkv_o,
                 wq, wo, wu, wd, h_g, h2_g, dm_g, da_g, qkv, prob, attn, act, gp, dpre, dqkv,
                 xh1, xh2, rs1, rs2, res, dres, acc, acct, part, own, rr, xx, ss, sg1, sg2, sgr1, sgr2,
                 wsem, osem, agsem, rssem, gsem):
    me = lax.axis_index('tp')
    x_id = lax.div(me, 2)
    core = lax.rem(me, 2)
    sib = x_id * 2 + (1 - core)
    cross = (1 - x_id) * 2 + core
    diag = (1 - x_id) * 2 + (1 - core)

    def remote(src, dst, send, recv, dev):
        return pltpu.make_async_remote_copy(src_ref=src, dst_ref=dst, send_sem=send, recv_sem=recv,
                                            device_id={'tp': dev}, device_id_type=MESH)

    def weight_copies(kind, layer):
        if kind == 0:
            return [pltpu.make_async_copy(wqkv_h.at[layer, j], wq.at[:, pl.ds(j * HD, HD)], wsem.at[0, j]) for j in range(3 * HEADS)]
        if kind == 1:
            return [pltpu.make_async_copy(wo_h.at[layer], wo, wsem.at[1, 0])]
        src, dst = ((wu_h, wu), (wd_h, wd))[kind - 2]
        return [pltpu.make_async_copy(src.at[layer, pl.ds(j * C, C)], dst.at[pl.ds(j * C, C)], wsem.at[kind, j]) for j in range(NC)]

    def load_w(kind, layer):
        for copy in weight_copies(kind, layer):
            copy.start()

    def wait_w(kind, layer):
        for copy in weight_copies(kind, layer):
            copy.wait()

    def out_copy(i, src, dst, layer):
        return pltpu.make_async_copy(src.at[layer], dst.at[layer], osem.at[i, layer])

    outs = [(h_g, h_o), (h2_g, h2_o), (dm_g, dm_o), (da_g, da_o), (attn, a_o), (act, act_o), (dpre, dpre_o), (dqkv, dqkv_o)]

    def ag_mine(g, layer, c, k, i, dev):
        mine = g.at[layer, me, :, chunk(c, CA)]
        return remote(mine, mine, agsem.at[k, i, c], agsem.at[k, i + 1, c], dev)

    def ag_side(g, layer, c, k=0):
        return ag_mine(g, layer, c, k, 0, sib)

    def ag_across(g, layer, c, k=0):
        return ag_mine(g, layer, c, k, 2, cross)

    def ag_forward(g, layer, c, k=0):
        theirs = g.at[layer, cross, :, chunk(c, CA)]
        return remote(theirs, theirs, agsem.at[k, 4, c], agsem.at[k, 5, c], sib)

    def ag_direct(g, layer, c, k=0):
        return ag_mine(g, layer, c, k, 4, diag)

    def ag_relay(g, layer, k):
        @pl.loop(0, NA)
        def _(c):
            ag_across(g, layer, c, k).wait_recv()

            @pl.when(c < NA - ND)
            def _():
                ag_forward(g, layer, c, k).start()

    def ag_finish(g, layer, k):
        @pl.loop(0, NA)
        def _(c):
            ag_side(g, layer, c, k).wait()
            ag_forward(g, layer, c, k).wait()
            ag_across(g, layer, c, k).wait_send()

    def ag_start(g, layer, k=0):
        @pl.loop(0, NA)
        def _(c):
            ag_across(g, layer, c, k).start()

            @pl.when(c >= NA - ND)
            def _():
                ag_direct(g, layer, c, k).start()

        @pl.loop(0, NA)
        def _(c):
            ag_side(g, layer, c, k).start()

    def ag_consume(g, layer, compute, lag=3):
        @pl.loop(0, NA + lag)
        def _(c):
            @pl.when(c < NA)
            def _():
                ag_across(g, layer, c).wait_recv()

            @pl.when(c < NA - ND)
            def _():
                ag_forward(g, layer, c).start()

            @pl.when(c >= lag)
            def _():
                cc = c - lag
                ag_side(g, layer, cc).wait_recv()
                ag_forward(g, layer, cc).wait_recv()
                compute(cc)

        @pl.loop(0, NA)
        def _(c):
            ag_side(g, layer, c).wait_send()
            ag_across(g, layer, c).wait_send()
            ag_forward(g, layer, c).wait_send()

    def rs_side(par, c):
        return remote(part.at[par // 2, :, 1 - core, :, chunk(c)], rr.at[par, :, :, chunk(c)],
                      rssem.at[par, 0, c], rssem.at[par, 1, c], sib)

    def rs_across(par, c):
        return remote(ss.at[par // 2, :, chunk(c)], xx.at[par, :, chunk(c)], rssem.at[par, 2, c], rssem.at[par, 3, c], cross)

    def rs_send(par, compute, lag=2):
        buf = par // 2

        @pl.loop(0, NC + lag)
        def _(c):
            @pl.when(c < NC)
            def _():
                vals = compute(c)
                for b in range(4):
                    part[buf, b // 2, b % 2, :, chunk(c)] = vals[b * BLK:(b + 1) * BLK]
                rs_side(par, c).start()

            @pl.when(c >= lag)
            def _():
                cc = c - lag
                rs_side(par, cc).wait_recv()
                cols = chunk(cc)
                ss[buf, :, cols] = (part[buf, 1 - x_id, core, :, cols] + rr[par, 1 - x_id, :, cols]).astype(BF16)
                rs_across(par, cc).start()
                own[buf, :, cols] = part[buf, x_id, core, :, cols] + rr[par, x_id, :, cols]

    def rs_finish(par):
        @pl.loop(0, NC)
        def _(c):
            rs_across(par, c).wait_recv()
            rs_side(par, c).wait_send()
            rs_across(par, c).wait_send()
            own[par // 2, :, chunk(c)] += xx[par, :, chunk(c)].astype(F32)

    def normed(vals, gain, shift, xh, rs, layer):
        mean_val = jnp.mean(vals, axis=-1, keepdims=True)
        centered = vals - mean_val
        rstd = lax.rsqrt(jnp.mean(centered * centered, axis=-1, keepdims=True) + 1e-5)
        hat = centered * rstd
        xh[layer] = hat
        rs[layer] = jnp.broadcast_to(rstd, (BLK, 128))
        return (hat * gain + shift).astype(BF16)

    def norm_grad(d_out, gain, xh, rs, layer, rows):
        hat = xh[layer]
        rstd = rs[layer][:, :1]
        rows[layer, 0:1, :] = jnp.sum(d_out * hat, axis=0, keepdims=True)
        rows[layer, 1:2, :] = jnp.sum(d_out, axis=0, keepdims=True)
        d_hat = d_out * gain
        m1 = jnp.mean(d_hat, axis=-1, keepdims=True)
        m2 = jnp.mean(d_hat * hat, axis=-1, keepdims=True)
        return rstd * (d_hat - m1 - hat * m2)

    def small_copies(kind, layer):
        src, dst = ((sg1, sgr1), (sg2, sgr2))[kind]
        return [remote(src.at[layer], dst.at[layer, i], gsem.at[kind, layer, 0, i], gsem.at[kind, layer, 1, i], dev)
                for i, dev in enumerate((sib, cross, diag))]

    def small_start(kind, layer):
        for copy in small_copies(kind, layer):
            copy.start()

    load_w(0, 0)
    barrier = pltpu.get_barrier_semaphore()
    for dev in (sib, cross, diag):
        pl.semaphore_signal(barrier, inc=1, device_id={'tp': dev}, device_id_type=MESH)
    res[...] = x_ref[0].astype(F32)
    pl.semaphore_wait(barrier, 3)

    row_id = lax.broadcasted_iota(jnp.int32, (SEQ, SEQ), 0)
    col_id = lax.broadcasted_iota(jnp.int32, (SEQ, SEQ), 1)
    causal = row_id >= col_id

    def dact_chunk(c):
        g = dm_g[0, :, :, chunk(c, CA)].reshape(SEQ, CA)
        acct[...] += mm_nt(wd[:, chunk(c, CA)], g)

    def dact_early(layer, lo, hi):
        @pl.when(layer == N_LAYERS - 1)
        def _():
            @pl.loop(lo, hi)
            def _(c):
                acct[chunk(c), :] = mm_nt(wd[chunk(c), :], dm_g[N_LAYERS - 1].reshape(SEQ, D))

    def act_chunk(layer, c):
        pre = acc[:, chunk(c)] + bup_ref[layer:layer + 1, chunk(c)]
        t = jnp.tanh(pre * (GELU_K + (GELU_K * GELU_C) * (pre * pre)))
        act[layer, :, chunk(c)] = (pre * (0.5 + 0.5 * t)).astype(BF16)

    def slope_chunk(layer, c):
        pre = acc[:, chunk(c)] + bup_ref[layer:layer + 1, chunk(c)]
        sq = pre * pre
        t = jnp.tanh(pre * (GELU_K + (GELU_K * GELU_C) * sq))
        return (0.5 + 0.5 * t) + (pre * (1.0 - t * t)) * (0.5 * GELU_K + (1.5 * GELU_K * GELU_C) * sq)

    def dpre_chunk(layer, c, slope):
        d_pre = acct[chunk(c), :].T * slope
        bupg_ref[layer:layer + 1, chunk(c)] = jnp.sum(d_pre, axis=0, keepdims=True)
        dpre[layer, :, chunk(c)] = d_pre.astype(BF16)

    @pl.loop(0, N_LAYERS)
    def _(layer):
        first = layer == 0
        last = layer == N_LAYERS - 1
        lnp = ln_ref[layer]
        h_g[layer, me] = normed(res[...], lnp[0:1], lnp[1:2], xh1, rs1, layer)
        ag_start(h_g, layer)
        acc[...] = jnp.zeros_like(acc)
        wait_w(0, layer)

        @pl.when(first)
        def _():
            load_w(1, 0)
            load_w(2, 0)

        def qkv_chunk(c):
            h = h_g[layer, :, :, chunk(c, CA)].reshape(SEQ, CA)
            for n in range(0, QKV, 640):
                acc[:, n:n + 640] += mm(h, wq[chunk(c, CA), n:n + 640])
        ag_consume(h_g, layer, qkv_chunk)
        out_copy(0, h_g, h_o, layer).start()

        @pl.when(first)
        def _():
            load_w(0, 1)
            dm_g[N_LAYERS - 1, me] = dy_ref[0]
            ag_start(dm_g, N_LAYERS - 1, 1)

        for j in range(3 * HEADS):
            qkv[layer, :, j * HD:(j + 1) * HD] = acc[:, j * HD:(j + 1) * HD].astype(BF16)
        for hd in range(HEADS):
            q = qkv[layer, :, hd * HD:(hd + 1) * HD]
            k = qkv[layer, :, ATT + hd * HD:ATT + (hd + 1) * HD]
            v = qkv[layer, :, 2 * ATT + hd * HD:2 * ATT + (hd + 1) * HD]
            scores = jnp.where(causal, mm_nt(q, k) * SCALE, -1e30)
            e = jnp.exp(scores - jnp.max(scores, axis=-1, keepdims=True))
            p = (e / jnp.sum(e, axis=-1, keepdims=True)).astype(BF16)
            prob[layer, hd] = p
            attn[layer, :, hd * HD:(hd + 1) * HD] = mm(p, v).astype(BF16)
        out_copy(4, attn, a_o, layer).start()
        wait_w(1, layer)

        @pl.when(first)
        def _():
            load_w(3, 0)
        @pl.when(last)
        def _():
            wait_w(3, N_LAYERS - 1)
        rs_send(0, lambda c: mm(attn[layer], wo[:, chunk(c)]))
        dact_early(layer, 0, 2)

        @pl.when(first)
        def _():
            ag_relay(dm_g, N_LAYERS - 1, 1)
        rs_finish(0)

        @pl.when(first)
        def _():
            load_w(1, 1)
            ag_finish(dm_g, N_LAYERS - 1, 1)
            out_copy(2, dm_g, dm_o, N_LAYERS - 1).start()
        res[...] = res[...] + own[0] + bias_ref[layer, 0:1]

        h2_g[layer, me] = normed(res[...], lnp[2:3], lnp[3:4], xh2, rs2, layer)
        ag_start(h2_g, layer)
        acc[...] = jnp.zeros_like(acc)
        wait_w(2, layer)
        dact_early(layer, 2, NC)

        def up_chunk(c):
            h = h2_g[layer, :, :, chunk(c, CA)].reshape(SEQ, CA)
            for n in range(0, FF, C):
                acc[:, n:n + C] += mm(h, wu[chunk(c, CA), n:n + C])
        ag_consume(h2_g, layer, up_chunk)
        out_copy(1, h2_g, h2_o, layer).start()

        @pl.when(first)
        def _():
            load_w(2, 1)

        @pl.when(first)
        def _():
            @pl.loop(0, FF // C)
            def _(c):
                act_chunk(0, c)
            out_copy(5, act, act_o, 0).start()
            wait_w(3, 0)
            rs_send(1, lambda c: mm(act[0], wd[:, chunk(c)]))

            @pl.loop(0, FF // C)
            def _(c):
                gp[:, chunk(c)] = slope_chunk(0, c)
            rs_finish(1)
            load_w(3, 1)
            res[...] = res[...] + own[0] + bias_ref[0, 1:2]

    @pl.loop(0, FF // C)
    def _(c):
        dpre_chunk(N_LAYERS - 1, c, slope_chunk(N_LAYERS - 1, c))
    out_copy(6, dpre, dpre_o, N_LAYERS - 1).start()
    dres[...] = dy_ref[0].astype(F32)

    @pl.loop(0, N_LAYERS)
    def _(step):
        layer = N_LAYERS - 1 - step
        top = step == 0
        low = step == N_LAYERS - 1
        lnp = ln_ref[layer]
        sg2[layer, 3:4, :] = jnp.sum(dres[...], axis=0, keepdims=True)
        @pl.when(low)
        def _():
            dm_g[0, me] = dres[...].astype(BF16)
            ag_start(dm_g, 0)
            acct[...] = jnp.zeros_like(acct)
            wait_w(3, 0)
            ag_consume(dm_g, 0, dact_chunk)
            out_copy(2, dm_g, dm_o, 0).start()

        @pl.when(low)
        def _():
            @pl.loop(0, FF // C)
            def _(c):
                dpre_chunk(0, c, gp[:, chunk(c)])
            out_copy(6, dpre, dpre_o, 0).start()

        @pl.when(low)
        def _():
            small_start(0, N_LAYERS - 1)
            small_start(1, N_LAYERS - 1)
            wait_w(2, 0)
        rs_send(0, lambda c: mm_nt(wu[chunk(c), :], dpre[layer]).T)

        @pl.when(top)
        def _():
            load_w(2, 0)

            @pl.loop(0, FF // C)
            def _(c):
                act_chunk(N_LAYERS - 1, c)
            out_copy(5, act, act_o, N_LAYERS - 1).start()
            rs_send(2, lambda c: mm(act[N_LAYERS - 1], wd[:, chunk(c)]))
            load_w(3, 0)
        rs_finish(0)
        dres[...] = dres[...] + norm_grad(own[0], lnp[2:3], xh2, rs2, layer, sg2)

        sg2[layer, 2:3, :] = jnp.sum(dres[...], axis=0, keepdims=True)
        da_g[layer, me] = dres[...].astype(BF16)
        ag_start(da_g, layer)
        acct[0:ATT, :] = jnp.zeros((ATT, SEQ), F32)

        @pl.when(low)
        def _():
            wait_w(1, 0)

        def dattn_chunk(c):
            g = da_g[layer, :, :, chunk(c, CA)].reshape(SEQ, CA)
            acct[0:ATT, :] += mm_nt(wo[:, chunk(c, CA)], g)
        ag_consume(da_g, layer, dattn_chunk)
        out_copy(3, da_g, da_o, layer).start()

        @pl.when(top)
        def _():
            load_w(1, 0)
            rs_finish(2)
            y_ref[...] = (res[...] + own[1] + bias_ref[N_LAYERS - 1, 1:2]).astype(BF16)

        @pl.when(low)
        def _():
            small_start(1, 0)

        for hd in range(HEADS):
            q = qkv[layer, :, hd * HD:(hd + 1) * HD]
            k = qkv[layer, :, ATT + hd * HD:ATT + (hd + 1) * HD]
            v = qkv[layer, :, 2 * ATT + hd * HD:2 * ATT + (hd + 1) * HD]
            p = prob[layer, hd]
            d_o = acct[hd * HD:(hd + 1) * HD, :].T.astype(BF16)
            d_p = mm_nt(d_o, v)
            d_v = mm(p.T, d_o)
            pf = p.astype(F32)
            dot = jnp.sum(d_p * pf, axis=-1, keepdims=True)
            d_s = (pf * (d_p - dot) * SCALE).astype(BF16)
            dqkv[layer, :, hd * HD:(hd + 1) * HD] = mm(d_s, k).astype(BF16)
            dqkv[layer, :, ATT + hd * HD:ATT + (hd + 1) * HD] = mm(d_s.T, q).astype(BF16)
            dqkv[layer, :, 2 * ATT + hd * HD:2 * ATT + (hd + 1) * HD] = d_v.astype(BF16)
        out_copy(7, dqkv, dqkv_o, layer).start()

        @pl.when(low)
        def _():
            wait_w(0, 0)
        rs_send(1, lambda c: mm_nt(wq[chunk(c), :], dqkv[layer]).T)
        rs_finish(1)

        @pl.when(top)
        def _():
            load_w(0, 0)
        dres[...] = dres[...] + norm_grad(own[0], lnp[0:1], xh1, rs1, layer, sg1)

    small_start(0, 0)
    xg_ref[...] = dres[...].astype(BF16)
    for kind, layer in ((0, 1), (1, 1), (1, 0), (0, 0)):
        src, dst, out = ((sg1, sgr1, small1_ref), (sg2, sgr2, small2_ref))[kind]
        for copy in small_copies(kind, layer):
            copy.wait()
        out[layer] = (src[layer] + dst[layer, 0]) + (dst[layer, 1] + dst[layer, 2])
    for layer in range(N_LAYERS):
        for i, (src, dst) in enumerate(outs):
            out_copy(i, src, dst, layer).wait()


def grads_kernel(y_in, xg_in, small1_in, small2_in, bupg_in, h_h, h2_h, dm_h, da_h, a_h, act_h, dpre_h, dqkv_h,
                 y_o, xg_o, lng_o, biasg_o, wqkv_o, wo_o, wu_o, bupg_o, wd_o,
                 h, h2, dm, da, attn, act, dpre, dqkv, big, qbuf, obuf, y_v, xg_v, small1_v, small2_v, bupg_v, lng_v, biasg_v, isem, bsem, qsem, osem, psem):
    ins = [(dm_h, dm), (act_h, act), (h2_h, h2), (dpre_h, dpre), (da_h, da), (a_h, attn), (h_h, h), (dqkv_h, dqkv)]

    def in_copy(i, layer):
        return pltpu.make_async_copy(ins[i][0].at[layer], ins[i][1].at[layer], isem.at[i, layer])

    order = [(i, layer) for layer in reversed(range(N_LAYERS)) for i in range(0, len(ins), 2)]

    def prefetch(k):
        if k < len(order):
            in_copy(order[k][0], order[k][1]).start()
            in_copy(order[k][0] + 1, order[k][1]).start()

    prefetch(0)
    prefetch(1)
    small_in = [pltpu.make_async_copy(src, dst, psem.at[i]) for i, (src, dst) in enumerate(
        ((y_in, y_v), (xg_in, xg_v), (small1_in, small1_v), (small2_in, small2_v), (bupg_in, bupg_v)))]
    small_out = [pltpu.make_async_copy(src, dst, psem.at[i]) for i, (src, dst) in enumerate(
        ((y_v, y_o), (xg_v, xg_o), (lng_v, lng_o), (biasg_v, biasg_o), (bupg_v, bupg_o)))]
    for copy in small_in:
        copy.start()

    def big_copies(dst, layer, c, slot):
        return [pltpu.make_async_copy(big.at[slot, pl.ds(r * 128, 128)], dst.at[layer, pl.ds(pl.multiple_of(c * C + r * 128, 128), 128)],
                                      bsem.at[slot, r]) for r in range(C // 128)]

    def q_copies(layer, c, slot):
        return [pltpu.make_async_copy(qbuf.at[slot, pl.ds(3 * j, 3)], wqkv_o.at[layer, pl.ds(3 * j, 3), chunk(c), :], qsem.at[slot, j])
                for j in range(HEADS)]

    def o_copies(layer, c):
        return [pltpu.make_async_copy(obuf.at[c, pl.ds(r * 160, 160)], wo_o.at[layer, pl.ds(c * (ATT // 2) + r * 160, 160)], osem.at[c, r])
                for r in range(2)]

    def start(copies):
        for copy in copies:
            copy.start()

    def wait(copies):
        for copy in copies:
            copy.wait()

    for step, layer in enumerate(reversed(range(N_LAYERS))):
        for w, (dst, left, right) in enumerate(((wd_o, act, dm), (wu_o, h2, dpre))):
            in_copy(2 * w, layer).wait()
            in_copy(2 * w + 1, layer).wait()
            prefetch(4 * step + w + 2)
            base = (2 * step + w) * NC

            @pl.loop(0, NC)
            def _(c):
                slot = lax.rem(base + c, SLOTS)

                @pl.when(base + c >= SLOTS)
                def _():
                    wait(big_copies(dst, layer, c, slot))
                lt = left[layer, :, chunk(c)].T
                for n in range(0, D, C):
                    big[slot, :, n:n + C] = mm(lt, right[layer, :, n:n + C]).astype(BF16)
                start(big_copies(dst, layer, c, slot))
        if step == 0:
            for copy in small_in:
                copy.wait()
            lng_v[:, 0:2, :] = small1_v[...]
            lng_v[:, 2:4, :] = small2_v[:, 0:2, :]
            biasg_v[...] = small2_v[:, 2:4, :]
            for copy in small_out:
                copy.start()
        in_copy(4, layer).wait()
        in_copy(5, layer).wait()
        prefetch(4 * step + 4)
        for c in range(2):
            if step > 0:
                wait(o_copies(layer, c))
            lt = attn[layer, :, :].T[c * (ATT // 2):(c + 1) * (ATT // 2)]
            for n in range(0, D, C):
                obuf[c, :, n:n + C] = mm(lt, da[layer, :, n:n + C]).astype(BF16)
            start(o_copies(layer, c))
        in_copy(6, layer).wait()
        in_copy(7, layer).wait()
        prefetch(4 * step + 5)
        qbase = step * NC

        @pl.loop(0, NC)
        def _(c):
            slot = lax.rem(qbase + c, 3)

            @pl.when(qbase + c >= 3)
            def _():
                wait(q_copies(layer, c, slot))
            lt = h[layer, :, chunk(c)].T
            for n in range(0, QKV, 3 * HD):
                vals = mm(lt, dqkv[layer, :, n:n + 3 * HD]).astype(BF16)
                for j in range(3):
                    qbuf[slot, n // HD + j] = vals[:, j * HD:(j + 1) * HD]
            start(q_copies(layer, c, slot))
    for copy in small_out:
        copy.wait()
    for slot in range(SLOTS):
        wait(big_copies(wu_o, 0, 0, slot))
    for slot in range(3):
        wait(q_copies(0, 0, slot))
    for c in range(2):
        wait(o_copies(0, c))


def solution(mesh):
    vmem = pl.BlockSpec(memory_space=pltpu.VMEM)
    hbm = pl.BlockSpec(memory_space=pl.ANY)

    def device_step(x_loc, dy_loc, ln_par, bias_d, w_qkv, w_out, w_up, b_up, w_down):
        wqkv_t = jnp.transpose(w_qkv, (0, 2, 3, 1, 4)).reshape(N_LAYERS, 3 * HEADS, D, HD)
        wo_t = w_out.reshape(N_LAYERS, ATT, D)
        sds = jax.ShapeDtypeStruct
        gath = (N_LAYERS, 4, BLK, D)
        dma = pltpu.SemaphoreType.DMA
        chain_out = pl.pallas_call(
            chain_kernel,
            name='chain',
            out_shape=(sds((BLK, D), BF16), sds((BLK, D), BF16), sds((N_LAYERS, 2, D), F32), sds((N_LAYERS, 4, D), F32), sds((N_LAYERS, FF), F32),
                       sds(gath, BF16), sds(gath, BF16), sds(gath, BF16), sds(gath, BF16),
                       sds((N_LAYERS, SEQ, ATT), BF16), sds((N_LAYERS, SEQ, FF), BF16), sds((N_LAYERS, SEQ, FF), BF16),
                       sds((N_LAYERS, SEQ, QKV), BF16)),
            in_specs=[vmem] * 5 + [hbm] * 4,
            out_specs=tuple([vmem] * 5 + [hbm] * 8),
            scratch_shapes=[
                pltpu.VMEM((D, QKV), BF16), pltpu.VMEM((ATT, D), BF16), pltpu.VMEM((D, FF), BF16), pltpu.VMEM((FF, D), BF16),
                pltpu.VMEM(gath, BF16), pltpu.VMEM(gath, BF16), pltpu.VMEM(gath, BF16), pltpu.VMEM(gath, BF16),
                pltpu.VMEM((N_LAYERS, SEQ, QKV), BF16), pltpu.VMEM((N_LAYERS, HEADS, SEQ, SEQ), BF16),
                pltpu.VMEM((N_LAYERS, SEQ, ATT), BF16), pltpu.VMEM((N_LAYERS, SEQ, FF), BF16), pltpu.VMEM((SEQ, FF), F32),
                pltpu.VMEM((N_LAYERS, SEQ, FF), BF16), pltpu.VMEM((N_LAYERS, SEQ, QKV), BF16),
                pltpu.VMEM((N_LAYERS, BLK, D), F32), pltpu.VMEM((N_LAYERS, BLK, D), F32),
                pltpu.VMEM((N_LAYERS, BLK, 128), F32), pltpu.VMEM((N_LAYERS, BLK, 128), F32),
                pltpu.VMEM((BLK, D), F32), pltpu.VMEM((BLK, D), F32), pltpu.VMEM((SEQ, D), F32), pltpu.VMEM((D, SEQ), F32),
                pltpu.VMEM((2, 2, 2, BLK, D), F32), pltpu.VMEM((2, BLK, D), F32), pltpu.VMEM((3, 2, BLK, D), F32),
                pltpu.VMEM((3, BLK, D), BF16), pltpu.VMEM((2, BLK, D), BF16),
                pltpu.VMEM((N_LAYERS, 2, D), F32), pltpu.VMEM((N_LAYERS, 4, D), F32), pltpu.VMEM((N_LAYERS, 3, 2, D), F32), pltpu.VMEM((N_LAYERS, 3, 4, D), F32),
                dma((4, 3 * HEADS)), dma((8, N_LAYERS)), dma((2, 6, NA)), dma((3, 4, NC)), dma((2, N_LAYERS, 2, 3)),
            ],
            compiler_params=pltpu.CompilerParams(collective_id=0, has_side_effects=True, vmem_limit_bytes=VMEM_ALL),
        )(x_loc, dy_loc, ln_par, bias_d, b_up, wqkv_t, wo_t, w_up, w_down)
        y_loc, xg_loc, small1, small2, bupg, h, h2, dm, da, attn, act, dpre, dqkv = chain_out
        flat = (N_LAYERS, SEQ, D)
        y_out, x_grad, lng, biasg, wqkv_g, wo_g, wu_g, bupg_o, wd_g = pl.pallas_call(
            grads_kernel,
            name='grads',
            out_shape=(sds((BLK, D), BF16), sds((BLK, D), BF16), sds((N_LAYERS, 4, D), F32), sds((N_LAYERS, 2, D), F32),
                       sds((N_LAYERS, 3 * HEADS, D, HD), BF16), sds((N_LAYERS, ATT, D), BF16), sds((N_LAYERS, D, FF), BF16),
                       sds((N_LAYERS, FF), F32), sds((N_LAYERS, FF, D), BF16)),
            in_specs=[hbm] * 13,
            out_specs=tuple([hbm] * 9),
            scratch_shapes=[
                pltpu.VMEM(flat, BF16), pltpu.VMEM(flat, BF16), pltpu.VMEM(flat, BF16), pltpu.VMEM(flat, BF16),
                pltpu.VMEM((N_LAYERS, SEQ, ATT), BF16), pltpu.VMEM((N_LAYERS, SEQ, FF), BF16), pltpu.VMEM((N_LAYERS, SEQ, FF), BF16),
                pltpu.VMEM((N_LAYERS, SEQ, QKV), BF16),
                pltpu.VMEM((SLOTS, C, D), BF16), pltpu.VMEM((3, 3 * HEADS, C, HD), BF16), pltpu.VMEM((2, ATT // 2, D), BF16),
                pltpu.VMEM((BLK, D), BF16), pltpu.VMEM((BLK, D), BF16), pltpu.VMEM((N_LAYERS, 2, D), F32), pltpu.VMEM((N_LAYERS, 4, D), F32),
                pltpu.VMEM((N_LAYERS, FF), F32), pltpu.VMEM((N_LAYERS, 4, D), F32), pltpu.VMEM((N_LAYERS, 2, D), F32),
                dma((8, N_LAYERS)), dma((SLOTS, C // 128)), dma((3, HEADS)), dma((2, 2)), dma((5,)),
            ],
            compiler_params=pltpu.CompilerParams(vmem_limit_bytes=VMEM_ALL),
        )(y_loc, xg_loc, small1, small2, bupg, h.reshape(flat), h2.reshape(flat), dm.reshape(flat), da.reshape(flat), attn, act, dpre, dqkv)
        wqkv_g = jnp.transpose(wqkv_g.reshape(N_LAYERS, 3, HEADS, D, HD), (0, 3, 1, 2, 4))
        return (y_out[None], x_grad[None], lng, biasg, wqkv_g, wo_g.reshape(N_LAYERS, HEADS, HD, D), wu_g, bupg_o, wd_g)

    in_specs = (P('dp', 'tp', None), P('dp', 'tp', None), P(None, None, None), P(None, None, None),
                P(None, None, None, 'tp', None), P(None, 'tp', None, None), P(None, None, 'tp'), P(None, 'tp'), P(None, 'tp', None))
    out_specs = (P('dp', 'tp', None), P('dp', 'tp', None), P('dp', None, None), P('dp', None, None),
                 P('dp', None, None, 'tp', None), P('dp', 'tp', None, None), P('dp', None, 'tp'), P('dp', 'tp'), P('dp', 'tp', None))
    return jax.shard_map(device_step, mesh=mesh, in_specs=in_specs, out_specs=out_specs, check_vma=False)
```

```python
import jax
import jax.numpy as jnp
from jax import lax
from jax.experimental import pallas as pl
from jax.experimental.pallas import tpu as pltpu
from jax.sharding import PartitionSpec as P

MESH = pl.DeviceIdType.MESH
F32, BF16 = jnp.float32, jnp.bfloat16
N_LAYERS, SEQ, BLK, D, HEADS, HD, FF = 2, 128, 32, 2560, 5, 128, 2560
ATT = HEADS * HD
QKV = 3 * ATT
C = 512
NC = D // C
SLOTS = 4
CA = 512
NA = D // CA
ND = 1
SCALE = HD ** -0.5
GELU_K = 0.7978845608028654
GELU_C = 0.044715
VMEM_ALL = 67043328


def mm(a, b):
    return jnp.dot(a, b, preferred_element_type=F32)


def mm_nt(a, b):
    return lax.dot_general(a, b, (((1,), (1,)), ((), ())), preferred_element_type=F32)


def chunk(c, size=C):
    return pl.ds(pl.multiple_of(c * size, size), size)


def chain_kernel(x_ref, dy_ref, ln_ref, bias_ref, bup_ref, wqkv_h, wo_h, wu_h, wd_h,
                 y_ref, xg_ref, small1_ref, small2_ref, bupg_ref, h_o, h2_o, dm_o, da_o, a_o, act_o, dpre_o, dqkv_o,
                 wq, wo, wu, wd, h_g, h2_g, dm_g, da_g, qkv, prob, attn, act, gp, dpre, dqkv,
                 xh1, xh2, rs1, rs2, res, dres, acc, acct, part, own, rr, xx, ss, sg1, sg2, sgr1, sgr2,
                 wsem, osem, agsem, rssem, gsem):
    me = lax.axis_index('tp')
    x_id = lax.div(me, 2)
    core = lax.rem(me, 2)
    sib = x_id * 2 + (1 - core)
    cross = (1 - x_id) * 2 + core
    diag = (1 - x_id) * 2 + (1 - core)

    def remote(src, dst, send, recv, dev):
        return pltpu.make_async_remote_copy(src_ref=src, dst_ref=dst, send_sem=send, recv_sem=recv,
                                            device_id={'tp': dev}, device_id_type=MESH)

    def weight_copies(kind, layer):
        if kind == 0:
            return [pltpu.make_async_copy(wqkv_h.at[layer, j], wq.at[:, pl.ds(j * HD, HD)], wsem.at[0, j]) for j in range(3 * HEADS)]
        if kind == 1:
            return [pltpu.make_async_copy(wo_h.at[layer], wo, wsem.at[1, 0])]
        src, dst = ((wu_h, wu), (wd_h, wd))[kind - 2]
        return [pltpu.make_async_copy(src.at[layer, pl.ds(j * C, C)], dst.at[pl.ds(j * C, C)], wsem.at[kind, j]) for j in range(NC)]

    def load_w(kind, layer):
        for copy in weight_copies(kind, layer):
            copy.start()

    def wait_w(kind, layer):
        for copy in weight_copies(kind, layer):
            copy.wait()

    def out_copy(i, src, dst, layer):
        return pltpu.make_async_copy(src.at[layer], dst.at[layer], osem.at[i, layer])

    outs = [(h_g, h_o), (h2_g, h2_o), (dm_g, dm_o), (da_g, da_o), (attn, a_o), (act, act_o), (dpre, dpre_o), (dqkv, dqkv_o)]

    def ag_mine(g, layer, c, k, i, dev):
        mine = g.at[layer, me, :, chunk(c, CA)]
        return remote(mine, mine, agsem.at[k, i, 0], agsem.at[k, i + 1, c], dev)

    def ag_side(g, layer, c, k=0):
        return ag_mine(g, layer, c, k, 0, sib)

    def ag_across(g, layer, c, k=0):
        return ag_mine(g, layer, c, k, 2, cross)

    def ag_forward(g, layer, c, k=0):
        theirs = g.at[layer, cross, :, chunk(c, CA)]
        return remote(theirs, theirs, agsem.at[k, 4, 0], agsem.at[k, 5, c], sib)

    def ag_direct(g, layer, c, k=0):
        return ag_mine(g, layer, c, k, 4, diag)

    def ag_sent(g, layer, k=0):
        for i, dev in ((0, sib), (2, cross), (4, sib)):
            remote(g.at[layer, me], g.at[layer, me], agsem.at[k, i, 0], agsem.at[k, i + 1, 0], dev).wait_send()

    def ag_relay(g, layer, k):
        @pl.loop(0, NA)
        def _(c):
            ag_across(g, layer, c, k).wait_recv()

            @pl.when(c < NA - ND)
            def _():
                ag_forward(g, layer, c, k).start()

    def ag_finish(g, layer, k):
        @pl.loop(0, NA)
        def _(c):
            ag_side(g, layer, c, k).wait_recv()
            ag_forward(g, layer, c, k).wait_recv()
        ag_sent(g, layer, k)

    def ag_start(g, layer, k=0):
        for c in range(NA):
            ag_across(g, layer, c, k).start()
            if c >= NA - ND:
                ag_direct(g, layer, c, k).start()
        for c in range(NA):
            ag_side(g, layer, c, k).start()

    def ag_consume(g, layer, compute, lag=2):
        @pl.loop(0, NA + lag)
        def _(c):
            @pl.when(c < NA)
            def _():
                ag_across(g, layer, c).wait_recv()

            @pl.when(c < NA - ND)
            def _():
                ag_forward(g, layer, c).start()

            @pl.when(c >= lag)
            def _():
                cc = c - lag
                ag_side(g, layer, cc).wait_recv()
                ag_forward(g, layer, cc).wait_recv()
                compute(cc)

        ag_sent(g, layer)

    def rs_side(par, c):
        return remote(part.at[par // 2, :, 1 - core, :, chunk(c)], rr.at[par, :, :, chunk(c)],
                      rssem.at[par, 0, 0], rssem.at[par, 1, c], sib)

    def rs_across(par, c):
        return remote(ss.at[par // 2, :, chunk(c)], xx.at[par, :, chunk(c)], rssem.at[par, 2, 0], rssem.at[par, 3, 0], cross)

    def rs_send(par, compute, lag=2):
        buf = par // 2

        @pl.loop(0, NC + lag)
        def _(c):
            @pl.when(c < NC)
            def _():
                vals = compute(c)
                for b in range(4):
                    part[buf, b // 2, b % 2, :, chunk(c)] = vals[b * BLK:(b + 1) * BLK]
                rs_side(par, c).start()

            @pl.when(c >= lag)
            def _():
                cc = c - lag
                rs_side(par, cc).wait_recv()
                cols = chunk(cc)
                ss[buf, :, cols] = (part[buf, 1 - x_id, core, :, cols] + rr[par, 1 - x_id, :, cols]).astype(BF16)
                rs_across(par, cc).start()
                own[buf, :, cols] = part[buf, x_id, core, :, cols] + rr[par, x_id, :, cols]

    def rs_finish(par):
        buf = par // 2
        remote(part.at[buf, :, 1 - core], rr.at[par], rssem.at[par, 0, 0], rssem.at[par, 1, 0], sib).wait_send()
        remote(ss.at[buf], xx.at[par], rssem.at[par, 2, 0], rssem.at[par, 3, 0], cross).wait()
        return own[buf] + xx[par].astype(F32)

    def normed(vals, gain, shift, xh, rs, layer):
        mean_val = jnp.mean(vals, axis=-1, keepdims=True)
        centered = vals - mean_val
        rstd = lax.rsqrt(jnp.mean(centered * centered, axis=-1, keepdims=True) + 1e-5)
        hat = centered * rstd
        xh[layer] = hat
        rs[layer] = jnp.broadcast_to(rstd, (BLK, 128))
        return (hat * gain + shift).astype(BF16)

    def norm_grad(d_out, gain, xh, rs, layer, rows):
        hat = xh[layer]
        rstd = rs[layer][:, :1]
        rows[layer, 0:1, :] = jnp.sum(d_out * hat, axis=0, keepdims=True)
        rows[layer, 1:2, :] = jnp.sum(d_out, axis=0, keepdims=True)
        d_hat = d_out * gain
        m1 = jnp.mean(d_hat, axis=-1, keepdims=True)
        m2 = jnp.mean(d_hat * hat, axis=-1, keepdims=True)
        return rstd * (d_hat - m1 - hat * m2)

    def small_copies(kind, layer):
        src, dst = ((sg1, sgr1), (sg2, sgr2))[kind]
        return [remote(src.at[layer], dst.at[layer, i], gsem.at[kind, layer, 0, i], gsem.at[kind, layer, 1, i], dev)
                for i, dev in enumerate((sib, cross, diag))]

    def small_start(kind, layer):
        for copy in small_copies(kind, layer):
            copy.start()

    load_w(0, 0)
    barrier = pltpu.get_barrier_semaphore()
    for dev in (sib, cross, diag):
        pl.semaphore_signal(barrier, inc=1, device_id={'tp': dev}, device_id_type=MESH)
    res[...] = x_ref[0].astype(F32)
    pl.semaphore_wait(barrier, 3)

    row_id = lax.broadcasted_iota(jnp.int32, (SEQ, SEQ), 0)
    col_id = lax.broadcasted_iota(jnp.int32, (SEQ, SEQ), 1)
    causal = row_id >= col_id

    def dact_chunk(c):
        g = dm_g[0, :, :, chunk(c, CA)].reshape(SEQ, CA)
        acct[...] += mm_nt(wd[:, chunk(c, CA)], g)

    def dact_early(layer, lo, hi):
        @pl.when(layer == N_LAYERS - 1)
        def _():
            @pl.loop(lo, hi)
            def _(c):
                acct[chunk(c), :] = mm_nt(wd[chunk(c), :], dm_g[N_LAYERS - 1].reshape(SEQ, D))

    def act_chunk(layer, c):
        pre = acc[:, chunk(c)] + bup_ref[layer:layer + 1, chunk(c)]
        t = jnp.tanh(pre * (GELU_K + (GELU_K * GELU_C) * (pre * pre)))
        act[layer, :, chunk(c)] = (pre * (0.5 + 0.5 * t)).astype(BF16)

    def slope_chunk(layer, c):
        pre = acc[:, chunk(c)] + bup_ref[layer:layer + 1, chunk(c)]
        sq = pre * pre
        t = jnp.tanh(pre * (GELU_K + (GELU_K * GELU_C) * sq))
        return (0.5 + 0.5 * t) + (pre * (1.0 - t * t)) * (0.5 * GELU_K + (1.5 * GELU_K * GELU_C) * sq)

    def dpre_chunk(layer, c, slope):
        d_pre = acct[chunk(c), :].T * slope
        bupg_ref[layer:layer + 1, chunk(c)] = jnp.sum(d_pre, axis=0, keepdims=True)
        dpre[layer, :, chunk(c)] = d_pre.astype(BF16)

    @pl.loop(0, N_LAYERS)
    def _(layer):
        first = layer == 0
        last = layer == N_LAYERS - 1
        lnp = ln_ref[layer]
        h_g[layer, me] = normed(res[...], lnp[0:1], lnp[1:2], xh1, rs1, layer)
        ag_start(h_g, layer)
        acc[...] = jnp.zeros_like(acc)
        wait_w(0, layer)

        @pl.when(first)
        def _():
            load_w(1, 0)
            load_w(2, 0)

        def qkv_chunk(c):
            h = h_g[layer, :, :, chunk(c, CA)].reshape(SEQ, CA)
            for n in range(0, QKV, 640):
                acc[:, n:n + 640] += mm(h, wq[chunk(c, CA), n:n + 640])
        ag_consume(h_g, layer, qkv_chunk)
        out_copy(0, h_g, h_o, layer).start()

        @pl.when(first)
        def _():
            load_w(0, 1)
            dm_g[N_LAYERS - 1, me] = dy_ref[0]
            ag_start(dm_g, N_LAYERS - 1, 1)

        for j in range(3 * HEADS):
            qkv[layer, :, j * HD:(j + 1) * HD] = acc[:, j * HD:(j + 1) * HD].astype(BF16)
        for hd in range(HEADS):
            q = qkv[layer, :, hd * HD:(hd + 1) * HD]
            k = qkv[layer, :, ATT + hd * HD:ATT + (hd + 1) * HD]
            v = qkv[layer, :, 2 * ATT + hd * HD:2 * ATT + (hd + 1) * HD]
            scores = jnp.where(causal, mm_nt(q, k) * SCALE, -1e30)
            e = jnp.exp(scores - jnp.max(scores, axis=-1, keepdims=True))
            p = (e / jnp.sum(e, axis=-1, keepdims=True)).astype(BF16)
            prob[layer, hd] = p
            attn[layer, :, hd * HD:(hd + 1) * HD] = mm(p, v).astype(BF16)
        out_copy(4, attn, a_o, layer).start()
        wait_w(1, layer)

        @pl.when(first)
        def _():
            load_w(3, 0)
        @pl.when(last)
        def _():
            wait_w(3, N_LAYERS - 1)
        rs_send(0, lambda c: mm(attn[layer], wo[:, chunk(c)]))
        dact_early(layer, 0, 2)

        @pl.when(first)
        def _():
            ag_relay(dm_g, N_LAYERS - 1, 1)
        total = rs_finish(0)
        res[...] = res[...] + total + bias_ref[layer, 0:1]

        @pl.when(first)
        def _():
            load_w(1, 1)
            ag_finish(dm_g, N_LAYERS - 1, 1)
            out_copy(2, dm_g, dm_o, N_LAYERS - 1).start()

        h2_g[layer, me] = normed(res[...], lnp[2:3], lnp[3:4], xh2, rs2, layer)
        ag_start(h2_g, layer)
        acc[...] = jnp.zeros_like(acc)
        wait_w(2, layer)
        dact_early(layer, 2, NC)

        def up_chunk(c):
            h = h2_g[layer, :, :, chunk(c, CA)].reshape(SEQ, CA)
            for n in range(0, FF, C):
                acc[:, n:n + C] += mm(h, wu[chunk(c, CA), n:n + C])
        ag_consume(h2_g, layer, up_chunk)
        out_copy(1, h2_g, h2_o, layer).start()

        @pl.when(first)
        def _():
            load_w(2, 1)

        @pl.when(first)
        def _():
            @pl.loop(0, FF // C)
            def _(c):
                act_chunk(0, c)
            out_copy(5, act, act_o, 0).start()
            wait_w(3, 0)
            rs_send(1, lambda c: mm(act[0], wd[:, chunk(c)]))

            @pl.loop(0, FF // C)
            def _(c):
                gp[:, chunk(c)] = slope_chunk(0, c)
            total = rs_finish(1)
            load_w(3, 1)
            res[...] = res[...] + total + bias_ref[0, 1:2]

    @pl.loop(0, FF // C)
    def _(c):
        dpre_chunk(N_LAYERS - 1, c, slope_chunk(N_LAYERS - 1, c))
    out_copy(6, dpre, dpre_o, N_LAYERS - 1).start()
    dres[...] = dy_ref[0].astype(F32)

    @pl.loop(0, N_LAYERS)
    def _(step):
        layer = N_LAYERS - 1 - step
        top = step == 0
        low = step == N_LAYERS - 1
        lnp = ln_ref[layer]
        sg2[layer, 3:4, :] = jnp.sum(dres[...], axis=0, keepdims=True)
        @pl.when(low)
        def _():
            dm_g[0, me] = dres[...].astype(BF16)
            ag_start(dm_g, 0)
            acct[...] = jnp.zeros_like(acct)
            wait_w(3, 0)
            ag_consume(dm_g, 0, dact_chunk)
            out_copy(2, dm_g, dm_o, 0).start()

        @pl.when(low)
        def _():
            @pl.loop(0, FF // C)
            def _(c):
                dpre_chunk(0, c, gp[:, chunk(c)])
            out_copy(6, dpre, dpre_o, 0).start()

        @pl.when(low)
        def _():
            small_start(0, N_LAYERS - 1)
            small_start(1, N_LAYERS - 1)
            wait_w(2, 0)
        rs_send(0, lambda c: mm_nt(wu[chunk(c), :], dpre[layer]).T)

        @pl.when(top)
        def _():
            load_w(2, 0)

            @pl.loop(0, FF // C)
            def _(c):
                act_chunk(N_LAYERS - 1, c)
            out_copy(5, act, act_o, N_LAYERS - 1).start()
            rs_send(2, lambda c: mm(act[N_LAYERS - 1], wd[:, chunk(c)]))
            load_w(3, 0)
        total = rs_finish(0)
        dres[...] = dres[...] + norm_grad(total, lnp[2:3], xh2, rs2, layer, sg2)

        sg2[layer, 2:3, :] = jnp.sum(dres[...], axis=0, keepdims=True)
        da_g[layer, me] = dres[...].astype(BF16)
        ag_start(da_g, layer)
        acct[0:ATT, :] = jnp.zeros((ATT, SEQ), F32)

        @pl.when(low)
        def _():
            wait_w(1, 0)

        def dattn_chunk(c):
            g = da_g[layer, :, :, chunk(c, CA)].reshape(SEQ, CA)
            acct[0:ATT, :] += mm_nt(wo[:, chunk(c, CA)], g)
        ag_consume(da_g, layer, dattn_chunk)
        out_copy(3, da_g, da_o, layer).start()

        @pl.when(top)
        def _():
            load_w(1, 0)
            total = rs_finish(2)
            y_ref[...] = (res[...] + total + bias_ref[N_LAYERS - 1, 1:2]).astype(BF16)

        @pl.when(low)
        def _():
            small_start(1, 0)

        for hd in range(HEADS):
            q = qkv[layer, :, hd * HD:(hd + 1) * HD]
            k = qkv[layer, :, ATT + hd * HD:ATT + (hd + 1) * HD]
            v = qkv[layer, :, 2 * ATT + hd * HD:2 * ATT + (hd + 1) * HD]
            p = prob[layer, hd]
            d_o = acct[hd * HD:(hd + 1) * HD, :].T.astype(BF16)
            d_p = mm_nt(d_o, v)
            d_v = mm(p.T, d_o)
            pf = p.astype(F32)
            dot = jnp.sum(d_p * pf, axis=-1, keepdims=True)
            d_s = (pf * (d_p - dot) * SCALE).astype(BF16)
            dqkv[layer, :, hd * HD:(hd + 1) * HD] = mm(d_s, k).astype(BF16)
            dqkv[layer, :, ATT + hd * HD:ATT + (hd + 1) * HD] = mm(d_s.T, q).astype(BF16)
            dqkv[layer, :, 2 * ATT + hd * HD:2 * ATT + (hd + 1) * HD] = d_v.astype(BF16)
        out_copy(7, dqkv, dqkv_o, layer).start()

        @pl.when(low)
        def _():
            wait_w(0, 0)
        rs_send(1, lambda c: mm_nt(wq[chunk(c), :], dqkv[layer]).T)
        total = rs_finish(1)

        @pl.when(top)
        def _():
            load_w(0, 0)
        dres[...] = dres[...] + norm_grad(total, lnp[0:1], xh1, rs1, layer, sg1)

    small_start(0, 0)
    xg_ref[...] = dres[...].astype(BF16)
    for kind, layer in ((0, 1), (1, 1), (1, 0), (0, 0)):
        src, dst, out = ((sg1, sgr1, small1_ref), (sg2, sgr2, small2_ref))[kind]
        for copy in small_copies(kind, layer):
            copy.wait()
        out[layer] = (src[layer] + dst[layer, 0]) + (dst[layer, 1] + dst[layer, 2])
    for layer in range(N_LAYERS):
        for i, (src, dst) in enumerate(outs):
            out_copy(i, src, dst, layer).wait()


def grads_kernel(y_in, xg_in, small1_in, small2_in, bupg_in, h_h, h2_h, dm_h, da_h, a_h, act_h, dpre_h, dqkv_h,
                 y_o, xg_o, lng_o, biasg_o, wqkv_o, wo_o, wu_o, bupg_o, wd_o,
                 h, h2, dm, da, attn, act, dpre, dqkv, big, qbuf, obuf, y_v, xg_v, small1_v, small2_v, bupg_v, lng_v, biasg_v, isem, bsem, qsem, osem, psem):
    ins = [(dm_h, dm), (act_h, act), (h2_h, h2), (dpre_h, dpre), (da_h, da), (a_h, attn), (h_h, h), (dqkv_h, dqkv)]

    def in_copy(i, layer):
        return pltpu.make_async_copy(ins[i][0].at[layer], ins[i][1].at[layer], isem.at[i, layer])

    order = [(i, layer) for layer in reversed(range(N_LAYERS)) for i in range(0, len(ins), 2)]

    def prefetch(k):
        if k < len(order):
            in_copy(order[k][0], order[k][1]).start()
            in_copy(order[k][0] + 1, order[k][1]).start()

    prefetch(0)
    prefetch(1)
    small_in = [pltpu.make_async_copy(src, dst, psem.at[i]) for i, (src, dst) in enumerate(
        ((y_in, y_v), (xg_in, xg_v), (small1_in, small1_v), (small2_in, small2_v), (bupg_in, bupg_v)))]
    small_out = [pltpu.make_async_copy(src, dst, psem.at[i]) for i, (src, dst) in enumerate(
        ((y_v, y_o), (xg_v, xg_o), (lng_v, lng_o), (biasg_v, biasg_o), (bupg_v, bupg_o)))]
    for copy in small_in:
        copy.start()

    def big_copies(dst, layer, c, slot):
        return [pltpu.make_async_copy(big.at[slot, pl.ds(r * 128, 128)], dst.at[layer, pl.ds(pl.multiple_of(c * C + r * 128, 128), 128)],
                                      bsem.at[slot, r]) for r in range(C // 128)]

    def q_copies(layer, c, slot):
        return [pltpu.make_async_copy(qbuf.at[slot, pl.ds(3 * j, 3)], wqkv_o.at[layer, pl.ds(3 * j, 3), chunk(c), :], qsem.at[slot, j])
                for j in range(HEADS)]

    def o_copies(layer, c):
        return [pltpu.make_async_copy(obuf.at[c, pl.ds(r * 160, 160)], wo_o.at[layer, pl.ds(c * (ATT // 2) + r * 160, 160)], osem.at[c, r])
                for r in range(2)]

    def start(copies):
        for copy in copies:
            copy.start()

    def wait(copies):
        for copy in copies:
            copy.wait()

    for step, layer in enumerate(reversed(range(N_LAYERS))):
        for w, (dst, left, right) in enumerate(((wd_o, act, dm), (wu_o, h2, dpre))):
            in_copy(2 * w, layer).wait()
            in_copy(2 * w + 1, layer).wait()
            prefetch(4 * step + w + 2)
            base = (2 * step + w) * NC

            @pl.loop(0, NC)
            def _(c):
                slot = lax.rem(base + c, SLOTS)

                @pl.when(base + c >= SLOTS)
                def _():
                    wait(big_copies(dst, layer, c, slot))
                lt = left[layer, :, chunk(c)].T
                for n in range(0, D, C):
                    big[slot, :, n:n + C] = mm(lt, right[layer, :, n:n + C]).astype(BF16)
                start(big_copies(dst, layer, c, slot))
        if step == 0:
            for copy in small_in:
                copy.wait()
            lng_v[:, 0:2, :] = small1_v[...]
            lng_v[:, 2:4, :] = small2_v[:, 0:2, :]
            biasg_v[...] = small2_v[:, 2:4, :]
            for copy in small_out:
                copy.start()
        in_copy(4, layer).wait()
        in_copy(5, layer).wait()
        prefetch(4 * step + 4)
        for c in range(2):
            if step > 0:
                wait(o_copies(layer, c))
            lt = attn[layer, :, :].T[c * (ATT // 2):(c + 1) * (ATT // 2)]
            for n in range(0, D, C):
                obuf[c, :, n:n + C] = mm(lt, da[layer, :, n:n + C]).astype(BF16)
            start(o_copies(layer, c))
        in_copy(6, layer).wait()
        in_copy(7, layer).wait()
        prefetch(4 * step + 5)
        qbase = step * NC

        @pl.loop(0, NC)
        def _(c):
            slot = lax.rem(qbase + c, 3)

            @pl.when(qbase + c >= 3)
            def _():
                wait(q_copies(layer, c, slot))
            lt = h[layer, :, chunk(c)].T
            for n in range(0, QKV, 3 * HD):
                vals = mm(lt, dqkv[layer, :, n:n + 3 * HD]).astype(BF16)
                for j in range(3):
                    qbuf[slot, n // HD + j] = vals[:, j * HD:(j + 1) * HD]
            start(q_copies(layer, c, slot))
    for copy in small_out:
        copy.wait()
    for slot in range(SLOTS):
        wait(big_copies(wu_o, 0, 0, slot))
    for slot in range(3):
        wait(q_copies(0, 0, slot))
    for c in range(2):
        wait(o_copies(0, c))


def solution(mesh):
    vmem = pl.BlockSpec(memory_space=pltpu.VMEM)
    hbm = pl.BlockSpec(memory_space=pl.ANY)

    def device_step(x_loc, dy_loc, ln_par, bias_d, w_qkv, w_out, w_up, b_up, w_down):
        wqkv_t = jnp.transpose(w_qkv, (0, 2, 3, 1, 4)).reshape(N_LAYERS, 3 * HEADS, D, HD)
        wo_t = w_out.reshape(N_LAYERS, ATT, D)
        sds = jax.ShapeDtypeStruct
        gath = (N_LAYERS, 4, BLK, D)
        dma = pltpu.SemaphoreType.DMA
        chain_out = pl.pallas_call(
            chain_kernel,
            name='chain',
            out_shape=(sds((BLK, D), BF16), sds((BLK, D), BF16), sds((N_LAYERS, 2, D), F32), sds((N_LAYERS, 4, D), F32), sds((N_LAYERS, FF), F32),
                       sds(gath, BF16), sds(gath, BF16), sds(gath, BF16), sds(gath, BF16),
                       sds((N_LAYERS, SEQ, ATT), BF16), sds((N_LAYERS, SEQ, FF), BF16), sds((N_LAYERS, SEQ, FF), BF16),
                       sds((N_LAYERS, SEQ, QKV), BF16)),
            in_specs=[vmem] * 5 + [hbm] * 4,
            out_specs=tuple([vmem] * 5 + [hbm] * 8),
            scratch_shapes=[
                pltpu.VMEM((D, QKV), BF16), pltpu.VMEM((ATT, D), BF16), pltpu.VMEM((D, FF), BF16), pltpu.VMEM((FF, D), BF16),
                pltpu.VMEM(gath, BF16), pltpu.VMEM(gath, BF16), pltpu.VMEM(gath, BF16), pltpu.VMEM(gath, BF16),
                pltpu.VMEM((N_LAYERS, SEQ, QKV), BF16), pltpu.VMEM((N_LAYERS, HEADS, SEQ, SEQ), BF16),
                pltpu.VMEM((N_LAYERS, SEQ, ATT), BF16), pltpu.VMEM((N_LAYERS, SEQ, FF), BF16), pltpu.VMEM((SEQ, FF), F32),
                pltpu.VMEM((N_LAYERS, SEQ, FF), BF16), pltpu.VMEM((N_LAYERS, SEQ, QKV), BF16),
                pltpu.VMEM((N_LAYERS, BLK, D), F32), pltpu.VMEM((N_LAYERS, BLK, D), F32),
                pltpu.VMEM((N_LAYERS, BLK, 128), F32), pltpu.VMEM((N_LAYERS, BLK, 128), F32),
                pltpu.VMEM((BLK, D), F32), pltpu.VMEM((BLK, D), F32), pltpu.VMEM((SEQ, D), F32), pltpu.VMEM((D, SEQ), F32),
                pltpu.VMEM((2, 2, 2, BLK, D), F32), pltpu.VMEM((2, BLK, D), F32), pltpu.VMEM((3, 2, BLK, D), F32),
                pltpu.VMEM((3, BLK, D), BF16), pltpu.VMEM((2, BLK, D), BF16),
                pltpu.VMEM((N_LAYERS, 2, D), F32), pltpu.VMEM((N_LAYERS, 4, D), F32), pltpu.VMEM((N_LAYERS, 3, 2, D), F32), pltpu.VMEM((N_LAYERS, 3, 4, D), F32),
                dma((4, 3 * HEADS)), dma((8, N_LAYERS)), dma((2, 6, NA)), dma((3, 4, NC)), dma((2, N_LAYERS, 2, 3)),
            ],
            compiler_params=pltpu.CompilerParams(collective_id=0, has_side_effects=True, vmem_limit_bytes=VMEM_ALL),
        )(x_loc, dy_loc, ln_par, bias_d, b_up, wqkv_t, wo_t, w_up, w_down)
        y_loc, xg_loc, small1, small2, bupg, h, h2, dm, da, attn, act, dpre, dqkv = chain_out
        flat = (N_LAYERS, SEQ, D)
        y_out, x_grad, lng, biasg, wqkv_g, wo_g, wu_g, bupg_o, wd_g = pl.pallas_call(
            grads_kernel,
            name='grads',
            out_shape=(sds((BLK, D), BF16), sds((BLK, D), BF16), sds((N_LAYERS, 4, D), F32), sds((N_LAYERS, 2, D), F32),
                       sds((N_LAYERS, 3 * HEADS, D, HD), BF16), sds((N_LAYERS, ATT, D), BF16), sds((N_LAYERS, D, FF), BF16),
                       sds((N_LAYERS, FF), F32), sds((N_LAYERS, FF, D), BF16)),
            in_specs=[hbm] * 13,
            out_specs=tuple([hbm] * 9),
            scratch_shapes=[
                pltpu.VMEM(flat, BF16), pltpu.VMEM(flat, BF16), pltpu.VMEM(flat, BF16), pltpu.VMEM(flat, BF16),
                pltpu.VMEM((N_LAYERS, SEQ, ATT), BF16), pltpu.VMEM((N_LAYERS, SEQ, FF), BF16), pltpu.VMEM((N_LAYERS, SEQ, FF), BF16),
                pltpu.VMEM((N_LAYERS, SEQ, QKV), BF16),
                pltpu.VMEM((SLOTS, C, D), BF16), pltpu.VMEM((3, 3 * HEADS, C, HD), BF16), pltpu.VMEM((2, ATT // 2, D), BF16),
                pltpu.VMEM((BLK, D), BF16), pltpu.VMEM((BLK, D), BF16), pltpu.VMEM((N_LAYERS, 2, D), F32), pltpu.VMEM((N_LAYERS, 4, D), F32),
                pltpu.VMEM((N_LAYERS, FF), F32), pltpu.VMEM((N_LAYERS, 4, D), F32), pltpu.VMEM((N_LAYERS, 2, D), F32),
                dma((8, N_LAYERS)), dma((SLOTS, C // 128)), dma((3, HEADS)), dma((2, 2)), dma((5,)),
            ],
            compiler_params=pltpu.CompilerParams(vmem_limit_bytes=VMEM_ALL),
        )(y_loc, xg_loc, small1, small2, bupg, h.reshape(flat), h2.reshape(flat), dm.reshape(flat), da.reshape(flat), attn, act, dpre, dqkv)
        wqkv_g = jnp.transpose(wqkv_g.reshape(N_LAYERS, 3, HEADS, D, HD), (0, 3, 1, 2, 4))
        return (y_out[None], x_grad[None], lng, biasg, wqkv_g, wo_g.reshape(N_LAYERS, HEADS, HD, D), wu_g, bupg_o, wd_g)

    in_specs = (P('dp', 'tp', None), P('dp', 'tp', None), P(None, None, None), P(None, None, None),
                P(None, None, None, 'tp', None), P(None, 'tp', None, None), P(None, None, 'tp'), P(None, 'tp'), P(None, 'tp', None))
    out_specs = (P('dp', 'tp', None), P('dp', 'tp', None), P('dp', None, None), P('dp', None, None),
                 P('dp', None, None, 'tp', None), P('dp', 'tp', None, None), P('dp', None, 'tp'), P('dp', 'tp'), P('dp', 'tp', None))
    return jax.shard_map(device_step, mesh=mesh, in_specs=in_specs, out_specs=out_specs, check_vma=False)
```

```python
import jax
import jax.numpy as jnp
from jax import lax
from jax.experimental import pallas as pl
from jax.experimental.pallas import tpu as pltpu
from jax.sharding import PartitionSpec as P

MESH = pl.DeviceIdType.MESH
F32, BF16 = jnp.float32, jnp.bfloat16
N_LAYERS, SEQ, BLK, D, HEADS, HD, FF = 2, 128, 32, 2560, 5, 128, 2560
ATT = HEADS * HD
QKV = 3 * ATT
C = 512
NC = D // C
SLOTS = 4
CA = 512
NA = D // CA
ND = 0
SCALE = HD ** -0.5
GELU_K = 0.7978845608028654
GELU_C = 0.044715
VMEM_ALL = 67043328


def mm(a, b):
    return jnp.dot(a, b, preferred_element_type=F32)


def mm_nt(a, b):
    return lax.dot_general(a, b, (((1,), (1,)), ((), ())), preferred_element_type=F32)


def chunk(c, size=C):
    return pl.ds(pl.multiple_of(c * size, size), size)


def chain_kernel(x_ref, dy_ref, ln_ref, bias_ref, bup_ref, wqkv_h, wo_h, wu_h, wd_h,
                 y_ref, xg_ref, small1_ref, small2_ref, bupg_ref, h_o, h2_o, dm_o, da_o, a_o, act_o, dpre_o, dqkv_o,
                 wq, wo, wu, wd, h_g, h2_g, dm_g, da_g, qkv, prob, attn, act, gp, dpre, dqkv,
                 xh1, xh2, rs1, rs2, res, dres, acc, acct, part, own, rr, xx, ss, sg1, sg2, sgr1, sgr2,
                 wsem, osem, agsem, rssem, gsem):
    me = lax.axis_index('tp')
    x_id = lax.div(me, 2)
    core = lax.rem(me, 2)
    sib = x_id * 2 + (1 - core)
    cross = (1 - x_id) * 2 + core
    diag = (1 - x_id) * 2 + (1 - core)

    def remote(src, dst, send, recv, dev):
        return pltpu.make_async_remote_copy(src_ref=src, dst_ref=dst, send_sem=send, recv_sem=recv,
                                            device_id={'tp': dev}, device_id_type=MESH)

    def weight_copies(kind, layer):
        if kind == 0:
            return [pltpu.make_async_copy(wqkv_h.at[layer, j], wq.at[:, pl.ds(j * HD, HD)], wsem.at[0, j]) for j in range(3 * HEADS)]
        if kind == 1:
            return [pltpu.make_async_copy(wo_h.at[layer], wo, wsem.at[1, 0])]
        src, dst = ((wu_h, wu), (wd_h, wd))[kind - 2]
        return [pltpu.make_async_copy(src.at[layer, pl.ds(j * C, C)], dst.at[pl.ds(j * C, C)], wsem.at[kind, j]) for j in range(NC)]

    def load_w(kind, layer):
        for copy in weight_copies(kind, layer):
            copy.start()

    def wait_w(kind, layer):
        for copy in weight_copies(kind, layer):
            copy.wait()

    def out_copy(i, src, dst, layer):
        return pltpu.make_async_copy(src.at[layer], dst.at[layer], osem.at[i, layer])

    outs = [(h_g, h_o), (h2_g, h2_o), (dm_g, dm_o), (da_g, da_o), (attn, a_o), (act, act_o), (dpre, dpre_o), (dqkv, dqkv_o)]

    def ag_mine(g, layer, c, k, i, dev):
        mine = g.at[layer, me, :, chunk(c, CA)]
        return remote(mine, mine, agsem.at[k, i, 0], agsem.at[k, i + 1, c], dev)

    def ag_side(g, layer, c, k=0):
        return ag_mine(g, layer, c, k, 0, sib)

    def ag_across(g, layer, c, k=0):
        return ag_mine(g, layer, c, k, 2, cross)

    def ag_forward(g, layer, c, k=0):
        theirs = g.at[layer, cross, :, chunk(c, CA)]
        return remote(theirs, theirs, agsem.at[k, 4, 0], agsem.at[k, 5, c], sib)

    def ag_direct(g, layer, c, k=0):
        return ag_mine(g, layer, c, k, 4, diag)

    def ag_sent(g, layer, k=0):
        for i, dev in ((0, sib), (2, cross), (4, sib)):
            remote(g.at[layer, me], g.at[layer, me], agsem.at[k, i, 0], agsem.at[k, i + 1, 0], dev).wait_send()

    def ag_relay(g, layer, k):
        @pl.loop(0, NA)
        def _(c):
            ag_across(g, layer, c, k).wait_recv()

            @pl.when(c < NA - ND)
            def _():
                ag_forward(g, layer, c, k).start()

    def ag_finish(g, layer, k):
        @pl.loop(0, NA)
        def _(c):
            ag_side(g, layer, c, k).wait_recv()
            ag_forward(g, layer, c, k).wait_recv()
        ag_sent(g, layer, k)

    def ag_start(g, layer, k=0):
        for c in range(NA):
            ag_across(g, layer, c, k).start()
            if c >= NA - ND:
                ag_direct(g, layer, c, k).start()
        for c in range(NA):
            ag_side(g, layer, c, k).start()

    def ag_consume(g, layer, compute, lag=2):
        @pl.loop(0, NA + lag)
        def _(c):
            @pl.when(c < NA)
            def _():
                ag_across(g, layer, c).wait_recv()

            @pl.when(c < NA - ND)
            def _():
                ag_forward(g, layer, c).start()

            @pl.when(c >= lag)
            def _():
                cc = c - lag
                ag_side(g, layer, cc).wait_recv()
                ag_forward(g, layer, cc).wait_recv()
                compute(cc)

        ag_sent(g, layer)

    def rs_side(par, c):
        return remote(part.at[par // 2, :, 1 - core, :, chunk(c)], rr.at[par, :, :, chunk(c)],
                      rssem.at[par, 0, 0], rssem.at[par, 1, c], sib)

    def rs_across(par, c):
        return remote(ss.at[par // 2, :, chunk(c)], xx.at[par, :, chunk(c)], rssem.at[par, 2, 0], rssem.at[par, 3, 0], cross)

    def rs_send(par, compute, lag=2):
        buf = par // 2

        @pl.loop(0, NC + lag)
        def _(c):
            @pl.when(c < NC)
            def _():
                vals = compute(c)
                for b in range(4):
                    part[buf, b // 2, b % 2, :, chunk(c)] = vals[b * BLK:(b + 1) * BLK]
                rs_side(par, c).start()

            @pl.when(c >= lag)
            def _():
                cc = c - lag
                rs_side(par, cc).wait_recv()
                cols = chunk(cc)
                ss[buf, :, cols] = (part[buf, 1 - x_id, core, :, cols] + rr[par, 1 - x_id, :, cols]).astype(BF16)
                rs_across(par, cc).start()
                own[buf, :, cols] = part[buf, x_id, core, :, cols] + rr[par, x_id, :, cols]

    def rs_within(par, compute):
        @pl.loop(0, NC)
        def _(c):
            vals = compute(c)
            for b in range(4):
                part[par // 2, b // 2, b % 2, :, chunk(c)] = vals[b * BLK:(b + 1) * BLK]
            rs_side(par, c).start()

    def rs_cross(par):
        buf = par // 2

        @pl.loop(0, NC)
        def _(c):
            rs_side(par, c).wait_recv()
            cols = chunk(c)
            ss[buf, :, cols] = (part[buf, 1 - x_id, core, :, cols] + rr[par, 1 - x_id, :, cols]).astype(BF16)
            rs_across(par, c).start()
            own[buf, :, cols] = part[buf, x_id, core, :, cols] + rr[par, x_id, :, cols]

    def rs_finish(par):
        buf = par // 2
        remote(part.at[buf, :, 1 - core], rr.at[par], rssem.at[par, 0, 0], rssem.at[par, 1, 0], sib).wait_send()
        remote(ss.at[buf], xx.at[par], rssem.at[par, 2, 0], rssem.at[par, 3, 0], cross).wait()
        return own[buf] + xx[par].astype(F32)

    def normed(vals, gain, shift, xh, rs, layer):
        mean_val = jnp.mean(vals, axis=-1, keepdims=True)
        centered = vals - mean_val
        rstd = lax.rsqrt(jnp.mean(centered * centered, axis=-1, keepdims=True) + 1e-5)
        hat = centered * rstd
        xh[layer] = hat
        rs[layer] = jnp.broadcast_to(rstd, (BLK, 128))
        return (hat * gain + shift).astype(BF16)

    def norm_grad(d_out, gain, xh, rs, layer, rows):
        hat = xh[layer]
        rstd = rs[layer][:, :1]
        rows[layer, 0:1, :] = jnp.sum(d_out * hat, axis=0, keepdims=True)
        rows[layer, 1:2, :] = jnp.sum(d_out, axis=0, keepdims=True)
        d_hat = d_out * gain
        m1 = jnp.mean(d_hat, axis=-1, keepdims=True)
        m2 = jnp.mean(d_hat * hat, axis=-1, keepdims=True)
        return rstd * (d_hat - m1 - hat * m2)

    def small_copies(kind, layer):
        src, dst = ((sg1, sgr1), (sg2, sgr2))[kind]
        return [remote(src.at[layer], dst.at[layer, i], gsem.at[kind, layer, 0, i], gsem.at[kind, layer, 1, i], dev)
                for i, dev in enumerate((sib, cross, diag))]

    def small_start(kind, layer):
        for copy in small_copies(kind, layer):
            copy.start()

    load_w(0, 0)
    barrier = pltpu.get_barrier_semaphore()
    for dev in (sib, cross, diag):
        pl.semaphore_signal(barrier, inc=1, device_id={'tp': dev}, device_id_type=MESH)
    res[...] = x_ref[0].astype(F32)
    pl.semaphore_wait(barrier, 3)

    row_id = lax.broadcasted_iota(jnp.int32, (SEQ, SEQ), 0)
    col_id = lax.broadcasted_iota(jnp.int32, (SEQ, SEQ), 1)
    causal = row_id >= col_id

    def dact_chunk(c):
        g = dm_g[0, :, :, chunk(c, CA)].reshape(SEQ, CA)
        acct[...] += mm_nt(wd[:, chunk(c, CA)], g)

    def dact_early(layer, lo, hi):
        @pl.when(layer == N_LAYERS - 1)
        def _():
            @pl.loop(lo, hi)
            def _(c):
                acct[chunk(c), :] = mm_nt(wd[chunk(c), :], dm_g[N_LAYERS - 1].reshape(SEQ, D))

    def act_chunk(layer, c):
        pre = acc[:, chunk(c)] + bup_ref[layer:layer + 1, chunk(c)]
        t = jnp.tanh(pre * (GELU_K + (GELU_K * GELU_C) * (pre * pre)))
        act[layer, :, chunk(c)] = (pre * (0.5 + 0.5 * t)).astype(BF16)

    def slope_chunk(layer, c):
        pre = acc[:, chunk(c)] + bup_ref[layer:layer + 1, chunk(c)]
        sq = pre * pre
        t = jnp.tanh(pre * (GELU_K + (GELU_K * GELU_C) * sq))
        return (0.5 + 0.5 * t) + (pre * (1.0 - t * t)) * (0.5 * GELU_K + (1.5 * GELU_K * GELU_C) * sq)

    def dpre_chunk(layer, c, slope):
        d_pre = acct[chunk(c), :].T * slope
        bupg_ref[layer:layer + 1, chunk(c)] = jnp.sum(d_pre, axis=0, keepdims=True)
        dpre[layer, :, chunk(c)] = d_pre.astype(BF16)

    @pl.loop(0, N_LAYERS)
    def _(layer):
        first = layer == 0
        last = layer == N_LAYERS - 1
        lnp = ln_ref[layer]
        h_g[layer, me] = normed(res[...], lnp[0:1], lnp[1:2], xh1, rs1, layer)
        ag_start(h_g, layer)
        acc[...] = jnp.zeros_like(acc)
        wait_w(0, layer)

        @pl.when(first)
        def _():
            load_w(1, 0)
            load_w(2, 0)

        def qkv_chunk(c):
            h = h_g[layer, :, :, chunk(c, CA)].reshape(SEQ, CA)
            for n in range(0, QKV, 640):
                acc[:, n:n + 640] += mm(h, wq[chunk(c, CA), n:n + 640])
        ag_consume(h_g, layer, qkv_chunk)
        out_copy(0, h_g, h_o, layer).start()

        @pl.when(first)
        def _():
            load_w(0, 1)
            dm_g[N_LAYERS - 1, me] = dy_ref[0]
            ag_start(dm_g, N_LAYERS - 1, 1)

        for j in range(3 * HEADS):
            qkv[layer, :, j * HD:(j + 1) * HD] = acc[:, j * HD:(j + 1) * HD].astype(BF16)
        for hd in range(HEADS):
            q = qkv[layer, :, hd * HD:(hd + 1) * HD]
            k = qkv[layer, :, ATT + hd * HD:ATT + (hd + 1) * HD]
            v = qkv[layer, :, 2 * ATT + hd * HD:2 * ATT + (hd + 1) * HD]
            scores = jnp.where(causal, mm_nt(q, k) * SCALE, -1e30)
            e = jnp.exp(scores - jnp.max(scores, axis=-1, keepdims=True))
            p = (e / jnp.sum(e, axis=-1, keepdims=True)).astype(BF16)
            prob[layer, hd] = p
            attn[layer, :, hd * HD:(hd + 1) * HD] = mm(p, v).astype(BF16)
        out_copy(4, attn, a_o, layer).start()
        wait_w(1, layer)

        @pl.when(first)
        def _():
            load_w(3, 0)
        @pl.when(last)
        def _():
            wait_w(3, N_LAYERS - 1)
        rs_send(0, lambda c: mm(attn[layer], wo[:, chunk(c)]))
        dact_early(layer, 0, 2)

        @pl.when(first)
        def _():
            ag_relay(dm_g, N_LAYERS - 1, 1)
        total = rs_finish(0)
        res[...] = res[...] + total + bias_ref[layer, 0:1]

        @pl.when(first)
        def _():
            load_w(1, 1)
            ag_finish(dm_g, N_LAYERS - 1, 1)
            out_copy(2, dm_g, dm_o, N_LAYERS - 1).start()

        h2_g[layer, me] = normed(res[...], lnp[2:3], lnp[3:4], xh2, rs2, layer)
        ag_start(h2_g, layer)
        acc[...] = jnp.zeros_like(acc)
        wait_w(2, layer)
        dact_early(layer, 2, NC)

        def up_chunk(c):
            h = h2_g[layer, :, :, chunk(c, CA)].reshape(SEQ, CA)
            for n in range(0, FF, C):
                acc[:, n:n + C] += mm(h, wu[chunk(c, CA), n:n + C])
        ag_consume(h2_g, layer, up_chunk)
        out_copy(1, h2_g, h2_o, layer).start()

        @pl.when(first)
        def _():
            load_w(2, 1)

        @pl.when(first)
        def _():
            @pl.loop(0, FF // C)
            def _(c):
                act_chunk(0, c)
            out_copy(5, act, act_o, 0).start()
            wait_w(3, 0)
            rs_send(1, lambda c: mm(act[0], wd[:, chunk(c)]))

            @pl.loop(0, FF // C)
            def _(c):
                gp[:, chunk(c)] = slope_chunk(0, c)
            total = rs_finish(1)
            load_w(3, 1)
            res[...] = res[...] + total + bias_ref[0, 1:2]

    @pl.loop(0, FF // C)
    def _(c):
        dpre_chunk(N_LAYERS - 1, c, slope_chunk(N_LAYERS - 1, c))
    out_copy(6, dpre, dpre_o, N_LAYERS - 1).start()
    dres[...] = dy_ref[0].astype(F32)

    @pl.loop(0, N_LAYERS)
    def _(step):
        layer = N_LAYERS - 1 - step
        top = step == 0
        low = step == N_LAYERS - 1
        lnp = ln_ref[layer]
        sg2[layer, 3:4, :] = jnp.sum(dres[...], axis=0, keepdims=True)
        @pl.when(low)
        def _():
            dm_g[0, me] = dres[...].astype(BF16)
            ag_start(dm_g, 0)
            acct[...] = jnp.zeros_like(acct)
            wait_w(3, 0)
            ag_consume(dm_g, 0, dact_chunk)
            out_copy(2, dm_g, dm_o, 0).start()

        @pl.when(low)
        def _():
            @pl.loop(0, FF // C)
            def _(c):
                dpre_chunk(0, c, gp[:, chunk(c)])
            out_copy(6, dpre, dpre_o, 0).start()

        @pl.when(low)
        def _():
            small_start(0, N_LAYERS - 1)
            small_start(1, N_LAYERS - 1)
            wait_w(2, 0)
        rs_send(0, lambda c: mm_nt(wu[chunk(c), :], dpre[layer]).T)

        @pl.when(top)
        def _():
            load_w(2, 0)

            @pl.loop(0, FF // C)
            def _(c):
                act_chunk(N_LAYERS - 1, c)
            out_copy(5, act, act_o, N_LAYERS - 1).start()
            rs_within(2, lambda c: mm(act[N_LAYERS - 1], wd[:, chunk(c)]))
            load_w(3, 0)
        total = rs_finish(0)
        dres[...] = dres[...] + norm_grad(total, lnp[2:3], xh2, rs2, layer, sg2)

        sg2[layer, 2:3, :] = jnp.sum(dres[...], axis=0, keepdims=True)
        da_g[layer, me] = dres[...].astype(BF16)
        ag_start(da_g, layer)
        acct[0:ATT, :] = jnp.zeros((ATT, SEQ), F32)

        @pl.when(low)
        def _():
            wait_w(1, 0)

        def dattn_chunk(c):
            g = da_g[layer, :, :, chunk(c, CA)].reshape(SEQ, CA)
            acct[0:ATT, :] += mm_nt(wo[:, chunk(c, CA)], g)
        ag_consume(da_g, layer, dattn_chunk)
        out_copy(3, da_g, da_o, layer).start()

        @pl.when(top)
        def _():
            load_w(1, 0)
            rs_cross(2)

        @pl.when(low)
        def _():
            small_start(1, 0)

        for hd in range(HEADS):
            q = qkv[layer, :, hd * HD:(hd + 1) * HD]
            k = qkv[layer, :, ATT + hd * HD:ATT + (hd + 1) * HD]
            v = qkv[layer, :, 2 * ATT + hd * HD:2 * ATT + (hd + 1) * HD]
            p = prob[layer, hd]
            d_o = acct[hd * HD:(hd + 1) * HD, :].T.astype(BF16)
            d_p = mm_nt(d_o, v)
            d_v = mm(p.T, d_o)
            pf = p.astype(F32)
            dot = jnp.sum(d_p * pf, axis=-1, keepdims=True)
            d_s = (pf * (d_p - dot) * SCALE).astype(BF16)
            dqkv[layer, :, hd * HD:(hd + 1) * HD] = mm(d_s, k).astype(BF16)
            dqkv[layer, :, ATT + hd * HD:ATT + (hd + 1) * HD] = mm(d_s.T, q).astype(BF16)
            dqkv[layer, :, 2 * ATT + hd * HD:2 * ATT + (hd + 1) * HD] = d_v.astype(BF16)
        out_copy(7, dqkv, dqkv_o, layer).start()

        @pl.when(low)
        def _():
            wait_w(0, 0)
        rs_send(1, lambda c: mm_nt(wq[chunk(c), :], dqkv[layer]).T)

        @pl.when(top)
        def _():
            load_w(0, 0)
            y_ref[...] = (res[...] + rs_finish(2) + bias_ref[N_LAYERS - 1, 1:2]).astype(BF16)
        total = rs_finish(1)
        dres[...] = dres[...] + norm_grad(total, lnp[0:1], xh1, rs1, layer, sg1)

    small_start(0, 0)
    xg_ref[...] = dres[...].astype(BF16)
    for kind, layer in ((0, 1), (1, 1), (1, 0), (0, 0)):
        src, dst, out = ((sg1, sgr1, small1_ref), (sg2, sgr2, small2_ref))[kind]
        for copy in small_copies(kind, layer):
            copy.wait()
        out[layer] = (src[layer] + dst[layer, 0]) + (dst[layer, 1] + dst[layer, 2])
    for layer in range(N_LAYERS):
        for i, (src, dst) in enumerate(outs):
            out_copy(i, src, dst, layer).wait()


def grads_kernel(y_in, xg_in, small1_in, small2_in, bupg_in, h_h, h2_h, dm_h, da_h, a_h, act_h, dpre_h, dqkv_h,
                 y_o, xg_o, lng_o, biasg_o, wqkv_o, wo_o, wu_o, bupg_o, wd_o,
                 h, h2, dm, da, attn, act, dpre, dqkv, big, qbuf, obuf, y_v, xg_v, small1_v, small2_v, bupg_v, lng_v, biasg_v, isem, bsem, qsem, osem, psem):
    ins = [(dm_h, dm), (act_h, act), (h2_h, h2), (dpre_h, dpre), (da_h, da), (a_h, attn), (h_h, h), (dqkv_h, dqkv)]

    def in_copy(i, layer):
        return pltpu.make_async_copy(ins[i][0].at[layer], ins[i][1].at[layer], isem.at[i, layer])

    order = [(i, layer) for layer in reversed(range(N_LAYERS)) for i in range(0, len(ins), 2)]

    def prefetch(k):
        if k < len(order):
            in_copy(order[k][0], order[k][1]).start()
            in_copy(order[k][0] + 1, order[k][1]).start()

    prefetch(0)
    prefetch(1)
    small_in = [pltpu.make_async_copy(src, dst, psem.at[i]) for i, (src, dst) in enumerate(
        ((y_in, y_v), (xg_in, xg_v), (small1_in, small1_v), (small2_in, small2_v), (bupg_in, bupg_v)))]
    small_out = [pltpu.make_async_copy(src, dst, psem.at[i]) for i, (src, dst) in enumerate(
        ((y_v, y_o), (xg_v, xg_o), (lng_v, lng_o), (biasg_v, biasg_o), (bupg_v, bupg_o)))]
    for copy in small_in:
        copy.start()

    def big_copies(dst, layer, c, slot):
        return [pltpu.make_async_copy(big.at[slot, pl.ds(r * 128, 128)], dst.at[layer, pl.ds(pl.multiple_of(c * C + r * 128, 128), 128)],
                                      bsem.at[slot, r]) for r in range(C // 128)]

    def q_copies(layer, c, slot):
        return [pltpu.make_async_copy(qbuf.at[slot, pl.ds(3 * j, 3)], wqkv_o.at[layer, pl.ds(3 * j, 3), chunk(c), :], qsem.at[slot, j])
                for j in range(HEADS)]

    def o_copies(layer, c):
        return [pltpu.make_async_copy(obuf.at[c, pl.ds(r * 160, 160)], wo_o.at[layer, pl.ds(c * (ATT // 2) + r * 160, 160)], osem.at[c, r])
                for r in range(2)]

    def start(copies):
        for copy in copies:
            copy.start()

    def wait(copies):
        for copy in copies:
            copy.wait()

    for step, layer in enumerate(reversed(range(N_LAYERS))):
        for w, (dst, left, right) in enumerate(((wd_o, act, dm), (wu_o, h2, dpre))):
            in_copy(2 * w, layer).wait()
            in_copy(2 * w + 1, layer).wait()
            prefetch(4 * step + w + 2)
            base = (2 * step + w) * NC

            @pl.loop(0, NC)
            def _(c):
                slot = lax.rem(base + c, SLOTS)

                @pl.when(base + c >= SLOTS)
                def _():
                    wait(big_copies(dst, layer, c, slot))
                lt = left[layer, :, chunk(c)].T
                for n in range(0, D, C):
                    big[slot, :, n:n + C] = mm(lt, right[layer, :, n:n + C]).astype(BF16)
                start(big_copies(dst, layer, c, slot))
        if step == 0:
            for copy in small_in:
                copy.wait()
            lng_v[:, 0:2, :] = small1_v[...]
            lng_v[:, 2:4, :] = small2_v[:, 0:2, :]
            biasg_v[...] = small2_v[:, 2:4, :]
            for copy in small_out:
                copy.start()
        in_copy(4, layer).wait()
        in_copy(5, layer).wait()
        prefetch(4 * step + 4)
        for c in range(2):
            if step > 0:
                wait(o_copies(layer, c))
            lt = attn[layer, :, :].T[c * (ATT // 2):(c + 1) * (ATT // 2)]
            for n in range(0, D, C):
                obuf[c, :, n:n + C] = mm(lt, da[layer, :, n:n + C]).astype(BF16)
            start(o_copies(layer, c))
        in_copy(6, layer).wait()
        in_copy(7, layer).wait()
        prefetch(4 * step + 5)
        qbase = step * NC

        @pl.loop(0, NC)
        def _(c):
            slot = lax.rem(qbase + c, 3)

            @pl.when(qbase + c >= 3)
            def _():
                wait(q_copies(layer, c, slot))
            lt = h[layer, :, chunk(c)].T
            for n in range(0, QKV, 3 * HD):
                vals = mm(lt, dqkv[layer, :, n:n + 3 * HD]).astype(BF16)
                for j in range(3):
                    qbuf[slot, n // HD + j] = vals[:, j * HD:(j + 1) * HD]
            start(q_copies(layer, c, slot))
    for copy in small_out:
        copy.wait()
    for slot in range(SLOTS):
        wait(big_copies(wu_o, 0, 0, slot))
    for slot in range(3):
        wait(q_copies(0, 0, slot))
    for c in range(2):
        wait(o_copies(0, c))


def solution(mesh):
    vmem = pl.BlockSpec(memory_space=pltpu.VMEM)
    hbm = pl.BlockSpec(memory_space=pl.ANY)

    def device_step(x_loc, dy_loc, ln_par, bias_d, w_qkv, w_out, w_up, b_up, w_down):
        wqkv_t = jnp.transpose(w_qkv, (0, 2, 3, 1, 4)).reshape(N_LAYERS, 3 * HEADS, D, HD)
        wo_t = w_out.reshape(N_LAYERS, ATT, D)
        sds = jax.ShapeDtypeStruct
        gath = (N_LAYERS, 4, BLK, D)
        dma = pltpu.SemaphoreType.DMA
        chain_out = pl.pallas_call(
            chain_kernel,
            name='chain',
            out_shape=(sds((BLK, D), BF16), sds((BLK, D), BF16), sds((N_LAYERS, 2, D), F32), sds((N_LAYERS, 4, D), F32), sds((N_LAYERS, FF), F32),
                       sds(gath, BF16), sds(gath, BF16), sds(gath, BF16), sds(gath, BF16),
                       sds((N_LAYERS, SEQ, ATT), BF16), sds((N_LAYERS, SEQ, FF), BF16), sds((N_LAYERS, SEQ, FF), BF16),
                       sds((N_LAYERS, SEQ, QKV), BF16)),
            in_specs=[vmem] * 5 + [hbm] * 4,
            out_specs=tuple([vmem] * 5 + [hbm] * 8),
            scratch_shapes=[
                pltpu.VMEM((D, QKV), BF16), pltpu.VMEM((ATT, D), BF16), pltpu.VMEM((D, FF), BF16), pltpu.VMEM((FF, D), BF16),
                pltpu.VMEM(gath, BF16), pltpu.VMEM(gath, BF16), pltpu.VMEM(gath, BF16), pltpu.VMEM(gath, BF16),
                pltpu.VMEM((N_LAYERS, SEQ, QKV), BF16), pltpu.VMEM((N_LAYERS, HEADS, SEQ, SEQ), BF16),
                pltpu.VMEM((N_LAYERS, SEQ, ATT), BF16), pltpu.VMEM((N_LAYERS, SEQ, FF), BF16), pltpu.VMEM((SEQ, FF), F32),
                pltpu.VMEM((N_LAYERS, SEQ, FF), BF16), pltpu.VMEM((N_LAYERS, SEQ, QKV), BF16),
                pltpu.VMEM((N_LAYERS, BLK, D), F32), pltpu.VMEM((N_LAYERS, BLK, D), F32),
                pltpu.VMEM((N_LAYERS, BLK, 128), F32), pltpu.VMEM((N_LAYERS, BLK, 128), F32),
                pltpu.VMEM((BLK, D), F32), pltpu.VMEM((BLK, D), F32), pltpu.VMEM((SEQ, D), F32), pltpu.VMEM((D, SEQ), F32),
                pltpu.VMEM((2, 2, 2, BLK, D), F32), pltpu.VMEM((2, BLK, D), F32), pltpu.VMEM((3, 2, BLK, D), F32),
                pltpu.VMEM((3, BLK, D), BF16), pltpu.VMEM((2, BLK, D), BF16),
                pltpu.VMEM((N_LAYERS, 2, D), F32), pltpu.VMEM((N_LAYERS, 4, D), F32), pltpu.VMEM((N_LAYERS, 3, 2, D), F32), pltpu.VMEM((N_LAYERS, 3, 4, D), F32),
                dma((4, 3 * HEADS)), dma((8, N_LAYERS)), dma((2, 6, NA)), dma((3, 4, NC)), dma((2, N_LAYERS, 2, 3)),
            ],
            compiler_params=pltpu.CompilerParams(collective_id=0, has_side_effects=True, vmem_limit_bytes=VMEM_ALL),
        )(x_loc, dy_loc, ln_par, bias_d, b_up, wqkv_t, wo_t, w_up, w_down)
        y_loc, xg_loc, small1, small2, bupg, h, h2, dm, da, attn, act, dpre, dqkv = chain_out
        flat = (N_LAYERS, SEQ, D)
        y_out, x_grad, lng, biasg, wqkv_g, wo_g, wu_g, bupg_o, wd_g = pl.pallas_call(
            grads_kernel,
            name='grads',
            out_shape=(sds((BLK, D), BF16), sds((BLK, D), BF16), sds((N_LAYERS, 4, D), F32), sds((N_LAYERS, 2, D), F32),
                       sds((N_LAYERS, 3 * HEADS, D, HD), BF16), sds((N_LAYERS, ATT, D), BF16), sds((N_LAYERS, D, FF), BF16),
                       sds((N_LAYERS, FF), F32), sds((N_LAYERS, FF, D), BF16)),
            in_specs=[hbm] * 13,
            out_specs=tuple([hbm] * 9),
            scratch_shapes=[
                pltpu.VMEM(flat, BF16), pltpu.VMEM(flat, BF16), pltpu.VMEM(flat, BF16), pltpu.VMEM(flat, BF16),
                pltpu.VMEM((N_LAYERS, SEQ, ATT), BF16), pltpu.VMEM((N_LAYERS, SEQ, FF), BF16), pltpu.VMEM((N_LAYERS, SEQ, FF), BF16),
                pltpu.VMEM((N_LAYERS, SEQ, QKV), BF16),
                pltpu.VMEM((SLOTS, C, D), BF16), pltpu.VMEM((3, 3 * HEADS, C, HD), BF16), pltpu.VMEM((2, ATT // 2, D), BF16),
                pltpu.VMEM((BLK, D), BF16), pltpu.VMEM((BLK, D), BF16), pltpu.VMEM((N_LAYERS, 2, D), F32), pltpu.VMEM((N_LAYERS, 4, D), F32),
                pltpu.VMEM((N_LAYERS, FF), F32), pltpu.VMEM((N_LAYERS, 4, D), F32), pltpu.VMEM((N_LAYERS, 2, D), F32),
                dma((8, N_LAYERS)), dma((SLOTS, C // 128)), dma((3, HEADS)), dma((2, 2)), dma((5,)),
            ],
            compiler_params=pltpu.CompilerParams(vmem_limit_bytes=VMEM_ALL),
        )(y_loc, xg_loc, small1, small2, bupg, h.reshape(flat), h2.reshape(flat), dm.reshape(flat), da.reshape(flat), attn, act, dpre, dqkv)
        wqkv_g = jnp.transpose(wqkv_g.reshape(N_LAYERS, 3, HEADS, D, HD), (0, 3, 1, 2, 4))
        return (y_out[None], x_grad[None], lng, biasg, wqkv_g, wo_g.reshape(N_LAYERS, HEADS, HD, D), wu_g, bupg_o, wd_g)

    in_specs = (P('dp', 'tp', None), P('dp', 'tp', None), P(None, None, None), P(None, None, None),
                P(None, None, None, 'tp', None), P(None, 'tp', None, None), P(None, None, 'tp'), P(None, 'tp'), P(None, 'tp', None))
    out_specs = (P('dp', 'tp', None), P('dp', 'tp', None), P('dp', None, None), P('dp', None, None),
                 P('dp', None, None, 'tp', None), P('dp', 'tp', None, None), P('dp', None, 'tp'), P('dp', 'tp'), P('dp', 'tp', None))
    return jax.shard_map(device_step, mesh=mesh, in_specs=in_specs, out_specs=out_specs, check_vma=False)
```

```python
import jax
import jax.numpy as jnp
from jax import lax
from jax.experimental import pallas as pl
from jax.experimental.pallas import tpu as pltpu
from jax.sharding import PartitionSpec as P

MESH = pl.DeviceIdType.MESH
F32, BF16 = jnp.float32, jnp.bfloat16
N_LAYERS, SEQ, BLK, D, HEADS, HD, FF = 2, 128, 32, 2560, 5, 128, 2560
ATT = HEADS * HD
QKV = 3 * ATT
C = 512
NC = D // C
SLOTS = 4
CA = 512
NA = D // CA
ND = 0
SCALE = HD ** -0.5
GELU_K = 0.7978845608028654
GELU_C = 0.044715
VMEM_ALL = 67043328


def mm(a, b):
    return jnp.dot(a, b, preferred_element_type=F32)


def mm_nt(a, b):
    return lax.dot_general(a, b, (((1,), (1,)), ((), ())), preferred_element_type=F32)


def chunk(c, size=C):
    return pl.ds(pl.multiple_of(c * size, size), size)


def chain_kernel(x_ref, dy_ref, ln_ref, bias_ref, bup_ref, wqkv_h, wo_h, wu_h, wd_h,
                 y_ref, xg_ref, small1_ref, small2_ref, bupg_ref, h_o, h2_o, dm_o, da_o, a_o, act_o, dpre_o, dqkv_o,
                 wq, wo, wu, wd, h_g, h2_g, dm_g, da_g, qkv, prob, attn, act, gp, dpre, dqkv,
                 xh1, xh2, rs1, rs2, res, dres, acc, acct, part, own, rr, xx, ss, sg1, sg2, sgr1, sgr2,
                 wsem, osem, agsem, rssem, gsem):
    me = lax.axis_index('tp')
    x_id = lax.div(me, 2)
    core = lax.rem(me, 2)
    sib = x_id * 2 + (1 - core)
    cross = (1 - x_id) * 2 + core
    diag = (1 - x_id) * 2 + (1 - core)

    def remote(src, dst, send, recv, dev):
        return pltpu.make_async_remote_copy(src_ref=src, dst_ref=dst, send_sem=send, recv_sem=recv,
                                            device_id={'tp': dev}, device_id_type=MESH)

    def weight_copies(kind, layer):
        if kind == 0:
            return [pltpu.make_async_copy(wqkv_h.at[layer, j], wq.at[:, pl.ds(j * HD, HD)], wsem.at[0, j]) for j in range(3 * HEADS)]
        if kind == 1:
            return [pltpu.make_async_copy(wo_h.at[layer], wo, wsem.at[1, 0])]
        src, dst = ((wu_h, wu), (wd_h, wd))[kind - 2]
        return [pltpu.make_async_copy(src.at[layer, pl.ds(j * C, C)], dst.at[pl.ds(j * C, C)], wsem.at[kind, j]) for j in range(NC)]

    def load_w(kind, layer):
        for copy in weight_copies(kind, layer):
            copy.start()

    def wait_w(kind, layer):
        for copy in weight_copies(kind, layer):
            copy.wait()

    def out_copy(i, src, dst, layer):
        return pltpu.make_async_copy(src.at[layer], dst.at[layer], osem.at[i, layer])

    outs = [(h_g, h_o), (h2_g, h2_o), (dm_g, dm_o), (da_g, da_o), (attn, a_o), (act, act_o), (dpre, dpre_o), (dqkv, dqkv_o)]

    def ag_mine(g, layer, c, k, i, dev):
        mine = g.at[layer, me, :, chunk(c, CA)]
        return remote(mine, mine, agsem.at[k, i, 0], agsem.at[k, i + 1, c], dev)

    def ag_side(g, layer, c, k=0):
        return ag_mine(g, layer, c, k, 0, sib)

    def ag_across(g, layer, c, k=0):
        return ag_mine(g, layer, c, k, 2, cross)

    def ag_forward(g, layer, c, k=0):
        theirs = g.at[layer, cross, :, chunk(c, CA)]
        return remote(theirs, theirs, agsem.at[k, 4, 0], agsem.at[k, 5, c], sib)

    def ag_direct(g, layer, c, k=0):
        return ag_mine(g, layer, c, k, 4, diag)

    def ag_sent(g, layer, k=0):
        for i, dev in ((0, sib), (2, cross), (4, sib)):
            remote(g.at[layer, me], g.at[layer, me], agsem.at[k, i, 0], agsem.at[k, i + 1, 0], dev).wait_send()

    def ag_relay(g, layer, k):
        @pl.loop(0, NA)
        def _(c):
            ag_across(g, layer, c, k).wait_recv()

            @pl.when(c < NA - ND)
            def _():
                ag_forward(g, layer, c, k).start()

    def ag_finish(g, layer, k):
        @pl.loop(0, NA)
        def _(c):
            ag_side(g, layer, c, k).wait_recv()
            ag_forward(g, layer, c, k).wait_recv()
        ag_sent(g, layer, k)

    def ag_start(g, layer, k=0):
        for c in range(NA):
            ag_across(g, layer, c, k).start()
            if c >= NA - ND:
                ag_direct(g, layer, c, k).start()
        for c in range(NA):
            ag_side(g, layer, c, k).start()

    def ag_consume(g, layer, compute, lag=2):
        @pl.loop(0, NA + lag)
        def _(c):
            @pl.when(c < NA)
            def _():
                ag_across(g, layer, c).wait_recv()

            @pl.when(c < NA - ND)
            def _():
                ag_forward(g, layer, c).start()

            @pl.when(c >= lag)
            def _():
                cc = c - lag
                ag_side(g, layer, cc).wait_recv()
                ag_forward(g, layer, cc).wait_recv()
                compute(cc)

        ag_sent(g, layer)

    def rs_side(par, c):
        return remote(part.at[par // 2, :, 1 - core, :, chunk(c)], rr.at[par, :, :, chunk(c)],
                      rssem.at[par, 0, 0], rssem.at[par, 1, c], sib)

    def rs_across(par, c):
        return remote(ss.at[par // 2, :, chunk(c)], xx.at[par, :, chunk(c)], rssem.at[par, 2, 0], rssem.at[par, 3, 0], cross)

    def rs_send(par, compute, lag=2):
        buf = par // 2

        @pl.loop(0, NC + lag)
        def _(c):
            @pl.when(c < NC)
            def _():
                vals = compute(c)
                for b in range(4):
                    part[buf, b // 2, b % 2, :, chunk(c)] = vals[b * BLK:(b + 1) * BLK]
                rs_side(par, c).start()

            @pl.when(c >= lag)
            def _():
                cc = c - lag
                rs_side(par, cc).wait_recv()
                cols = chunk(cc)
                ss[buf, :, cols] = (part[buf, 1 - x_id, core, :, cols] + rr[par, 1 - x_id, :, cols]).astype(BF16)
                rs_across(par, cc).start()
                own[buf, :, cols] = part[buf, x_id, core, :, cols] + rr[par, x_id, :, cols]

    def rs_within(par, compute):
        @pl.loop(0, NC)
        def _(c):
            vals = compute(c)
            for b in range(4):
                part[par // 2, b // 2, b % 2, :, chunk(c)] = vals[b * BLK:(b + 1) * BLK]
            rs_side(par, c).start()

    def rs_cross(par):
        buf = par // 2

        @pl.loop(0, NC)
        def _(c):
            rs_side(par, c).wait_recv()
            cols = chunk(c)
            ss[buf, :, cols] = (part[buf, 1 - x_id, core, :, cols] + rr[par, 1 - x_id, :, cols]).astype(BF16)
            rs_across(par, c).start()
            own[buf, :, cols] = part[buf, x_id, core, :, cols] + rr[par, x_id, :, cols]

    def rs_finish(par):
        buf = par // 2
        remote(part.at[buf, :, 1 - core], rr.at[par], rssem.at[par, 0, 0], rssem.at[par, 1, 0], sib).wait_send()
        remote(ss.at[buf], xx.at[par], rssem.at[par, 2, 0], rssem.at[par, 3, 0], cross).wait()
        return own[buf] + xx[par].astype(F32)

    def normed(vals, gain, shift, xh, rs, layer):
        mean_val = jnp.mean(vals, axis=-1, keepdims=True)
        centered = vals - mean_val
        rstd = lax.rsqrt(jnp.mean(centered * centered, axis=-1, keepdims=True) + 1e-5)
        hat = centered * rstd
        xh[layer] = hat
        rs[layer] = jnp.broadcast_to(rstd, (BLK, 128))
        return (hat * gain + shift).astype(BF16)

    def norm_grad(d_out, gain, xh, rs, layer, rows):
        hat = xh[layer]
        rstd = rs[layer][:, :1]
        rows[layer, 0:1, :] = jnp.sum(d_out * hat, axis=0, keepdims=True)
        rows[layer, 1:2, :] = jnp.sum(d_out, axis=0, keepdims=True)
        d_hat = d_out * gain
        m1 = jnp.mean(d_hat, axis=-1, keepdims=True)
        m2 = jnp.mean(d_hat * hat, axis=-1, keepdims=True)
        return rstd * (d_hat - m1 - hat * m2)

    def small_copies(kind, layer):
        src, dst = ((sg1, sgr1), (sg2, sgr2))[kind]
        return [remote(src.at[layer], dst.at[layer, i], gsem.at[kind, layer, 0, i], gsem.at[kind, layer, 1, i], dev)
                for i, dev in enumerate((sib, cross, diag))]

    def small_start(kind, layer):
        for copy in small_copies(kind, layer):
            copy.start()

    load_w(0, 0)
    barrier = pltpu.get_barrier_semaphore()
    for dev in (sib, cross, diag):
        pl.semaphore_signal(barrier, inc=1, device_id={'tp': dev}, device_id_type=MESH)
    res[...] = x_ref[0].astype(F32)
    pl.semaphore_wait(barrier, 3)

    row_id = lax.broadcasted_iota(jnp.int32, (SEQ, SEQ), 0)
    col_id = lax.broadcasted_iota(jnp.int32, (SEQ, SEQ), 1)
    causal = row_id >= col_id

    def dact_chunk(c):
        g = dm_g[0, :, :, chunk(c, CA)].reshape(SEQ, CA)
        acct[...] += mm_nt(wd[:, chunk(c, CA)], g)

    def dact_early(layer, lo, hi):
        @pl.when(layer == N_LAYERS - 1)
        def _():
            @pl.loop(lo, hi)
            def _(c):
                acct[chunk(c), :] = mm_nt(wd[chunk(c), :], dm_g[N_LAYERS - 1].reshape(SEQ, D))

    def act_chunk(layer, c):
        pre = acc[:, chunk(c)] + bup_ref[layer:layer + 1, chunk(c)]
        t = jnp.tanh(pre * (GELU_K + (GELU_K * GELU_C) * (pre * pre)))
        act[layer, :, chunk(c)] = (pre * (0.5 + 0.5 * t)).astype(BF16)

    def slope_chunk(layer, c):
        pre = acc[:, chunk(c)] + bup_ref[layer:layer + 1, chunk(c)]
        sq = pre * pre
        t = jnp.tanh(pre * (GELU_K + (GELU_K * GELU_C) * sq))
        return (0.5 + 0.5 * t) + (pre * (1.0 - t * t)) * (0.5 * GELU_K + (1.5 * GELU_K * GELU_C) * sq)

    def dpre_chunk(layer, c, slope):
        d_pre = acct[chunk(c), :].T * slope
        bupg_ref[layer:layer + 1, chunk(c)] = jnp.sum(d_pre, axis=0, keepdims=True)
        dpre[layer, :, chunk(c)] = d_pre.astype(BF16)

    @pl.loop(0, N_LAYERS)
    def _(layer):
        first = layer == 0
        last = layer == N_LAYERS - 1
        lnp = ln_ref[layer]
        h_g[layer, me] = normed(res[...], lnp[0:1], lnp[1:2], xh1, rs1, layer)
        ag_start(h_g, layer)

        @pl.when(first)
        def _():
            dm_g[N_LAYERS - 1, me] = dy_ref[0]
            ag_start(dm_g, N_LAYERS - 1, 1)
        acc[...] = jnp.zeros_like(acc)
        wait_w(0, layer)

        @pl.when(first)
        def _():
            load_w(1, 0)
            load_w(2, 0)

        def qkv_chunk(c):
            h = h_g[layer, :, :, chunk(c, CA)].reshape(SEQ, CA)
            for n in range(0, QKV, 640):
                acc[:, n:n + 640] += mm(h, wq[chunk(c, CA), n:n + 640])
        ag_consume(h_g, layer, qkv_chunk)
        out_copy(0, h_g, h_o, layer).start()

        @pl.when(first)
        def _():
            load_w(0, 1)

        for j in range(3 * HEADS):
            qkv[layer, :, j * HD:(j + 1) * HD] = acc[:, j * HD:(j + 1) * HD].astype(BF16)
        for hd in range(HEADS):
            q = qkv[layer, :, hd * HD:(hd + 1) * HD]
            k = qkv[layer, :, ATT + hd * HD:ATT + (hd + 1) * HD]
            v = qkv[layer, :, 2 * ATT + hd * HD:2 * ATT + (hd + 1) * HD]
            scores = jnp.where(causal, mm_nt(q, k) * SCALE, -1e30)
            e = jnp.exp(scores - jnp.max(scores, axis=-1, keepdims=True))
            p = (e / jnp.sum(e, axis=-1, keepdims=True)).astype(BF16)
            prob[layer, hd] = p
            attn[layer, :, hd * HD:(hd + 1) * HD] = mm(p, v).astype(BF16)
        out_copy(4, attn, a_o, layer).start()
        wait_w(1, layer)

        @pl.when(first)
        def _():
            load_w(3, 0)
        @pl.when(last)
        def _():
            wait_w(3, N_LAYERS - 1)
        rs_send(0, lambda c: mm(attn[layer], wo[:, chunk(c)]))
        dact_early(layer, 0, 2)

        @pl.when(first)
        def _():
            ag_relay(dm_g, N_LAYERS - 1, 1)
        total = rs_finish(0)
        res[...] = res[...] + total + bias_ref[layer, 0:1]

        @pl.when(first)
        def _():
            load_w(1, 1)
            ag_finish(dm_g, N_LAYERS - 1, 1)
            out_copy(2, dm_g, dm_o, N_LAYERS - 1).start()

        h2_g[layer, me] = normed(res[...], lnp[2:3], lnp[3:4], xh2, rs2, layer)
        ag_start(h2_g, layer)
        acc[...] = jnp.zeros_like(acc)
        wait_w(2, layer)
        dact_early(layer, 2, NC)

        def up_chunk(c):
            h = h2_g[layer, :, :, chunk(c, CA)].reshape(SEQ, CA)
            for n in range(0, FF, C):
                acc[:, n:n + C] += mm(h, wu[chunk(c, CA), n:n + C])
        ag_consume(h2_g, layer, up_chunk)
        out_copy(1, h2_g, h2_o, layer).start()

        @pl.when(first)
        def _():
            load_w(2, 1)

        @pl.when(first)
        def _():
            @pl.loop(0, FF // C)
            def _(c):
                act_chunk(0, c)
            out_copy(5, act, act_o, 0).start()
            wait_w(3, 0)
            rs_send(1, lambda c: mm(act[0], wd[:, chunk(c)]))

            @pl.loop(0, FF // C)
            def _(c):
                gp[:, chunk(c)] = slope_chunk(0, c)
            total = rs_finish(1)
            load_w(3, 1)
            res[...] = res[...] + total + bias_ref[0, 1:2]

    @pl.loop(0, FF // C)
    def _(c):
        dpre_chunk(N_LAYERS - 1, c, slope_chunk(N_LAYERS - 1, c))
    out_copy(6, dpre, dpre_o, N_LAYERS - 1).start()
    dres[...] = dy_ref[0].astype(F32)

    @pl.loop(0, N_LAYERS)
    def _(step):
        layer = N_LAYERS - 1 - step
        top = step == 0
        low = step == N_LAYERS - 1
        lnp = ln_ref[layer]
        sg2[layer, 3:4, :] = jnp.sum(dres[...], axis=0, keepdims=True)
        @pl.when(low)
        def _():
            dm_g[0, me] = dres[...].astype(BF16)
            ag_start(dm_g, 0)
            small_start(0, N_LAYERS - 1)
            small_start(1, N_LAYERS - 1)
            acct[...] = jnp.zeros_like(acct)
            wait_w(3, 0)
            ag_consume(dm_g, 0, dact_chunk)
            out_copy(2, dm_g, dm_o, 0).start()

        @pl.when(low)
        def _():
            @pl.loop(0, FF // C)
            def _(c):
                dpre_chunk(0, c, gp[:, chunk(c)])
            out_copy(6, dpre, dpre_o, 0).start()

        @pl.when(low)
        def _():
            wait_w(2, 0)
        rs_send(0, lambda c: mm_nt(wu[chunk(c), :], dpre[layer]).T)

        @pl.when(top)
        def _():
            load_w(2, 0)

            @pl.loop(0, FF // C)
            def _(c):
                act_chunk(N_LAYERS - 1, c)
            out_copy(5, act, act_o, N_LAYERS - 1).start()
            rs_within(2, lambda c: mm(act[N_LAYERS - 1], wd[:, chunk(c)]))
            load_w(3, 0)
        total = rs_finish(0)
        dres[...] = dres[...] + norm_grad(total, lnp[2:3], xh2, rs2, layer, sg2)

        sg2[layer, 2:3, :] = jnp.sum(dres[...], axis=0, keepdims=True)
        da_g[layer, me] = dres[...].astype(BF16)
        ag_start(da_g, layer)

        @pl.when(top)
        def _():
            rs_cross(2)

        @pl.when(low)
        def _():
            small_start(1, 0)
        acct[0:ATT, :] = jnp.zeros((ATT, SEQ), F32)

        @pl.when(low)
        def _():
            wait_w(1, 0)

        def dattn_chunk(c):
            g = da_g[layer, :, :, chunk(c, CA)].reshape(SEQ, CA)
            acct[0:ATT, :] += mm_nt(wo[:, chunk(c, CA)], g)
        ag_consume(da_g, layer, dattn_chunk)
        out_copy(3, da_g, da_o, layer).start()

        @pl.when(top)
        def _():
            load_w(1, 0)

        for hd in range(HEADS):
            q = qkv[layer, :, hd * HD:(hd + 1) * HD]
            k = qkv[layer, :, ATT + hd * HD:ATT + (hd + 1) * HD]
            v = qkv[layer, :, 2 * ATT + hd * HD:2 * ATT + (hd + 1) * HD]
            p = prob[layer, hd]
            d_o = acct[hd * HD:(hd + 1) * HD, :].T.astype(BF16)
            d_p = mm_nt(d_o, v)
            d_v = mm(p.T, d_o)
            pf = p.astype(F32)
            dot = jnp.sum(d_p * pf, axis=-1, keepdims=True)
            d_s = (pf * (d_p - dot) * SCALE).astype(BF16)
            dqkv[layer, :, hd * HD:(hd + 1) * HD] = mm(d_s, k).astype(BF16)
            dqkv[layer, :, ATT + hd * HD:ATT + (hd + 1) * HD] = mm(d_s.T, q).astype(BF16)
            dqkv[layer, :, 2 * ATT + hd * HD:2 * ATT + (hd + 1) * HD] = d_v.astype(BF16)
        out_copy(7, dqkv, dqkv_o, layer).start()

        @pl.when(low)
        def _():
            wait_w(0, 0)
        rs_send(1, lambda c: mm_nt(wq[chunk(c), :], dqkv[layer]).T)

        @pl.when(top)
        def _():
            load_w(0, 0)
            y_ref[...] = (res[...] + rs_finish(2) + bias_ref[N_LAYERS - 1, 1:2]).astype(BF16)
        total = rs_finish(1)
        dres[...] = dres[...] + norm_grad(total, lnp[0:1], xh1, rs1, layer, sg1)

    small_start(0, 0)
    xg_ref[...] = dres[...].astype(BF16)
    for kind, layer in ((0, 1), (1, 1), (1, 0), (0, 0)):
        src, dst, out = ((sg1, sgr1, small1_ref), (sg2, sgr2, small2_ref))[kind]
        for copy in small_copies(kind, layer):
            copy.wait()
        out[layer] = (src[layer] + dst[layer, 0]) + (dst[layer, 1] + dst[layer, 2])
    for layer in range(N_LAYERS):
        for i, (src, dst) in enumerate(outs):
            out_copy(i, src, dst, layer).wait()


def grads_kernel(y_in, xg_in, small1_in, small2_in, bupg_in, h_h, h2_h, dm_h, da_h, a_h, act_h, dpre_h, dqkv_h,
                 y_o, xg_o, lng_o, biasg_o, wqkv_o, wo_o, wu_o, bupg_o, wd_o,
                 h, h2, dm, da, attn, act, dpre, dqkv, big, qbuf, obuf, y_v, xg_v, small1_v, small2_v, bupg_v, lng_v, biasg_v, isem, bsem, qsem, osem, psem):
    ins = [(dm_h, dm), (act_h, act), (h2_h, h2), (dpre_h, dpre), (da_h, da), (a_h, attn), (h_h, h), (dqkv_h, dqkv)]

    def in_copy(i, layer):
        return pltpu.make_async_copy(ins[i][0].at[layer], ins[i][1].at[layer], isem.at[i, layer])

    order = [(i, layer) for layer in reversed(range(N_LAYERS)) for i in range(0, len(ins), 2)]

    def prefetch(k):
        if k < len(order):
            in_copy(order[k][0], order[k][1]).start()
            in_copy(order[k][0] + 1, order[k][1]).start()

    prefetch(0)
    prefetch(1)
    small_in = [pltpu.make_async_copy(src, dst, psem.at[i]) for i, (src, dst) in enumerate(
        ((y_in, y_v), (xg_in, xg_v), (small1_in, small1_v), (small2_in, small2_v), (bupg_in, bupg_v)))]
    small_out = [pltpu.make_async_copy(src, dst, psem.at[i]) for i, (src, dst) in enumerate(
        ((y_v, y_o), (xg_v, xg_o), (lng_v, lng_o), (biasg_v, biasg_o), (bupg_v, bupg_o)))]
    for copy in small_in:
        copy.start()

    def big_copies(dst, layer, c, slot):
        return [pltpu.make_async_copy(big.at[slot, pl.ds(r * 128, 128)], dst.at[layer, pl.ds(pl.multiple_of(c * C + r * 128, 128), 128)],
                                      bsem.at[slot, r]) for r in range(C // 128)]

    def q_copies(layer, c, slot):
        return [pltpu.make_async_copy(qbuf.at[slot, pl.ds(3 * j, 3)], wqkv_o.at[layer, pl.ds(3 * j, 3), chunk(c), :], qsem.at[slot, j])
                for j in range(HEADS)]

    def o_copies(layer, c):
        return [pltpu.make_async_copy(obuf.at[c, pl.ds(r * 160, 160)], wo_o.at[layer, pl.ds(c * (ATT // 2) + r * 160, 160)], osem.at[c, r])
                for r in range(2)]

    def start(copies):
        for copy in copies:
            copy.start()

    def wait(copies):
        for copy in copies:
            copy.wait()

    for step, layer in enumerate(reversed(range(N_LAYERS))):
        for w, (dst, left, right) in enumerate(((wd_o, act, dm), (wu_o, h2, dpre))):
            in_copy(2 * w, layer).wait()
            in_copy(2 * w + 1, layer).wait()
            prefetch(4 * step + w + 2)
            base = (2 * step + w) * NC

            @pl.loop(0, NC)
            def _(c):
                slot = lax.rem(base + c, SLOTS)

                @pl.when(base + c >= SLOTS)
                def _():
                    wait(big_copies(dst, layer, c, slot))
                lt = left[layer, :, chunk(c)].T
                for n in range(0, D, C):
                    big[slot, :, n:n + C] = mm(lt, right[layer, :, n:n + C]).astype(BF16)
                start(big_copies(dst, layer, c, slot))
        if step == 0:
            for copy in small_in:
                copy.wait()
            lng_v[:, 0:2, :] = small1_v[...]
            lng_v[:, 2:4, :] = small2_v[:, 0:2, :]
            biasg_v[...] = small2_v[:, 2:4, :]
            for copy in small_out:
                copy.start()
        in_copy(4, layer).wait()
        in_copy(5, layer).wait()
        prefetch(4 * step + 4)
        for c in range(2):
            if step > 0:
                wait(o_copies(layer, c))
            lt = attn[layer, :, :].T[c * (ATT // 2):(c + 1) * (ATT // 2)]
            for n in range(0, D, C):
                obuf[c, :, n:n + C] = mm(lt, da[layer, :, n:n + C]).astype(BF16)
            start(o_copies(layer, c))
        in_copy(6, layer).wait()
        in_copy(7, layer).wait()
        prefetch(4 * step + 5)
        qbase = step * NC

        @pl.loop(0, NC)
        def _(c):
            slot = lax.rem(qbase + c, 3)

            @pl.when(qbase + c >= 3)
            def _():
                wait(q_copies(layer, c, slot))
            lt = h[layer, :, chunk(c)].T
            for n in range(0, QKV, 3 * HD):
                vals = mm(lt, dqkv[layer, :, n:n + 3 * HD]).astype(BF16)
                for j in range(3):
                    qbuf[slot, n // HD + j] = vals[:, j * HD:(j + 1) * HD]
            start(q_copies(layer, c, slot))
    for copy in small_out:
        copy.wait()
    for slot in range(SLOTS):
        wait(big_copies(wu_o, 0, 0, slot))
    for slot in range(3):
        wait(q_copies(0, 0, slot))
    for c in range(2):
        wait(o_copies(0, c))


def solution(mesh):
    vmem = pl.BlockSpec(memory_space=pltpu.VMEM)
    hbm = pl.BlockSpec(memory_space=pl.ANY)

    def device_step(x_loc, dy_loc, ln_par, bias_d, w_qkv, w_out, w_up, b_up, w_down):
        wqkv_t = jnp.transpose(w_qkv, (0, 2, 3, 1, 4)).reshape(N_LAYERS, 3 * HEADS, D, HD)
        wo_t = w_out.reshape(N_LAYERS, ATT, D)
        sds = jax.ShapeDtypeStruct
        gath = (N_LAYERS, 4, BLK, D)
        dma = pltpu.SemaphoreType.DMA
        chain_out = pl.pallas_call(
            chain_kernel,
            name='chain',
            out_shape=(sds((BLK, D), BF16), sds((BLK, D), BF16), sds((N_LAYERS, 2, D), F32), sds((N_LAYERS, 4, D), F32), sds((N_LAYERS, FF), F32),
                       sds(gath, BF16), sds(gath, BF16), sds(gath, BF16), sds(gath, BF16),
                       sds((N_LAYERS, SEQ, ATT), BF16), sds((N_LAYERS, SEQ, FF), BF16), sds((N_LAYERS, SEQ, FF), BF16),
                       sds((N_LAYERS, SEQ, QKV), BF16)),
            in_specs=[vmem] * 5 + [hbm] * 4,
            out_specs=tuple([vmem] * 5 + [hbm] * 8),
            scratch_shapes=[
                pltpu.VMEM((D, QKV), BF16), pltpu.VMEM((ATT, D), BF16), pltpu.VMEM((D, FF), BF16), pltpu.VMEM((FF, D), BF16),
                pltpu.VMEM(gath, BF16), pltpu.VMEM(gath, BF16), pltpu.VMEM(gath, BF16), pltpu.VMEM(gath, BF16),
                pltpu.VMEM((N_LAYERS, SEQ, QKV), BF16), pltpu.VMEM((N_LAYERS, HEADS, SEQ, SEQ), BF16),
                pltpu.VMEM((N_LAYERS, SEQ, ATT), BF16), pltpu.VMEM((N_LAYERS, SEQ, FF), BF16), pltpu.VMEM((SEQ, FF), F32),
                pltpu.VMEM((N_LAYERS, SEQ, FF), BF16), pltpu.VMEM((N_LAYERS, SEQ, QKV), BF16),
                pltpu.VMEM((N_LAYERS, BLK, D), F32), pltpu.VMEM((N_LAYERS, BLK, D), F32),
                pltpu.VMEM((N_LAYERS, BLK, 128), F32), pltpu.VMEM((N_LAYERS, BLK, 128), F32),
                pltpu.VMEM((BLK, D), F32), pltpu.VMEM((BLK, D), F32), pltpu.VMEM((SEQ, D), F32), pltpu.VMEM((D, SEQ), F32),
                pltpu.VMEM((2, 2, 2, BLK, D), F32), pltpu.VMEM((2, BLK, D), F32), pltpu.VMEM((3, 2, BLK, D), F32),
                pltpu.VMEM((3, BLK, D), BF16), pltpu.VMEM((2, BLK, D), BF16),
                pltpu.VMEM((N_LAYERS, 2, D), F32), pltpu.VMEM((N_LAYERS, 4, D), F32), pltpu.VMEM((N_LAYERS, 3, 2, D), F32), pltpu.VMEM((N_LAYERS, 3, 4, D), F32),
                dma((4, 3 * HEADS)), dma((8, N_LAYERS)), dma((2, 6, NA)), dma((3, 4, NC)), dma((2, N_LAYERS, 2, 3)),
            ],
            compiler_params=pltpu.CompilerParams(collective_id=0, has_side_effects=True, vmem_limit_bytes=VMEM_ALL),
        )(x_loc, dy_loc, ln_par, bias_d, b_up, wqkv_t, wo_t, w_up, w_down)
        y_loc, xg_loc, small1, small2, bupg, h, h2, dm, da, attn, act, dpre, dqkv = chain_out
        flat = (N_LAYERS, SEQ, D)
        y_out, x_grad, lng, biasg, wqkv_g, wo_g, wu_g, bupg_o, wd_g = pl.pallas_call(
            grads_kernel,
            name='grads',
            out_shape=(sds((BLK, D), BF16), sds((BLK, D), BF16), sds((N_LAYERS, 4, D), F32), sds((N_LAYERS, 2, D), F32),
                       sds((N_LAYERS, 3 * HEADS, D, HD), BF16), sds((N_LAYERS, ATT, D), BF16), sds((N_LAYERS, D, FF), BF16),
                       sds((N_LAYERS, FF), F32), sds((N_LAYERS, FF, D), BF16)),
            in_specs=[hbm] * 13,
            out_specs=tuple([hbm] * 9),
            scratch_shapes=[
                pltpu.VMEM(flat, BF16), pltpu.VMEM(flat, BF16), pltpu.VMEM(flat, BF16), pltpu.VMEM(flat, BF16),
                pltpu.VMEM((N_LAYERS, SEQ, ATT), BF16), pltpu.VMEM((N_LAYERS, SEQ, FF), BF16), pltpu.VMEM((N_LAYERS, SEQ, FF), BF16),
                pltpu.VMEM((N_LAYERS, SEQ, QKV), BF16),
                pltpu.VMEM((SLOTS, C, D), BF16), pltpu.VMEM((3, 3 * HEADS, C, HD), BF16), pltpu.VMEM((2, ATT // 2, D), BF16),
                pltpu.VMEM((BLK, D), BF16), pltpu.VMEM((BLK, D), BF16), pltpu.VMEM((N_LAYERS, 2, D), F32), pltpu.VMEM((N_LAYERS, 4, D), F32),
                pltpu.VMEM((N_LAYERS, FF), F32), pltpu.VMEM((N_LAYERS, 4, D), F32), pltpu.VMEM((N_LAYERS, 2, D), F32),
                dma((8, N_LAYERS)), dma((SLOTS, C // 128)), dma((3, HEADS)), dma((2, 2)), dma((5,)),
            ],
            compiler_params=pltpu.CompilerParams(vmem_limit_bytes=VMEM_ALL),
        )(y_loc, xg_loc, small1, small2, bupg, h.reshape(flat), h2.reshape(flat), dm.reshape(flat), da.reshape(flat), attn, act, dpre, dqkv)
        wqkv_g = jnp.transpose(wqkv_g.reshape(N_LAYERS, 3, HEADS, D, HD), (0, 3, 1, 2, 4))
        return (y_out[None], x_grad[None], lng, biasg, wqkv_g, wo_g.reshape(N_LAYERS, HEADS, HD, D), wu_g, bupg_o, wd_g)

    in_specs = (P('dp', 'tp', None), P('dp', 'tp', None), P(None, None, None), P(None, None, None),
                P(None, None, None, 'tp', None), P(None, 'tp', None, None), P(None, None, 'tp'), P(None, 'tp'), P(None, 'tp', None))
    out_specs = (P('dp', 'tp', None), P('dp', 'tp', None), P('dp', None, None), P('dp', None, None),
                 P('dp', None, None, 'tp', None), P('dp', 'tp', None, None), P('dp', None, 'tp'), P('dp', 'tp'), P('dp', 'tp', None))
    return jax.shard_map(device_step, mesh=mesh, in_specs=in_specs, out_specs=out_specs, check_vma=False)
```

```python
import jax
import jax.numpy as jnp
from jax import lax
from jax.experimental import pallas as pl
from jax.experimental.pallas import tpu as pltpu
from jax.sharding import PartitionSpec as P

MESH = pl.DeviceIdType.MESH
F32, BF16 = jnp.float32, jnp.bfloat16
N_LAYERS, SEQ, BLK, D, HEADS, HD, FF = 2, 128, 32, 2560, 5, 128, 2560
ATT = HEADS * HD
QKV = 3 * ATT
C = 512
NC = D // C
SLOTS = 4
CA = 512
NA = D // CA
ND = 0
SCALE = HD ** -0.5
GELU_K = 0.7978845608028654
GELU_C = 0.044715
VMEM_ALL = 67043328


def mm(a, b):
    return jnp.dot(a, b, preferred_element_type=F32)


def mm_nt(a, b):
    return lax.dot_general(a, b, (((1,), (1,)), ((), ())), preferred_element_type=F32)


def chunk(c, size=C):
    return pl.ds(pl.multiple_of(c * size, size), size)


def chain_kernel(x_ref, dy_ref, ln_ref, bias_ref, bup_ref, wqkv_h, wo_h, wu_h, wd_h,
                 y_ref, xg_ref, small1_ref, small2_ref, bupg_ref, h_o, h2_o, dm_o, da_o, a_o, act_o, dpre_o, dqkv_o,
                 wq, wo, wu, wd, h_g, h2_g, dm_g, da_g, qkv, prob, attn, act, gp, dpre, dqkv,
                 xh1, xh2, rs1, rs2, res, dres, acc, acct, part, own, rr, xx, ss, sg1, sg2, sgr1, sgr2,
                 wsem, osem, agsem, rssem, gsem):
    me = lax.axis_index('tp')
    x_id = lax.div(me, 2)
    core = lax.rem(me, 2)
    sib = x_id * 2 + (1 - core)
    cross = (1 - x_id) * 2 + core
    diag = (1 - x_id) * 2 + (1 - core)

    def remote(src, dst, send, recv, dev):
        return pltpu.make_async_remote_copy(src_ref=src, dst_ref=dst, send_sem=send, recv_sem=recv,
                                            device_id={'tp': dev}, device_id_type=MESH)

    def weight_copies(kind, layer):
        if kind == 0:
            return [pltpu.make_async_copy(wqkv_h.at[layer, j], wq.at[:, pl.ds(j * HD, HD)], wsem.at[0, j]) for j in range(3 * HEADS)]
        if kind == 1:
            return [pltpu.make_async_copy(wo_h.at[layer], wo, wsem.at[1, 0])]
        src, dst = ((wu_h, wu), (wd_h, wd))[kind - 2]
        return [pltpu.make_async_copy(src.at[layer, pl.ds(j * C, C)], dst.at[pl.ds(j * C, C)], wsem.at[kind, j]) for j in range(NC)]

    def load_w(kind, layer):
        for copy in weight_copies(kind, layer):
            copy.start()

    def wait_w(kind, layer):
        for copy in weight_copies(kind, layer):
            copy.wait()

    def out_copy(i, src, dst, layer):
        return pltpu.make_async_copy(src.at[layer], dst.at[layer], osem.at[i, layer])

    outs = [(h_g, h_o), (h2_g, h2_o), (dm_g, dm_o), (da_g, da_o), (attn, a_o), (act, act_o), (dpre, dpre_o), (dqkv, dqkv_o)]

    def ag_mine(g, layer, c, k, i, dev):
        mine = g.at[layer, me, :, chunk(c, CA)]
        return remote(mine, mine, agsem.at[k, i, 0], agsem.at[k, i + 1, c], dev)

    def ag_side(g, layer, c, k=0):
        return ag_mine(g, layer, c, k, 0, sib)

    def ag_across(g, layer, c, k=0):
        return ag_mine(g, layer, c, k, 2, cross)

    def ag_forward(g, layer, c, k=0):
        theirs = g.at[layer, cross, :, chunk(c, CA)]
        return remote(theirs, theirs, agsem.at[k, 4, 0], agsem.at[k, 5, c], sib)

    def ag_direct(g, layer, c, k=0):
        return ag_mine(g, layer, c, k, 4, diag)

    def ag_sent(g, layer, k=0):
        for i, dev in ((0, sib), (2, cross), (4, sib)):
            remote(g.at[layer, me], g.at[layer, me], agsem.at[k, i, 0], agsem.at[k, i + 1, 0], dev).wait_send()

    def ag_relay(g, layer, k):
        @pl.loop(0, NA)
        def _(c):
            ag_across(g, layer, c, k).wait_recv()

            @pl.when(c < NA - ND)
            def _():
                ag_forward(g, layer, c, k).start()

    def ag_finish(g, layer, k):
        @pl.loop(0, NA)
        def _(c):
            ag_side(g, layer, c, k).wait_recv()
            ag_forward(g, layer, c, k).wait_recv()
        ag_sent(g, layer, k)

    def ag_start(g, layer, k=0):
        for c in range(NA):
            ag_across(g, layer, c, k).start()
            if c >= NA - ND:
                ag_direct(g, layer, c, k).start()
        for c in range(NA):
            ag_side(g, layer, c, k).start()

    def ag_consume(g, layer, compute, lag=2):
        @pl.loop(0, NA + lag)
        def _(c):
            @pl.when(c < NA)
            def _():
                ag_across(g, layer, c).wait_recv()

            @pl.when(c < NA - ND)
            def _():
                ag_forward(g, layer, c).start()

            @pl.when(c >= lag)
            def _():
                cc = c - lag
                ag_side(g, layer, cc).wait_recv()
                ag_forward(g, layer, cc).wait_recv()
                compute(cc)

        ag_sent(g, layer)

    def rs_side(par, c):
        return remote(part.at[par // 2, :, 1 - core, :, chunk(c)], rr.at[par, :, :, chunk(c)],
                      rssem.at[par, 0, 0], rssem.at[par, 1, c], sib)

    def rs_across(par, c):
        return remote(ss.at[par // 2, :, chunk(c)], xx.at[par, :, chunk(c)], rssem.at[par, 2, 0], rssem.at[par, 3, 0], cross)

    def rs_send(par, compute, lag=2):
        buf = par // 2

        @pl.loop(0, NC + lag)
        def _(c):
            @pl.when(c < NC)
            def _():
                vals = compute(c)
                for b in range(4):
                    part[buf, b // 2, b % 2, :, chunk(c)] = vals[b * BLK:(b + 1) * BLK]
                rs_side(par, c).start()

            @pl.when(c >= lag)
            def _():
                cc = c - lag
                rs_side(par, cc).wait_recv()
                cols = chunk(cc)
                ss[buf, :, cols] = (part[buf, 1 - x_id, core, :, cols] + rr[par, 1 - x_id, :, cols]).astype(BF16)
                rs_across(par, cc).start()
                own[buf, :, cols] = part[buf, x_id, core, :, cols] + rr[par, x_id, :, cols]

    def rs_within(par, compute):
        @pl.loop(0, NC)
        def _(c):
            vals = compute(c)
            for b in range(4):
                part[par // 2, b // 2, b % 2, :, chunk(c)] = vals[b * BLK:(b + 1) * BLK]
            rs_side(par, c).start()

    def rs_cross(par):
        buf = par // 2

        @pl.loop(0, NC)
        def _(c):
            rs_side(par, c).wait_recv()
            cols = chunk(c)
            ss[buf, :, cols] = (part[buf, 1 - x_id, core, :, cols] + rr[par, 1 - x_id, :, cols]).astype(BF16)
            rs_across(par, c).start()
            own[buf, :, cols] = part[buf, x_id, core, :, cols] + rr[par, x_id, :, cols]

    def rs_finish(par):
        buf = par // 2
        remote(part.at[buf, :, 1 - core], rr.at[par], rssem.at[par, 0, 0], rssem.at[par, 1, 0], sib).wait_send()
        remote(ss.at[buf], xx.at[par], rssem.at[par, 2, 0], rssem.at[par, 3, 0], cross).wait()
        return own[buf] + xx[par].astype(F32)

    def normed(vals, gain, shift, xh, rs, layer):
        mean_val = jnp.mean(vals, axis=-1, keepdims=True)
        centered = vals - mean_val
        rstd = lax.rsqrt(jnp.mean(centered * centered, axis=-1, keepdims=True) + 1e-5)
        hat = centered * rstd
        xh[layer] = hat
        rs[layer] = jnp.broadcast_to(rstd, (BLK, 128))
        return (hat * gain + shift).astype(BF16)

    def norm_grad(d_out, gain, xh, rs, layer, rows):
        hat = xh[layer]
        rstd = rs[layer][:, :1]
        rows[layer, 0:1, :] = jnp.sum(d_out * hat, axis=0, keepdims=True)
        rows[layer, 1:2, :] = jnp.sum(d_out, axis=0, keepdims=True)
        d_hat = d_out * gain
        m1 = jnp.mean(d_hat, axis=-1, keepdims=True)
        m2 = jnp.mean(d_hat * hat, axis=-1, keepdims=True)
        return rstd * (d_hat - m1 - hat * m2)

    def small_copies(kind, layer):
        src, dst = ((sg1, sgr1), (sg2, sgr2))[kind]
        return [remote(src.at[layer], dst.at[layer, i], gsem.at[kind, layer, 0, i], gsem.at[kind, layer, 1, i], dev)
                for i, dev in enumerate((sib, cross, diag))]

    def small_start(kind, layer):
        for copy in small_copies(kind, layer):
            copy.start()

    load_w(0, 0)
    barrier = pltpu.get_barrier_semaphore()
    for dev in (sib, cross, diag):
        pl.semaphore_signal(barrier, inc=1, device_id={'tp': dev}, device_id_type=MESH)
    res[...] = x_ref[0].astype(F32)
    pl.semaphore_wait(barrier, 3)

    row_id = lax.broadcasted_iota(jnp.int32, (SEQ, SEQ), 0)
    col_id = lax.broadcasted_iota(jnp.int32, (SEQ, SEQ), 1)
    causal = row_id >= col_id

    def dact_chunk(c):
        g = dm_g[0, :, :, chunk(c, CA)].reshape(SEQ, CA)
        acct[...] += mm_nt(wd[:, chunk(c, CA)], g)

    def dact_early(layer, lo, hi):
        @pl.when(layer == N_LAYERS - 1)
        def _():
            @pl.loop(lo, hi)
            def _(c):
                acct[chunk(c), :] = mm_nt(wd[chunk(c), :], dm_g[N_LAYERS - 1].reshape(SEQ, D))

    def act_chunk(layer, c):
        pre = acc[:, chunk(c)] + bup_ref[layer:layer + 1, chunk(c)]
        t = jnp.tanh(pre * (GELU_K + (GELU_K * GELU_C) * (pre * pre)))
        act[layer, :, chunk(c)] = (pre * (0.5 + 0.5 * t)).astype(BF16)

    def slope_chunk(layer, c):
        pre = acc[:, chunk(c)] + bup_ref[layer:layer + 1, chunk(c)]
        sq = pre * pre
        t = jnp.tanh(pre * (GELU_K + (GELU_K * GELU_C) * sq))
        return (0.5 + 0.5 * t) + (pre * (1.0 - t * t)) * (0.5 * GELU_K + (1.5 * GELU_K * GELU_C) * sq)

    def dpre_chunk(layer, c, slope):
        d_pre = acct[chunk(c), :].T * slope
        bupg_ref[layer:layer + 1, chunk(c)] = jnp.sum(d_pre, axis=0, keepdims=True)
        dpre[layer, :, chunk(c)] = d_pre.astype(BF16)

    @pl.loop(0, N_LAYERS)
    def _(layer):
        first = layer == 0
        last = layer == N_LAYERS - 1
        lnp = ln_ref[layer]
        h_g[layer, me] = normed(res[...], lnp[0:1], lnp[1:2], xh1, rs1, layer)
        ag_start(h_g, layer)
        acc[...] = jnp.zeros_like(acc)
        wait_w(0, layer)

        @pl.when(first)
        def _():
            load_w(1, 0)
            load_w(2, 0)

        def qkv_chunk(c):
            h = h_g[layer, :, :, chunk(c, CA)].reshape(SEQ, CA)
            for n in range(0, QKV, 640):
                acc[:, n:n + 640] += mm(h, wq[chunk(c, CA), n:n + 640])
        ag_consume(h_g, layer, qkv_chunk)
        out_copy(0, h_g, h_o, layer).start()

        @pl.when(first)
        def _():
            load_w(0, 1)
            dm_g[N_LAYERS - 1, me] = dy_ref[0]
            ag_start(dm_g, N_LAYERS - 1, 1)

        for j in range(3 * HEADS):
            qkv[layer, :, j * HD:(j + 1) * HD] = acc[:, j * HD:(j + 1) * HD].astype(BF16)
        for hd in range(HEADS):
            q = qkv[layer, :, hd * HD:(hd + 1) * HD]
            k = qkv[layer, :, ATT + hd * HD:ATT + (hd + 1) * HD]
            v = qkv[layer, :, 2 * ATT + hd * HD:2 * ATT + (hd + 1) * HD]
            scores = jnp.where(causal, mm_nt(q, k) * SCALE, -1e30)
            e = jnp.exp(scores - jnp.max(scores, axis=-1, keepdims=True))
            p = (e / jnp.sum(e, axis=-1, keepdims=True)).astype(BF16)
            prob[layer, hd] = p
            attn[layer, :, hd * HD:(hd + 1) * HD] = mm(p, v).astype(BF16)
        out_copy(4, attn, a_o, layer).start()
        wait_w(1, layer)

        @pl.when(first)
        def _():
            load_w(3, 0)
        @pl.when(last)
        def _():
            wait_w(3, N_LAYERS - 1)
        rs_send(0, lambda c: mm(attn[layer], wo[:, chunk(c)]))
        dact_early(layer, 0, 2)

        @pl.when(first)
        def _():
            ag_relay(dm_g, N_LAYERS - 1, 1)
        total = rs_finish(0)
        res[...] = res[...] + total + bias_ref[layer, 0:1]

        @pl.when(first)
        def _():
            load_w(1, 1)
            ag_finish(dm_g, N_LAYERS - 1, 1)
            out_copy(2, dm_g, dm_o, N_LAYERS - 1).start()

        h2_g[layer, me] = normed(res[...], lnp[2:3], lnp[3:4], xh2, rs2, layer)
        ag_start(h2_g, layer)
        acc[...] = jnp.zeros_like(acc)
        wait_w(2, layer)
        dact_early(layer, 2, NC)

        def up_chunk(c):
            h = h2_g[layer, :, :, chunk(c, CA)].reshape(SEQ, CA)
            for n in range(0, FF, C):
                acc[:, n:n + C] += mm(h, wu[chunk(c, CA), n:n + C])
        ag_consume(h2_g, layer, up_chunk)
        out_copy(1, h2_g, h2_o, layer).start()

        @pl.when(first)
        def _():
            load_w(2, 1)

        @pl.when(first)
        def _():
            @pl.loop(0, FF // C)
            def _(c):
                act_chunk(0, c)
            out_copy(5, act, act_o, 0).start()
            wait_w(3, 0)
            rs_send(1, lambda c: mm(act[0], wd[:, chunk(c)]))

            @pl.loop(0, FF // C)
            def _(c):
                gp[:, chunk(c)] = slope_chunk(0, c)
            total = rs_finish(1)
            load_w(3, 1)
            res[...] = res[...] + total + bias_ref[0, 1:2]

    @pl.loop(0, FF // C)
    def _(c):
        dpre_chunk(N_LAYERS - 1, c, slope_chunk(N_LAYERS - 1, c))
    out_copy(6, dpre, dpre_o, N_LAYERS - 1).start()
    dres[...] = dy_ref[0].astype(F32)

    @pl.loop(0, N_LAYERS)
    def _(step):
        layer = N_LAYERS - 1 - step
        top = step == 0
        low = step == N_LAYERS - 1
        lnp = ln_ref[layer]
        sg2[layer, 3:4, :] = jnp.sum(dres[...], axis=0, keepdims=True)
        @pl.when(low)
        def _():
            dm_g[0, me] = dres[...].astype(BF16)
            ag_start(dm_g, 0)
            small_start(0, N_LAYERS - 1)
            small_start(1, N_LAYERS - 1)
            acct[...] = jnp.zeros_like(acct)
            wait_w(3, 0)
            ag_consume(dm_g, 0, dact_chunk)
            out_copy(2, dm_g, dm_o, 0).start()

        @pl.when(low)
        def _():
            @pl.loop(0, FF // C)
            def _(c):
                dpre_chunk(0, c, gp[:, chunk(c)])
            out_copy(6, dpre, dpre_o, 0).start()

        @pl.when(low)
        def _():
            wait_w(2, 0)
        rs_send(0, lambda c: mm_nt(wu[chunk(c), :], dpre[layer]).T)

        @pl.when(top)
        def _():
            load_w(2, 0)

            @pl.loop(0, FF // C)
            def _(c):
                act_chunk(N_LAYERS - 1, c)
            out_copy(5, act, act_o, N_LAYERS - 1).start()
            rs_within(2, lambda c: mm(act[N_LAYERS - 1], wd[:, chunk(c)]))
            load_w(3, 0)
        total = rs_finish(0)
        dres[...] = dres[...] + norm_grad(total, lnp[2:3], xh2, rs2, layer, sg2)

        sg2[layer, 2:3, :] = jnp.sum(dres[...], axis=0, keepdims=True)
        da_g[layer, me] = dres[...].astype(BF16)
        ag_start(da_g, layer)
        acct[0:ATT, :] = jnp.zeros((ATT, SEQ), F32)

        @pl.when(low)
        def _():
            wait_w(1, 0)

        def dattn_chunk(c):
            g = da_g[layer, :, :, chunk(c, CA)].reshape(SEQ, CA)
            acct[0:ATT, :] += mm_nt(wo[:, chunk(c, CA)], g)
        ag_consume(da_g, layer, dattn_chunk)
        out_copy(3, da_g, da_o, layer).start()

        @pl.when(top)
        def _():
            load_w(1, 0)
            rs_cross(2)

        @pl.when(low)
        def _():
            small_start(1, 0)

        for hd in range(HEADS):
            q = qkv[layer, :, hd * HD:(hd + 1) * HD]
            k = qkv[layer, :, ATT + hd * HD:ATT + (hd + 1) * HD]
            v = qkv[layer, :, 2 * ATT + hd * HD:2 * ATT + (hd + 1) * HD]
            p = prob[layer, hd]
            d_o = acct[hd * HD:(hd + 1) * HD, :].T.astype(BF16)
            d_p = mm_nt(d_o, v)
            d_v = mm(p.T, d_o)
            pf = p.astype(F32)
            dot = jnp.sum(d_p * pf, axis=-1, keepdims=True)
            d_s = (pf * (d_p - dot) * SCALE).astype(BF16)
            dqkv[layer, :, hd * HD:(hd + 1) * HD] = mm(d_s, k).astype(BF16)
            dqkv[layer, :, ATT + hd * HD:ATT + (hd + 1) * HD] = mm(d_s.T, q).astype(BF16)
            dqkv[layer, :, 2 * ATT + hd * HD:2 * ATT + (hd + 1) * HD] = d_v.astype(BF16)
        out_copy(7, dqkv, dqkv_o, layer).start()

        @pl.when(low)
        def _():
            wait_w(0, 0)
        rs_send(1, lambda c: mm_nt(wq[chunk(c), :], dqkv[layer]).T)

        @pl.when(top)
        def _():
            load_w(0, 0)
            y_ref[...] = (res[...] + rs_finish(2) + bias_ref[N_LAYERS - 1, 1:2]).astype(BF16)
        total = rs_finish(1)
        dres[...] = dres[...] + norm_grad(total, lnp[0:1], xh1, rs1, layer, sg1)

    small_start(0, 0)
    xg_ref[...] = dres[...].astype(BF16)
    for kind, layer in ((0, 1), (1, 1), (1, 0), (0, 0)):
        src, dst, out = ((sg1, sgr1, small1_ref), (sg2, sgr2, small2_ref))[kind]
        for copy in small_copies(kind, layer):
            copy.wait()
        out[layer] = (src[layer] + dst[layer, 0]) + (dst[layer, 1] + dst[layer, 2])
    for layer in range(N_LAYERS):
        for i, (src, dst) in enumerate(outs):
            out_copy(i, src, dst, layer).wait()


def grads_kernel(y_in, xg_in, small1_in, small2_in, bupg_in, h_h, h2_h, dm_h, da_h, a_h, act_h, dpre_h, dqkv_h,
                 y_o, xg_o, lng_o, biasg_o, wqkv_o, wo_o, wu_o, bupg_o, wd_o,
                 h, h2, dm, da, attn, act, dpre, dqkv, big, qbuf, obuf, y_v, xg_v, small1_v, small2_v, bupg_v, lng_v, biasg_v, isem, bsem, qsem, osem, psem):
    ins = [(dm_h, dm), (act_h, act), (h2_h, h2), (dpre_h, dpre), (da_h, da), (a_h, attn), (h_h, h), (dqkv_h, dqkv)]

    def in_copy(i, layer):
        return pltpu.make_async_copy(ins[i][0].at[layer], ins[i][1].at[layer], isem.at[i, layer])

    order = [(i, layer) for layer in reversed(range(N_LAYERS)) for i in range(0, len(ins), 2)]

    def prefetch(k):
        if k < len(order):
            in_copy(order[k][0], order[k][1]).start()
            in_copy(order[k][0] + 1, order[k][1]).start()

    prefetch(0)
    prefetch(1)
    small_in = [pltpu.make_async_copy(src, dst, psem.at[i]) for i, (src, dst) in enumerate(
        ((y_in, y_v), (xg_in, xg_v), (small1_in, small1_v), (small2_in, small2_v), (bupg_in, bupg_v)))]
    small_out = [pltpu.make_async_copy(src, dst, psem.at[i]) for i, (src, dst) in enumerate(
        ((y_v, y_o), (xg_v, xg_o), (lng_v, lng_o), (biasg_v, biasg_o), (bupg_v, bupg_o)))]
    for copy in small_in:
        copy.start()

    def big_copies(dst, layer, c, slot):
        return [pltpu.make_async_copy(big.at[slot, pl.ds(r * 128, 128)], dst.at[layer, pl.ds(pl.multiple_of(c * C + r * 128, 128), 128)],
                                      bsem.at[slot, r]) for r in range(C // 128)]

    def q_copies(layer, c, slot):
        return [pltpu.make_async_copy(qbuf.at[slot, pl.ds(3 * j, 3)], wqkv_o.at[layer, pl.ds(3 * j, 3), chunk(c), :], qsem.at[slot, j])
                for j in range(HEADS)]

    def o_copies(layer, c):
        return [pltpu.make_async_copy(obuf.at[c, pl.ds(r * 160, 160)], wo_o.at[layer, pl.ds(c * (ATT // 2) + r * 160, 160)], osem.at[c, r])
                for r in range(2)]

    def start(copies):
        for copy in copies:
            copy.start()

    def wait(copies):
        for copy in copies:
            copy.wait()

    for step, layer in enumerate(reversed(range(N_LAYERS))):
        for w, (dst, left, right) in enumerate(((wd_o, act, dm), (wu_o, h2, dpre))):
            in_copy(2 * w, layer).wait()
            in_copy(2 * w + 1, layer).wait()
            prefetch(4 * step + w + 2)
            base = (2 * step + w) * NC

            @pl.loop(0, NC)
            def _(c):
                slot = lax.rem(base + c, SLOTS)

                @pl.when(base + c >= SLOTS)
                def _():
                    wait(big_copies(dst, layer, c, slot))
                lt = left[layer, :, chunk(c)].T
                for n in range(0, D, C):
                    big[slot, :, n:n + C] = mm(lt, right[layer, :, n:n + C]).astype(BF16)
                start(big_copies(dst, layer, c, slot))
        if step == 0:
            for copy in small_in:
                copy.wait()
            lng_v[:, 0:2, :] = small1_v[...]
            lng_v[:, 2:4, :] = small2_v[:, 0:2, :]
            biasg_v[...] = small2_v[:, 2:4, :]
            for copy in small_out:
                copy.start()
        in_copy(4, layer).wait()
        in_copy(5, layer).wait()
        prefetch(4 * step + 4)
        for c in range(2):
            if step > 0:
                wait(o_copies(layer, c))
            lt = attn[layer, :, :].T[c * (ATT // 2):(c + 1) * (ATT // 2)]
            for n in range(0, D, C):
                obuf[c, :, n:n + C] = mm(lt, da[layer, :, n:n + C]).astype(BF16)
            start(o_copies(layer, c))
        in_copy(6, layer).wait()
        in_copy(7, layer).wait()
        prefetch(4 * step + 5)
        qbase = step * NC

        @pl.loop(0, NC)
        def _(c):
            slot = lax.rem(qbase + c, 3)

            @pl.when(qbase + c >= 3)
            def _():
                wait(q_copies(layer, c, slot))
            lt = h[layer, :, chunk(c)].T
            for n in range(0, QKV, 3 * HD):
                vals = mm(lt, dqkv[layer, :, n:n + 3 * HD]).astype(BF16)
                for j in range(3):
                    qbuf[slot, n // HD + j] = vals[:, j * HD:(j + 1) * HD]
            start(q_copies(layer, c, slot))
    for copy in small_out:
        copy.wait()
    for slot in range(SLOTS):
        wait(big_copies(wu_o, 0, 0, slot))
    for slot in range(3):
        wait(q_copies(0, 0, slot))
    for c in range(2):
        wait(o_copies(0, c))


def solution(mesh):
    vmem = pl.BlockSpec(memory_space=pltpu.VMEM)
    hbm = pl.BlockSpec(memory_space=pl.ANY)

    def device_step(x_loc, dy_loc, ln_par, bias_d, w_qkv, w_out, w_up, b_up, w_down):
        wqkv_t = jnp.transpose(w_qkv, (0, 2, 3, 1, 4)).reshape(N_LAYERS, 3 * HEADS, D, HD)
        wo_t = w_out.reshape(N_LAYERS, ATT, D)
        sds = jax.ShapeDtypeStruct
        gath = (N_LAYERS, 4, BLK, D)
        dma = pltpu.SemaphoreType.DMA
        chain_out = pl.pallas_call(
            chain_kernel,
            name='chain',
            out_shape=(sds((BLK, D), BF16), sds((BLK, D), BF16), sds((N_LAYERS, 2, D), F32), sds((N_LAYERS, 4, D), F32), sds((N_LAYERS, FF), F32),
                       sds(gath, BF16), sds(gath, BF16), sds(gath, BF16), sds(gath, BF16),
                       sds((N_LAYERS, SEQ, ATT), BF16), sds((N_LAYERS, SEQ, FF), BF16), sds((N_LAYERS, SEQ, FF), BF16),
                       sds((N_LAYERS, SEQ, QKV), BF16)),
            in_specs=[vmem] * 5 + [hbm] * 4,
            out_specs=tuple([vmem] * 5 + [hbm] * 8),
            scratch_shapes=[
                pltpu.VMEM((D, QKV), BF16), pltpu.VMEM((ATT, D), BF16), pltpu.VMEM((D, FF), BF16), pltpu.VMEM((FF, D), BF16),
                pltpu.VMEM(gath, BF16), pltpu.VMEM(gath, BF16), pltpu.VMEM(gath, BF16), pltpu.VMEM(gath, BF16),
                pltpu.VMEM((N_LAYERS, SEQ, QKV), BF16), pltpu.VMEM((N_LAYERS, HEADS, SEQ, SEQ), BF16),
                pltpu.VMEM((N_LAYERS, SEQ, ATT), BF16), pltpu.VMEM((N_LAYERS, SEQ, FF), BF16), pltpu.VMEM((SEQ, FF), F32),
                pltpu.VMEM((N_LAYERS, SEQ, FF), BF16), pltpu.VMEM((N_LAYERS, SEQ, QKV), BF16),
                pltpu.VMEM((N_LAYERS, BLK, D), F32), pltpu.VMEM((N_LAYERS, BLK, D), F32),
                pltpu.VMEM((N_LAYERS, BLK, 128), F32), pltpu.VMEM((N_LAYERS, BLK, 128), F32),
                pltpu.VMEM((BLK, D), F32), pltpu.VMEM((BLK, D), F32), pltpu.VMEM((SEQ, D), F32), pltpu.VMEM((D, SEQ), F32),
                pltpu.VMEM((2, 2, 2, BLK, D), F32), pltpu.VMEM((2, BLK, D), F32), pltpu.VMEM((3, 2, BLK, D), F32),
                pltpu.VMEM((3, BLK, D), BF16), pltpu.VMEM((2, BLK, D), BF16),
                pltpu.VMEM((N_LAYERS, 2, D), F32), pltpu.VMEM((N_LAYERS, 4, D), F32), pltpu.VMEM((N_LAYERS, 3, 2, D), F32), pltpu.VMEM((N_LAYERS, 3, 4, D), F32),
                dma((4, 3 * HEADS)), dma((8, N_LAYERS)), dma((2, 6, NA)), dma((3, 4, NC)), dma((2, N_LAYERS, 2, 3)),
            ],
            compiler_params=pltpu.CompilerParams(collective_id=0, has_side_effects=True, vmem_limit_bytes=VMEM_ALL),
        )(x_loc, dy_loc, ln_par, bias_d, b_up, wqkv_t, wo_t, w_up, w_down)
        y_loc, xg_loc, small1, small2, bupg, h, h2, dm, da, attn, act, dpre, dqkv = chain_out
        flat = (N_LAYERS, SEQ, D)
        y_out, x_grad, lng, biasg, wqkv_g, wo_g, wu_g, bupg_o, wd_g = pl.pallas_call(
            grads_kernel,
            name='grads',
            out_shape=(sds((BLK, D), BF16), sds((BLK, D), BF16), sds((N_LAYERS, 4, D), F32), sds((N_LAYERS, 2, D), F32),
                       sds((N_LAYERS, 3 * HEADS, D, HD), BF16), sds((N_LAYERS, ATT, D), BF16), sds((N_LAYERS, D, FF), BF16),
                       sds((N_LAYERS, FF), F32), sds((N_LAYERS, FF, D), BF16)),
            in_specs=[hbm] * 13,
            out_specs=tuple([hbm] * 9),
            scratch_shapes=[
                pltpu.VMEM(flat, BF16), pltpu.VMEM(flat, BF16), pltpu.VMEM(flat, BF16), pltpu.VMEM(flat, BF16),
                pltpu.VMEM((N_LAYERS, SEQ, ATT), BF16), pltpu.VMEM((N_LAYERS, SEQ, FF), BF16), pltpu.VMEM((N_LAYERS, SEQ, FF), BF16),
                pltpu.VMEM((N_LAYERS, SEQ, QKV), BF16),
                pltpu.VMEM((SLOTS, C, D), BF16), pltpu.VMEM((3, 3 * HEADS, C, HD), BF16), pltpu.VMEM((2, ATT // 2, D), BF16),
                pltpu.VMEM((BLK, D), BF16), pltpu.VMEM((BLK, D), BF16), pltpu.VMEM((N_LAYERS, 2, D), F32), pltpu.VMEM((N_LAYERS, 4, D), F32),
                pltpu.VMEM((N_LAYERS, FF), F32), pltpu.VMEM((N_LAYERS, 4, D), F32), pltpu.VMEM((N_LAYERS, 2, D), F32),
                dma((8, N_LAYERS)), dma((SLOTS, C // 128)), dma((3, HEADS)), dma((2, 2)), dma((5,)),
            ],
            compiler_params=pltpu.CompilerParams(vmem_limit_bytes=VMEM_ALL),
        )(y_loc, xg_loc, small1, small2, bupg, h.reshape(flat), h2.reshape(flat), dm.reshape(flat), da.reshape(flat), attn, act, dpre, dqkv)
        wqkv_g = jnp.transpose(wqkv_g.reshape(N_LAYERS, 3, HEADS, D, HD), (0, 3, 1, 2, 4))
        return (y_out[None], x_grad[None], lng, biasg, wqkv_g, wo_g.reshape(N_LAYERS, HEADS, HD, D), wu_g, bupg_o, wd_g)

    in_specs = (P('dp', 'tp', None), P('dp', 'tp', None), P(None, None, None), P(None, None, None),
                P(None, None, None, 'tp', None), P(None, 'tp', None, None), P(None, None, 'tp'), P(None, 'tp'), P(None, 'tp', None))
    out_specs = (P('dp', 'tp', None), P('dp', 'tp', None), P('dp', None, None), P('dp', None, None),
                 P('dp', None, None, 'tp', None), P('dp', 'tp', None, None), P('dp', None, 'tp'), P('dp', 'tp'), P('dp', 'tp', None))
    return jax.shard_map(device_step, mesh=mesh, in_specs=in_specs, out_specs=out_specs, check_vma=False)
```
